32 devices in a mesh: dp: 2 (over x), row: 4 (over z), col: 4 (over y, core).
Axes of the slice: x: 2, y: 2, z: 4, core: 2. Of those that a mesh axis runs over, the one named last changes fastest.
Arguments:
- images_in: bfloat16 [24, 577, 1024], P(('dp', 'row'), None, 'col'), may hold values from -6 to 6
- cotangent: bfloat16 [24, 577, 1024], P(('dp', 'row'), None, 'col'), may hold values from -6 to 6
- first_gain: float32 [1024], P('col'), may hold values from 0.1 to 1.9
- first_shift: float32 [1024], P('col'), may hold values from -3 to 3
- second_gain: float32 [1024], P('col'), may hold values from 0.1 to 1.9
- second_shift: float32 [1024], P('col'), may hold values from -3 to 3
- qkv_weight: bfloat16 [1024, 3, 1024], P('row', None, 'col'), may hold values from -0.1875 to 0.1875
- qv_bias: float32 [2, 1024], P(None, 'col'), may hold values from -3 to 3
- out_weight: bfloat16 [1024, 1024], P('row', 'col'), may hold values from -0.75 to 0.75
- out_bias: float32 [1024], P('col'), may hold values from -3 to 3
- fc1_weight: bfloat16 [1024, 4096], P('row', 'col'), may hold values from -0.1875 to 0.1875
- fc1_bias: float32 [4096], P('col'), may hold values from -3 to 3
- fc2_weight: bfloat16 [1024, 4096], P('row', 'col'), may hold values from -0.09375 to 0.09375
- fc2_bias: float32 [1024], P('col'), may hold values from -3 to 3
- qkv_momentum: float32 [1024, 3, 1024], P('row', None, 'col'), may hold values from -48 to 48
- qkv_variance: float32 [1024, 3, 1024], P('row', None, 'col'), may hold values from 0.1 to 4
- out_momentum: float32 [1024, 1024], P('row', 'col'), may hold values from -15 to 15
- out_variance: float32 [1024, 1024], P('row', 'col'), may hold values from 0.01 to 0.8
- fc1_momentum: float32 [1024, 4096], P('row', 'col'), may hold values from -60 to 60
- fc1_variance: float32 [1024, 4096], P('row', 'col'), may hold values from 0.5 to 10
- fc2_momentum: float32 [1024, 4096], P('row', 'col'), may hold values from -120 to 120
- fc2_variance: float32 [1024, 4096], P('row', 'col'), may hold values from 1 to 40
Outputs:
- images_out: bfloat16 [24, 577, 1024], P(('dp', 'row'), None, 'col')
- images_grad: float32 [24, 577, 1024], P(('dp', 'row'), None, 'col')
- qkv_weight_grad: float32 [1024, 3, 1024], P('row', None, 'col')
- out_weight_grad: float32 [1024, 1024], P('row', 'col')
- fc1_weight_grad: float32 [1024, 4096], P('row', 'col')
- fc2_weight_grad: float32 [1024, 4096], P('row', 'col')
- qv_bias_grad: float32 [2, 1024], P(None, 'col')
- out_bias_grad: float32 [1024], P('col')
- fc1_bias_grad: float32 [4096], P('col')
- fc2_bias_grad: float32 [1024], P('col')
- first_gain_grad: float32 [1024], P('col')
- first_shift_grad: float32 [1024], P('col')
- second_gain_grad: float32 [1024], P('col')
- second_shift_grad: float32 [1024], P('col')
- qkv_weight_new: float32 [1024, 3, 1024], P('row', None, 'col')
- out_weight_new: float32 [1024, 1024], P('row', 'col')
- fc1_weight_new: float32 [1024, 4096], P('row', 'col')
- fc2_weight_new: float32 [1024, 4096], P('row', 'col')
- qkv_momentum_new: float32 [1024, 3, 1024], P('row', None, 'col')
- out_momentum_new: float32 [1024, 1024], P('row', 'col')
- fc1_momentum_new: float32 [1024, 4096], P('row', 'col')
- fc2_momentum_new: float32 [1024, 4096], P('row', 'col')
- qkv_variance_new: float32 [1024, 3, 1024], P('row', None, 'col')
- out_variance_new: float32 [1024, 1024], P('row', 'col')
- fc1_variance_new: float32 [1024, 4096], P('row', 'col')
- fc2_variance_new: float32 [1024, 4096], P('row', 'col')
The draws below stay inside these ranges and needn't reach their ends.
All inputs are finite; a program needn't handle non-finite values.
Results may differ from the reference program's by a relative error of at most 0.019.
Values may be sent and summed in bfloat16 or wider, within the bound.
A program may use at most 192 MiB of HBM per device.

```python
import math
import jax
import jax.numpy as jnp
from jax import lax

D = 1024
HEADS = 16
HEAD_DIM = 64
FF = 4096
SEQ = 577
STEP = 3
IMAGES = 24


def levels(stream_key, dims, split, smallest, top_value):
    factor_of = 1.0
    for position, shards_of in split:
        steps = jax.random.uniform(jax.random.fold_in(jax.random.fold_in(stream_key, 6), position), (shards_of,), jnp.float32, smallest / len(split), top_value / len(split))
        factor_of = factor_of * jnp.repeat(jnp.exp(steps), dims[position] // shards_of).reshape((-1,) + (1,) * (len(dims) - 1 - position))
    return factor_of


def centred(own_key, extent, deviation, bound, split=(), held_as=jnp.bfloat16):
    factor_of = levels(own_key, extent, split, -0.22, 0.18) if split else 1.0
    values = jax.random.normal(own_key, extent, jnp.float32) * deviation * factor_of
    return jnp.minimum(jnp.maximum(values, -bound), bound).astype(held_as)


def setup_inputs(seed: int = 0) -> dict:
    arg_keys = jax.random.split(jax.random.key(seed), 23)
    images_in = centred(arg_keys[0], (IMAGES, SEQ, D), 1.0, 6.0, ((0, 8), (2, 4)))
    cotangent = centred(arg_keys[1], (IMAGES, SEQ, D), 1.0, 6.0, ((0, 8), (2, 4)))
    first_gain = jnp.clip(1.0 + 0.18 * jax.random.normal(arg_keys[2], (D,), jnp.float32), 0.1, 1.9)
    first_shift = centred(arg_keys[3], (D,), 0.5, 3.0, ((0, 4),), jnp.float32)
    second_gain = jnp.clip(1.0 + 0.18 * jax.random.normal(arg_keys[4], (D,), jnp.float32), 0.1, 1.9)
    second_shift = centred(arg_keys[5], (D,), 0.5, 3.0, ((0, 4),), jnp.float32)
    qkv_weight = centred(arg_keys[6], (D, 3, D), D ** -0.5, 0.1875, ((0, 4), (2, 4)))
    qv_bias = centred(arg_keys[7], (2, D), 0.5, 3.0, ((1, 4),), jnp.float32)
    out_weight = centred(arg_keys[8], (D, D), HEAD_DIM ** -0.5, 0.75, ((0, 4), (1, 4)))
    out_bias = centred(arg_keys[9], (D,), 0.5, 3.0, ((0, 4),), jnp.float32)
    fc1_weight = centred(arg_keys[10], (D, FF), D ** -0.5, 0.1875, ((0, 4), (1, 4)))
    fc1_bias = centred(arg_keys[11], (FF,), 0.5, 3.0, ((0, 4),), jnp.float32)
    fc2_weight = centred(arg_keys[12], (D, FF), FF ** -0.5, 0.09375, ((0, 4), (1, 4)))
    fc2_bias = centred(arg_keys[13], (D,), 0.5, 3.0, ((0, 4),), jnp.float32)
    qkv_momentum = centred(arg_keys[14], (D, 3, D), 8.0, 48.0, ((0, 4), (2, 4)), jnp.float32)
    qkv_variance = jnp.clip(jnp.exp(math.log(4.0) - 3.6888794 * jax.random.uniform(arg_keys[15], (D, 3, D), jnp.float32) ** levels(arg_keys[15], (D, 3, D), ((0, 4), (2, 4)), -0.2, 0.2)), 0.1, 4.0)
    out_momentum = centred(arg_keys[16], (D, D), 2.5, 15.0, ((0, 4), (1, 4)), jnp.float32)
    out_variance = jnp.clip(jnp.exp(math.log(0.8) - 4.3820267 * jax.random.uniform(arg_keys[17], (D, D), jnp.float32) ** levels(arg_keys[17], (D, D), ((0, 4), (1, 4)), -0.2, 0.2)), 0.01, 0.8)
    fc1_momentum = centred(arg_keys[18], (D, FF), 10.0, 60.0, ((0, 4), (1, 4)), jnp.float32)
    fc1_variance = jnp.clip(jnp.exp(math.log(10.0) - 2.9957323 * jax.random.uniform(arg_keys[19], (D, FF), jnp.float32) ** levels(arg_keys[19], (D, FF), ((0, 4), (1, 4)), -0.2, 0.2)), 0.5, 10.0)
    fc2_momentum = centred(arg_keys[20], (D, FF), 20.0, 120.0, ((0, 4), (1, 4)), jnp.float32)
    fc2_variance = jnp.clip(jnp.exp(math.log(40.0) - 3.6888795 * jax.random.uniform(arg_keys[21], (D, FF), jnp.float32) ** levels(arg_keys[21], (D, FF), ((0, 4), (1, 4)), -0.2, 0.2)), 1.0, 40.0)
    return dict(images_in=images_in, cotangent=cotangent, first_gain=first_gain, first_shift=first_shift, second_gain=second_gain, second_shift=second_shift, qkv_weight=qkv_weight, qv_bias=qv_bias, out_weight=out_weight, out_bias=out_bias, fc1_weight=fc1_weight, fc1_bias=fc1_bias, fc2_weight=fc2_weight, fc2_bias=fc2_bias, qkv_momentum=qkv_momentum, qkv_variance=qkv_variance, out_momentum=out_momentum, out_variance=out_variance, fc1_momentum=fc1_momentum, fc1_variance=fc1_variance, fc2_momentum=fc2_momentum, fc2_variance=fc2_variance)


NORM_EPS = 1e-06
LEARN_RATE = 0.02
BETA_FIRST = 0.9
BETA_SECOND = 0.999
ADAM_EPS = 1e-08
WEIGHT_DECAY = 0.05
ROOT_HALF = 0.7071067811865476
ROOT_TWO_PI = 2.5066282746310002

def norm_forward(values, norm_gain, norm_shift):
    middle = lax.optimization_barrier(jnp.mean(values, axis=-1, keepdims=True))
    square = lax.optimization_barrier(jnp.mean(values * values, axis=-1, keepdims=True))
    inverse = lax.rsqrt(square - middle * middle + NORM_EPS)
    normed = (values - middle) * inverse
    return (normed, inverse, (normed * norm_gain + norm_shift).astype(jnp.bfloat16))

def norm_backward(grad_out, normed, inverse, norm_gain):
    scaled = grad_out * norm_gain
    first_mean = lax.optimization_barrier(jnp.mean(scaled, axis=-1, keepdims=True))
    second_mean = lax.optimization_barrier(jnp.mean(scaled * normed, axis=-1, keepdims=True))
    return inverse * (scaled - first_mean - normed * second_mean)

def gelu_value(pre_act):
    return 0.5 * pre_act * (1.0 + jax.scipy.special.erf(pre_act * ROOT_HALF))

def gelu_slope(pre_act):
    return 0.5 * (1.0 + jax.scipy.special.erf(pre_act * ROOT_HALF)) + pre_act * jnp.exp(-0.5 * pre_act * pre_act) / ROOT_TWO_PI

def adam_step(weight, grad, momentum, variance):
    moment_new = BETA_FIRST * momentum + (1.0 - BETA_FIRST) * grad
    second_new = BETA_SECOND * variance + (1.0 - BETA_SECOND) * grad * grad
    corrected = moment_new / (1.0 - BETA_FIRST ** STEP)
    second_corrected = second_new / (1.0 - BETA_SECOND ** STEP)
    master = weight.astype(jnp.float32)
    updated = master - LEARN_RATE * (corrected / (jnp.sqrt(second_corrected) + ADAM_EPS) + WEIGHT_DECAY * master)
    return (updated, moment_new, second_new)

def reference(images_in, cotangent, first_gain, first_shift, second_gain, second_shift, qkv_weight, qv_bias, out_weight, out_bias, fc1_weight, fc1_bias, fc2_weight, fc2_bias, qkv_momentum, qkv_variance, out_momentum, out_variance, fc1_momentum, fc1_variance, fc2_momentum, fc2_variance):
    scale = HEAD_DIM ** (-0.5)
    qkv_flat = qkv_weight.reshape(D, 3 * D)
    qkv_shift = jnp.concatenate([qv_bias[0], jnp.zeros_like(qv_bias[0]), qv_bias[1]])

    def one_image(totals, inputs_pair):
        image_x, image_cot = inputs_pair
        source = image_x.astype(jnp.float32)
        normed1, inverse1, low1 = norm_forward(source, first_gain, first_shift)
        mixed_rows = (jnp.dot(low1, qkv_flat, preferred_element_type=jnp.float32) + qkv_shift).astype(jnp.bfloat16)
        mixed_rows = mixed_rows.reshape(SEQ, 3, HEADS, HEAD_DIM)
        queries = mixed_rows[:, 0].astype(jnp.float32)
        key_rows = mixed_rows[:, 1].astype(jnp.float32)
        value_rows = mixed_rows[:, 2].astype(jnp.float32)
        scores = jnp.einsum('qhe,khe->hqk', queries, key_rows) * scale
        row_peak = lax.optimization_barrier(jnp.max(scores, axis=2, keepdims=True))
        logsum = row_peak + jnp.log(lax.optimization_barrier(jnp.sum(jnp.exp(scores - row_peak), axis=2, keepdims=True)))
        soft_probs = jnp.exp(scores - logsum)
        probs_low = soft_probs.astype(jnp.bfloat16).astype(jnp.float32)
        attended = jnp.einsum('hqk,khe->qhe', probs_low, value_rows).astype(jnp.bfloat16).reshape(SEQ, D)
        hidden1 = source + jnp.dot(attended, out_weight.T, preferred_element_type=jnp.float32) + out_bias
        normed2, inverse2, low2 = norm_forward(hidden1, second_gain, second_shift)
        pre_act = jnp.dot(low2, fc1_weight, preferred_element_type=jnp.float32) + fc1_bias
        active = gelu_value(pre_act).astype(jnp.bfloat16)
        result = (hidden1 + jnp.dot(active, fc2_weight.T, preferred_element_type=jnp.float32) + fc2_bias).astype(jnp.bfloat16)
        grad_out = image_cot.astype(jnp.float32)
        fc2_grad = jnp.dot(image_cot.T, active, preferred_element_type=jnp.float32)
        grad_pre = jnp.dot(image_cot, fc2_weight, preferred_element_type=jnp.float32) * gelu_slope(pre_act)
        grad_pre_low = grad_pre.astype(jnp.bfloat16)
        fc1_grad = jnp.dot(low2.T, grad_pre_low, preferred_element_type=jnp.float32)
        grad_low2 = jnp.dot(grad_pre_low, fc1_weight.T, preferred_element_type=jnp.float32)
        grad_hidden = grad_out + norm_backward(grad_low2, normed2, inverse2, second_gain)
        grad_hidden_low = grad_hidden.astype(jnp.bfloat16)
        out_grad = jnp.dot(grad_hidden_low.T, attended, preferred_element_type=jnp.float32)
        grad_att = jnp.dot(grad_hidden_low, out_weight, preferred_element_type=jnp.float32).astype(jnp.bfloat16)
        grad_att = grad_att.reshape(SEQ, HEADS, HEAD_DIM).astype(jnp.float32)
        grad_values = jnp.einsum('hqk,qhe->khe', probs_low, grad_att)
        grad_probs = jnp.einsum('qhe,khe->hqk', grad_att, value_rows)
        row_delta = lax.optimization_barrier(jnp.sum(grad_att * attended.reshape(SEQ, HEADS, HEAD_DIM).astype(jnp.float32), axis=2))
        grad_scores = (soft_probs * (grad_probs - row_delta.T[:, :, None])).astype(jnp.bfloat16).astype(jnp.float32)
        grad_queries = jnp.einsum('hqk,khe->qhe', grad_scores, key_rows) * scale
        grad_keys = jnp.einsum('hqk,qhe->khe', grad_scores, queries) * scale
        grad_mixed = jnp.stack([grad_queries, grad_keys, grad_values], axis=1).reshape(SEQ, 3 * D).astype(jnp.bfloat16)
        qkv_grad = jnp.dot(low1.T, grad_mixed, preferred_element_type=jnp.float32)
        grad_low1 = jnp.dot(grad_mixed, qkv_flat.T, preferred_element_type=jnp.float32)
        grad_source = grad_hidden + norm_backward(grad_low1, normed1, inverse1, first_gain)
        bias_pair = jnp.stack([lax.optimization_barrier(jnp.sum(grad_queries, axis=0)).reshape(D), lax.optimization_barrier(jnp.sum(grad_values, axis=0)).reshape(D)])
        terms = (qkv_grad, out_grad, fc1_grad, fc2_grad, bias_pair, lax.optimization_barrier(jnp.sum(grad_hidden, axis=0)), lax.optimization_barrier(jnp.sum(grad_pre, axis=0)), lax.optimization_barrier(jnp.sum(grad_out, axis=0)), lax.optimization_barrier(jnp.sum(grad_low1 * normed1, axis=0)), lax.optimization_barrier(jnp.sum(grad_low1, axis=0)), lax.optimization_barrier(jnp.sum(grad_low2 * normed2, axis=0)), lax.optimization_barrier(jnp.sum(grad_low2, axis=0)))
        new_totals = tuple((before + added for before, added in zip(totals, terms)))
        return (new_totals, (result, grad_source))
    start = (jnp.zeros((D, 3 * D), jnp.float32), jnp.zeros((D, D), jnp.float32), jnp.zeros((D, FF), jnp.float32), jnp.zeros((D, FF), jnp.float32), jnp.zeros((2, D), jnp.float32), jnp.zeros((D,), jnp.float32), jnp.zeros((FF,), jnp.float32), jnp.zeros((D,), jnp.float32), jnp.zeros((D,), jnp.float32), jnp.zeros((D,), jnp.float32), jnp.zeros((D,), jnp.float32), jnp.zeros((D,), jnp.float32))
    totals, outputs = lax.scan(one_image, start, (images_in, cotangent))
    images_out, images_grad = outputs
    qkv_grad = totals[0].reshape(D, 3, D)
    qkv_new = adam_step(qkv_weight, qkv_grad, qkv_momentum, qkv_variance)
    out_new = adam_step(out_weight, totals[1], out_momentum, out_variance)
    fc1_new = adam_step(fc1_weight, totals[2], fc1_momentum, fc1_variance)
    fc2_new = adam_step(fc2_weight, totals[3], fc2_momentum, fc2_variance)
    return (images_out, images_grad, qkv_grad, totals[1], totals[2], totals[3], totals[4], totals[5], totals[6], totals[7], totals[8], totals[9], totals[10], totals[11], qkv_new[0], out_new[0], fc1_new[0], fc2_new[0], qkv_new[1], out_new[1], fc1_new[1], fc2_new[1], qkv_new[2], out_new[2], fc1_new[2], fc2_new[2])
```

```python
import functools

import jax
import jax.numpy as jnp
from jax import lax
from jax.experimental import pallas as pl
from jax.experimental.pallas import tpu as pltpu
from jax.sharding import PartitionSpec as P

HEAD_DIM = 64
STEP = 3


NORM_EPS = 1e-06
LEARN_RATE = 0.02
BETA_FIRST = 0.9
BETA_SECOND = 0.999
ADAM_EPS = 1e-08
WEIGHT_DECAY = 0.05
ROOT_HALF = 0.7071067811865476
ROOT_TWO_PI = 2.5066282746310002
LOG2E = 1.4426950408889634
ROW_TILE = 16
PLACE = (0, 2, 1, 3)
NT = (((1,), (1,)), ((), ()))
F32 = jnp.float32
BF16 = jnp.bfloat16


def swap(value, axis, distance):
    pairs = [(i, i ^ distance) for i in range(lax.axis_size(axis))]
    return lax.ppermute(value, axis, pairs)


def over_y(value):
    return swap(value, "col", 2)


def over_core(value):
    return swap(value, "col", 1)


def whole_width(own):
    pair = jnp.concatenate([own, over_y(own)], axis=1)
    return jnp.concatenate([pair, over_core(pair)], axis=1)


def rel_rows(weight, place):
    rows = weight.shape[0] // 4
    parts = [lax.dynamic_slice_in_dim(weight, (place ^ PLACE[p]) * rows, rows, 0) for p in range(4)]
    return jnp.concatenate(parts, axis=0)


def abs_rows(grad, place):
    rows = grad.shape[0] // 4
    parts = []
    for quarter in range(4):
        code = quarter ^ place
        at = (code & 1) * 2 + (code >> 1)
        parts.append(lax.dynamic_slice_in_dim(grad, at * rows, rows, 0))
    return jnp.concatenate(parts, axis=0)


def pair_sum(partial):
    half = partial.shape[1] // 2
    theirs = partial[:, half:].astype(BF16)
    return partial[:, :half] + over_core(theirs).astype(F32)


def all_sum(partial):
    pair = pair_sum(partial)
    quarter = pair.shape[1] // 2
    got = over_y(pair.astype(BF16)).astype(F32)
    total = pair + jnp.concatenate([got[:, quarter:], got[:, :quarter]], axis=1)
    other = over_core(total.astype(BF16)).astype(F32)
    return jnp.concatenate([total, other], axis=1)


def own_sum(partial):
    pair = pair_sum(partial)
    quarter = pair.shape[1] // 2
    return pair[:, :quarter] + over_y(pair[:, quarter:].astype(BF16)).astype(F32)


def col_sum(value):
    value = value + over_core(value)
    return value + over_y(value)


def norm_stats(values):
    middle = jnp.mean(values, axis=1, keepdims=True)
    square = jnp.mean(values * values, axis=1, keepdims=True)
    return middle, lax.rsqrt(square - middle * middle + NORM_EPS)


def gelu_value(pre_act):
    return 0.5 * pre_act * (1.0 + jax.scipy.special.erf(pre_act * ROOT_HALF))


def gelu_slope(pre_act):
    return (
        0.5 * (1.0 + jax.scipy.special.erf(pre_act * ROOT_HALF))
        + pre_act * jnp.exp(-0.5 * pre_act * pre_act) / ROOT_TWO_PI
    )


def attend_kernel(seq, heads, mixed_ref, att_ref, probs_ref):
    rows = mixed_ref.shape[0]
    width = heads * HEAD_DIM
    lane = lax.broadcasted_iota(jnp.int32, (1, width), 1)
    key_at = lax.broadcasted_iota(jnp.int32, (1, rows), 1)
    queries = mixed_ref[:, :width]
    key_rows = mixed_ref[:, width : 2 * width]
    value_rows = mixed_ref[:, 2 * width :]
    out = jnp.zeros((rows, width), F32)
    for head in range(heads):
        mask = (lane // HEAD_DIM) == head
        head_q = jnp.where(mask, queries, jnp.zeros_like(queries))
        scores = lax.dot_general(head_q, key_rows, NT, preferred_element_type=F32)
        scores = jnp.where(key_at < seq, scores, -1e30)
        peak = jnp.max(scores, axis=1, keepdims=True)
        powers = jnp.exp2((scores - peak) * (HEAD_DIM**-0.5 * LOG2E))
        total = jnp.sum(powers, axis=1, keepdims=True)
        probs_low = (powers * (1.0 / total)).astype(BF16)
        probs_ref[head] = probs_low
        part = jnp.dot(probs_low, value_rows, preferred_element_type=F32)
        out = jnp.where(mask, part, out)
    att_ref[...] = out.astype(BF16)


def attend(mixed, seq):
    rows, width3 = mixed.shape
    width = width3 // 3
    heads = width // HEAD_DIM
    return pl.pallas_call(
        functools.partial(attend_kernel, seq, heads),
        out_shape=(
            jax.ShapeDtypeStruct((rows, width), BF16),
            jax.ShapeDtypeStruct((heads, rows, rows), BF16),
        ),
        name="attend",
        compiler_params=pltpu.CompilerParams(vmem_limit_bytes=40 * 2**20),
        cost_estimate=pl.CostEstimate(
            flops=4 * rows * rows * width * heads,
            transcendentals=heads * rows * rows,
            bytes_accessed=2 * rows * (width3 + width + heads * rows),
        ),
    )(mixed)


def attend_back_kernel(heads, mixed_ref, att_ref, grad_ref, probs_ref, mixed_grad_ref, bias_ref, k_turned, v_turned):
    rows = mixed_ref.shape[0]
    width = heads * HEAD_DIM
    lane = lax.broadcasted_iota(jnp.int32, (1, width), 1)
    queries = mixed_ref[:, :width]
    key_rows = mixed_ref[:, width : 2 * width]
    value_rows = mixed_ref[:, 2 * width :]
    grad = grad_ref[...]
    down = lax.broadcasted_iota(jnp.int32, (width, width), 0)
    across = lax.broadcasted_iota(jnp.int32, (width, width), 1)
    eye = (down == across).astype(BF16)
    q_turned = lax.dot_general(eye, queries, NT, preferred_element_type=F32).astype(BF16)
    grad_turned = lax.dot_general(eye, grad, NT, preferred_element_type=F32).astype(BF16)
    product = grad.astype(F32) * att_ref[...].astype(F32)
    q_grad = jnp.zeros((rows, width), F32)
    scale = HEAD_DIM**-0.5
    for head in range(heads):
        mask = (lane // HEAD_DIM) == head
        span = slice(head * HEAD_DIM, (head + 1) * HEAD_DIM)
        head_grad = jnp.where(mask, grad, jnp.zeros_like(grad))
        grad_probs = lax.dot_general(head_grad, value_rows, NT, preferred_element_type=F32)
        delta = jnp.sum(jnp.where(mask, product, 0.0), axis=1, keepdims=True)
        probs_low = probs_ref[head]
        grad_scores = (probs_low.astype(F32) * (grad_probs - delta)).astype(BF16)
        part = jnp.dot(grad_scores, key_rows, preferred_element_type=F32)
        q_grad = jnp.where(mask, part, q_grad)
        k_turned[span, :] = jnp.dot(q_turned[span, :], grad_scores, preferred_element_type=F32)
        v_turned[span, :] = jnp.dot(grad_turned[span, :], probs_low, preferred_element_type=F32)
    q_grad = q_grad * scale
    v_grad = v_turned[...].T
    mixed_grad_ref[:, :width] = q_grad.astype(BF16)
    mixed_grad_ref[:, width : 2 * width] = (k_turned[...].T * scale).astype(BF16)
    mixed_grad_ref[:, 2 * width :] = v_grad.astype(BF16)
    bias_ref[0:1, :] = jnp.sum(q_grad, axis=0, keepdims=True)
    bias_ref[1:2, :] = jnp.sum(v_grad, axis=0, keepdims=True)


def attend_back(mixed, attended, grad_att, probs):
    rows, width3 = mixed.shape
    width = width3 // 3
    heads = width // HEAD_DIM
    return pl.pallas_call(
        functools.partial(attend_back_kernel, heads),
        out_shape=(
            jax.ShapeDtypeStruct((rows, width3), BF16),
            jax.ShapeDtypeStruct((2, width), F32),
        ),
        scratch_shapes=[pltpu.VMEM((width, rows), F32)] * 2,
        name="attend_back",
        compiler_params=pltpu.CompilerParams(vmem_limit_bytes=40 * 2**20),
        cost_estimate=pl.CostEstimate(
            flops=8 * rows * rows * width * heads,
            transcendentals=0,
            bytes_accessed=2 * rows * (2 * width3 + 2 * width + heads * rows),
        ),
    )(mixed, attended, grad_att, probs)


def adam_step(weight, grad, momentum, variance):
    moment_new = BETA_FIRST * momentum + (1.0 - BETA_FIRST) * grad
    second_new = BETA_SECOND * variance + (1.0 - BETA_SECOND) * grad * grad
    corrected = moment_new / (1.0 - BETA_FIRST**STEP)
    second_corrected = second_new / (1.0 - BETA_SECOND**STEP)
    master = weight.astype(jnp.float32)
    updated = master - LEARN_RATE * (
        corrected / (jnp.sqrt(second_corrected) + ADAM_EPS) + WEIGHT_DECAY * master
    )
    return (updated, moment_new, second_new)


def replica_sum(value):
    for axis in ("dp", "row"):
        size = lax.axis_size(axis)
        step = 1
        while step < size:
            value = value + swap(value, axis, step)
            step *= 2
    return value


def block_total(grad, place):
    block = lax.psum_scatter(abs_rows(grad.astype(BF16), place), "row", scatter_dimension=0, tiled=True)
    return block.astype(F32) + swap(block, "dp", 1).astype(F32)


def mm(left, right):
    return jnp.dot(left, right, preferred_element_type=F32)


def mm_nt(left, right):
    return lax.dot_general(left, right, NT, preferred_element_type=F32)


def mm_tn(left, right):
    return lax.dot_general(left, right, (((0,), (0,)), ((), ())), preferred_element_type=F32)


def per_device(
    images_in,
    cotangent,
    first_gain,
    first_shift,
    second_gain,
    second_shift,
    qkv_weight,
    qv_bias,
    out_weight,
    out_bias,
    fc1_weight,
    fc1_bias,
    fc2_weight,
    fc2_bias,
    qkv_momentum,
    qkv_variance,
    out_momentum,
    out_variance,
    fc1_momentum,
    fc1_variance,
    fc2_momentum,
    fc2_variance,
):
    image_count, seq, local = images_in.shape
    width = 4 * local
    rows = -(-seq // ROW_TILE) * ROW_TILE
    place = lax.axis_index("col")
    own_rows = qkv_weight.shape[0]

    def padded(value):
        return jnp.pad(value, ((0, rows - seq), (0, 0)))

    qkv_full = rel_rows(lax.all_gather(qkv_weight.reshape(own_rows, 3 * local), "row", axis=0, tiled=True), place)
    out_full = rel_rows(lax.all_gather(out_weight, "row", axis=0, tiled=True), place)
    fc1_full = rel_rows(lax.all_gather(fc1_weight, "row", axis=0, tiled=True), place)
    fc2_full = rel_rows(lax.all_gather(fc2_weight, "row", axis=0, tiled=True), place)
    vectors = whole_width(jnp.stack([first_gain, first_shift, second_gain, second_shift, out_bias]))
    gain1, shift1, gain2, shift2, bias_out = (vectors[i] for i in range(5))
    qkv_shift = jnp.concatenate([qv_bias[0], jnp.zeros_like(qv_bias[0]), qv_bias[1]])

    images = range(image_count)
    source = [whole_width(padded(images_in[i])) for i in images]
    cot = [whole_width(padded(cotangent[i])) for i in images]
    stats1 = [norm_stats(source[i].astype(F32)) for i in images]
    normed1 = [(source[i].astype(F32) - stats1[i][0]) * stats1[i][1] for i in images]
    low1 = [(normed1[i] * gain1 + shift1).astype(BF16) for i in images]
    mixed = [(mm(low1[i], qkv_full) + qkv_shift).astype(BF16) for i in images]
    attended, probs, hidden1 = [], [], []
    for i in images:
        att, prob = attend(mixed[i], seq)
        attended.append(att)
        probs.append(prob)
        hidden1.append(source[i].astype(F32) + all_sum(mm_nt(att, out_full)) + bias_out)
    normed2, inverse2, low2 = [], [], []
    for i in images:
        middle, inverse = norm_stats(hidden1[i])
        normed2.append((hidden1[i] - middle) * inverse)
        inverse2.append(inverse)
        low2.append((normed2[i] * gain2 + shift2).astype(BF16))
    out_rows, active, grad_pre, grad_pre_low, grad_low2 = [], [], [], [], []
    for i in images:
        pre_act = mm(low2[i], fc1_full) + fc1_bias
        active.append(gelu_value(pre_act).astype(BF16))
        grad_pre.append(mm(cot[i], fc2_full) * gelu_slope(pre_act))
        grad_pre_low.append(grad_pre[i].astype(BF16))
        grad_low2.append(all_sum(mm_nt(grad_pre_low[i], fc1_full)))
        moved = own_sum(mm_nt(active[i], fc2_full))
        out_rows.append((hidden1[i][:, :local] + moved + fc2_bias).astype(BF16)[:seq])
    fc2_grad = sum(mm_tn(cot[i], active[i]) for i in images)
    fc1_grad = sum(mm_tn(low2[i], grad_pre_low[i]) for i in images)
    grad_hidden, hidden_low, mixed_grad, bias_pair = [], [], [], []
    for i in images:
        scaled = grad_low2[i] * gain2
        first = jnp.mean(scaled, axis=1, keepdims=True)
        second = jnp.mean(scaled * normed2[i], axis=1, keepdims=True)
        grad_hidden.append(cot[i].astype(F32) + inverse2[i] * (scaled - first - normed2[i] * second))
        hidden_low.append(grad_hidden[i].astype(BF16))
        grad_att = mm(hidden_low[i], out_full).astype(BF16)
        grads, biases = attend_back(mixed[i], attended[i], grad_att, probs[i])
        mixed_grad.append(grads)
        bias_pair.append(biases)
    out_grad = sum(mm_tn(hidden_low[i], attended[i]) for i in images)
    qkv_grad = sum(mm_tn(low1[i], mixed_grad[i]) for i in images)
    images_grad, grad_low1 = [], []
    for i in images:
        partial = mm_nt(mixed_grad[i], qkv_full)
        scaled = partial * gain1
        sums = col_sum(jnp.stack([jnp.sum(scaled, axis=1), jnp.sum(scaled * normed1[i], axis=1)]))
        grad_low1.append(own_sum(partial))
        mine = grad_low1[i] * first_gain
        back = stats1[i][1] * (
            mine - (sums[0] / width)[:, None] - normed1[i][:, :local] * (sums[1] / width)[:, None]
        )
        images_grad.append((grad_hidden[i][:, :local] + back)[:seq])

    def token_sum(terms):
        return sum(jnp.sum(term, axis=0) for term in terms)

    small = jnp.concatenate(
        [
            sum(bias_pair).reshape(-1),
            token_sum([grad_hidden[i][:, :local] for i in images]),
            token_sum(grad_pre),
            token_sum([cot[i][:, :local].astype(F32) for i in images]),
            token_sum([grad_low1[i] * normed1[i][:, :local] for i in images]),
            token_sum(grad_low1),
            token_sum([grad_low2[i][:, :local] * normed2[i][:, :local] for i in images]),
            token_sum([grad_low2[i][:, :local] for i in images]),
        ]
    ).reshape(-1, 128)
    small = replica_sum(small).reshape(-1)
    sizes = [local, local, local, fc1_bias.shape[0], local, local, local, local, local]
    cuts, at = [], 0
    for size in sizes:
        cuts.append(small[at : at + size])
        at += size
    fc2_total = block_total(fc2_grad, place)
    fc1_total = block_total(fc1_grad, place)
    out_total = block_total(out_grad, place)
    qkv_total = block_total(qkv_grad, place).reshape(qkv_weight.shape)
    qkv_new = adam_step(qkv_weight, qkv_total, qkv_momentum, qkv_variance)
    out_new = adam_step(out_weight, out_total, out_momentum, out_variance)
    fc1_new = adam_step(fc1_weight, fc1_total, fc1_momentum, fc1_variance)
    fc2_new = adam_step(fc2_weight, fc2_total, fc2_momentum, fc2_variance)
    return (
        jnp.stack(out_rows),
        jnp.stack(images_grad),
        qkv_total,
        out_total,
        fc1_total,
        fc2_total,
        jnp.stack([cuts[0], cuts[1]]),
        cuts[2],
        cuts[3],
        cuts[4],
        cuts[5],
        cuts[6],
        cuts[7],
        cuts[8],
        qkv_new[0],
        out_new[0],
        fc1_new[0],
        fc2_new[0],
        qkv_new[1],
        out_new[1],
        fc1_new[1],
        fc2_new[1],
        qkv_new[2],
        out_new[2],
        fc1_new[2],
        fc2_new[2],
    )


def solution(mesh):
    return jax.shard_map(
        per_device,
        mesh=mesh,
        in_specs=(
            P(("dp", "row"), None, "col"),
            P(("dp", "row"), None, "col"),
            P("col"),
            P("col"),
            P("col"),
            P("col"),
            P("row", None, "col"),
            P(None, "col"),
            P("row", "col"),
            P("col"),
            P("row", "col"),
            P("col"),
            P("row", "col"),
            P("col"),
            P("row", None, "col"),
            P("row", None, "col"),
            P("row", "col"),
            P("row", "col"),
            P("row", "col"),
            P("row", "col"),
            P("row", "col"),
            P("row", "col"),
        ),
        out_specs=(
            P(("dp", "row"), None, "col"),
            P(("dp", "row"), None, "col"),
            P("row", None, "col"),
            P("row", "col"),
            P("row", "col"),
            P("row", "col"),
            P(None, "col"),
            P("col"),
            P("col"),
            P("col"),
            P("col"),
            P("col"),
            P("col"),
            P("col"),
            P("row", None, "col"),
            P("row", "col"),
            P("row", "col"),
            P("row", "col"),
            P("row", None, "col"),
            P("row", "col"),
            P("row", "col"),
            P("row", "col"),
            P("row", None, "col"),
            P("row", "col"),
            P("row", "col"),
            P("row", "col"),
        ),
        check_vma=False,
    )
```

```python
import functools

import jax
import jax.numpy as jnp
from jax import lax
from jax.experimental import pallas as pl
from jax.experimental.pallas import tpu as pltpu
from jax.sharding import PartitionSpec as P

HEAD_DIM = 64
STEP = 3


NORM_EPS = 1e-06
LEARN_RATE = 0.02
BETA_FIRST = 0.9
BETA_SECOND = 0.999
ADAM_EPS = 1e-08
WEIGHT_DECAY = 0.05
ROOT_HALF = 0.7071067811865476
ROOT_TWO_PI = 2.5066282746310002
LOG2E = 1.4426950408889634
ROW_TILE = 16
MESH = pl.DeviceIdType.MESH
NT = (((1,), (1,)), ((), ()))
F32 = jnp.float32
BF16 = jnp.bfloat16


def swap(value, axis, distance):
    pairs = [(i, i ^ distance) for i in range(lax.axis_size(axis))]
    return lax.ppermute(value, axis, pairs)


def over_y(value):
    return swap(value, "col", 2)


def over_core(value):
    return swap(value, "col", 1)


def whole_width(own):
    pair = jnp.concatenate([own, over_y(own)], axis=1)
    return jnp.concatenate([pair, over_core(pair)], axis=1)


def abs_rows(grad, place):
    rows = grad.shape[0] // 4
    parts = []
    for quarter in range(4):
        code = quarter ^ place
        at = (code & 1) * 2 + (code >> 1)
        parts.append(lax.dynamic_slice_in_dim(grad, at * rows, rows, 0))
    return jnp.concatenate(parts, axis=0)


def pair_sum(partial):
    half = partial.shape[1] // 2
    theirs = partial[:, half:].astype(BF16)
    return partial[:, :half] + over_core(theirs).astype(F32)


def all_sum(partial):
    pair = pair_sum(partial)
    quarter = pair.shape[1] // 2
    got = over_y(pair.astype(BF16)).astype(F32)
    total = pair + jnp.concatenate([got[:, quarter:], got[:, :quarter]], axis=1)
    other = over_core(total.astype(BF16)).astype(F32)
    return jnp.concatenate([total, other], axis=1)


def own_sum(partial):
    pair = pair_sum(partial)
    quarter = pair.shape[1] // 2
    return pair[:, :quarter] + over_y(pair[:, quarter:].astype(BF16)).astype(F32)


def col_sum(value):
    value = value + over_core(value)
    return value + over_y(value)


def norm_stats(values):
    middle = jnp.mean(values, axis=1, keepdims=True)
    square = jnp.mean(values * values, axis=1, keepdims=True)
    return middle, lax.rsqrt(square - middle * middle + NORM_EPS)


def gelu_value(pre_act):
    return 0.5 * pre_act * (1.0 + jax.scipy.special.erf(pre_act * ROOT_HALF))


def gelu_slope(pre_act):
    return (
        0.5 * (1.0 + jax.scipy.special.erf(pre_act * ROOT_HALF))
        + pre_act * jnp.exp(-0.5 * pre_act * pre_act) / ROOT_TWO_PI
    )


def copy_to(src, dst, send, recv, where):
    return pltpu.make_async_remote_copy(
        src_ref=src, dst_ref=dst, send_sem=send, recv_sem=recv, device_id=where, device_id_type=MESH
    )


def rel_place(quarter, place):
    return (quarter // 2 + place // 2) % 2 + 2 * ((quarter % 2 + place % 2) % 2)


def front_kernel(
    sizes,
    images_ref, cot_ref, qkv_ref, out_ref, fc1_ref, fc2_ref, gain_ref, shift_ref, qkv_bias_ref,
    source_out, cot_out, low_out, mixed_out, probs_out, att_out, total_out, qkv_out, outw_out, fc1_out, fc2_out,
    source, cot, low, mixed, probs, att, theirs, given, mine, pair, pair_in, total, qkv_full, out_full, fc1_full, fc2_full,
    row_send, row_recv, dp_send, dp_recv, own_sem, in_send, in_recv, sum_send, sum_recv, out_sem,
):
    count, seq, rows, local, row_count = sizes
    dp, row, place = lax.axis_index("dp"), lax.axis_index("row"), lax.axis_index("col")
    core_at = {"col": place + 1 - 2 * (place % 2)}
    y_at = {"col": (place + 2) % 4}
    dp_at = {"dp": 1 - dp}
    barrier = pltpu.get_barrier_semaphore()
    partners = [core_at, y_at, dp_at] + [{"row": (row + d) % row_count} for d in range(1, row_count)]
    for partner in partners:
        pl.semaphore_signal(barrier, inc=1, device_id=partner, device_id_type=MESH)
    pl.semaphore_wait(barrier, len(partners))

    block = qkv_ref.shape[0]
    per = row_count // 4

    def rows_of(owner):
        at = (rel_place(owner // per, place) * per + owner % per) * block
        return pl.ds(pl.multiple_of(at, block), block)

    weights = ((qkv_ref, qkv_full), (out_ref, out_full), (fc1_ref, fc1_full), (fc2_ref, fc2_full))

    def half_of(full):
        half = full.shape[1] // 2
        return pl.ds(pl.multiple_of(dp * half, half), half)

    def row_copy(w, d):
        ref, full = weights[w]
        cols = half_of(full)
        return copy_to(
            ref.at[:, cols], full.at[rows_of(row), cols], row_send.at[w, d], row_recv.at[w, d], {"row": (row + d) % row_count}
        )

    def dp_copy(w, d):
        _, full = weights[w]
        part = full.at[rows_of((row + row_count - d) % row_count), half_of(full)]
        return copy_to(part, part, dp_send.at[w, d], dp_recv.at[w, d], dp_at)

    def own_copy(w):
        ref, full = weights[w]
        return pltpu.make_async_copy(ref, full.at[rows_of(row), :], own_sem.at[w])

    inputs = ((images_ref, source), (cot_ref, cot))

    def y_copy(a, i):
        ref, full = inputs[a]
        return copy_to(ref.at[i], full.at[i, :, pl.ds(local, local)], in_send.at[a, 0, i], in_recv.at[a, 0, i], y_at)

    def core_copy(a, i):
        ref, full = inputs[a]
        return copy_to(ref.at[i], full.at[i, :, pl.ds(2 * local, local)], in_send.at[a, 1, i], in_recv.at[a, 1, i], core_at)

    def hand_copy(a, i):
        _, full = inputs[a]
        return copy_to(
            full.at[i, :, pl.ds(local, local)],
            full.at[i, :, pl.ds(3 * local, local)],
            in_send.at[a, 2, i],
            in_recv.at[a, 2, i],
            core_at,
        )

    def here_copy(a, i):
        ref, full = inputs[a]
        return pltpu.make_async_copy(ref.at[i], full.at[i, :, pl.ds(0, local)], in_send.at[a, 3, i])

    def given_copy(i):
        return copy_to(theirs.at[i], given.at[i], sum_send.at[0, i], sum_recv.at[0, i], core_at)

    def pair_copy(i):
        return copy_to(pair.at[i], pair_in.at[i], sum_send.at[1, i], sum_recv.at[1, i], y_at)

    def total_copy(i):
        return copy_to(
            total.at[i, :, pl.ds(0, 2 * local)],
            total.at[i, :, pl.ds(2 * local, 2 * local)],
            sum_send.at[2, i],
            sum_recv.at[2, i],
            core_at,
        )

    for w in range(4):
        for d in range(1, row_count):
            row_copy(w, d).start()
        own_copy(w).start()
    for a in range(2):
        for i in range(count):
            y_copy(a, i).start()
            core_copy(a, i).start()
            here_copy(a, i).start()

    def forward(w):
        for d in range(1, row_count):
            row_copy(w, d).wait_recv()
            dp_copy(w, d).start()

    def arrived(w):
        for d in range(1, row_count):
            dp_copy(w, d).wait_recv()
        own_copy(w).wait()

    forward(0)
    y_copy(0, 0).wait_recv()
    hand_copy(0, 0).start()
    forward(1)
    arrived(0)
    arrived(1)

    width = 4 * local
    lane = lax.broadcasted_iota(jnp.int32, (1, 2 * HEAD_DIM), 1)
    key_at = lax.broadcasted_iota(jnp.int32, (1, rows), 1)
    pairs = local // (2 * HEAD_DIM)

    @pl.loop(0, count)
    def _(i):
        @pl.when(i > 0)
        def _():
            y_copy(0, i).wait_recv()
            hand_copy(0, i).start()

        here_copy(0, i).wait()
        core_copy(0, i).wait_recv()
        hand_copy(0, i).wait_recv()
        values = source[i].astype(F32)
        middle = jnp.sum(values, axis=1, keepdims=True) / width
        square = jnp.sum(values * values, axis=1, keepdims=True) / width
        inverse = lax.rsqrt(square - middle * middle + NORM_EPS)
        low[i] = ((values - middle) * inverse * gain_ref[...] + shift_ref[...]).astype(BF16)
        mixed[i] = (jnp.dot(low[i], qkv_full[...], preferred_element_type=F32) + qkv_bias_ref[...]).astype(BF16)
        for pair_at in range(pairs):
            base = pair_at * 6 * HEAD_DIM
            queries = mixed[i, :, base : base + 2 * HEAD_DIM]
            key_rows = mixed[i, :, base + 2 * HEAD_DIM : base + 4 * HEAD_DIM]
            value_rows = mixed[i, :, base + 4 * HEAD_DIM : base + 6 * HEAD_DIM]
            parts = []
            for side in range(2):
                mask = (lane // HEAD_DIM) == side
                head_q = jnp.where(mask, queries, jnp.zeros_like(queries))
                scores = lax.dot_general(head_q, key_rows, NT, preferred_element_type=F32)
                scores = jnp.where(key_at < seq, scores, -1e30)
                peak = jnp.max(scores, axis=1, keepdims=True)
                powers = jnp.exp2((scores - peak) * (HEAD_DIM**-0.5 * LOG2E))
                share = 1.0 / jnp.sum(powers, axis=1, keepdims=True)
                probs_low = (powers * share).astype(BF16)
                probs[i, 2 * pair_at + side] = probs_low
                parts.append(jnp.dot(probs_low, value_rows, preferred_element_type=F32))
            joined = jnp.where((lane // HEAD_DIM) == 0, parts[0], parts[1])
            att[i, :, 2 * HEAD_DIM * pair_at : 2 * HEAD_DIM * (pair_at + 1)] = joined.astype(BF16)
        attended = att[i]
        theirs[i] = lax.dot_general(attended, out_full[2 * local :, :], NT, preferred_element_type=F32).astype(BF16)
        given_copy(i).start()
        mine[...] = lax.dot_general(attended, out_full[: 2 * local, :], NT, preferred_element_type=F32)
        given_copy(i).wait_recv()
        pair[i] = (mine[...] + given[i].astype(F32)).astype(BF16)
        pair_copy(i).start()

    outs = (
        (source, source_out), (low, low_out), (mixed, mixed_out), (probs, probs_out), (att, att_out),
        (qkv_full, qkv_out), (out_full, outw_out),
    )
    for k, (here, there) in enumerate(outs):
        pltpu.make_async_copy(here, there, out_sem.at[k]).start()
    forward(2)
    forward(3)
    for i in range(count):
        y_copy(1, i).wait_recv()
        hand_copy(1, i).start()

    @pl.loop(0, count)
    def _(i):
        pair_copy(i).wait_recv()
        total[i, :, : local] = (pair[i, :, : local].astype(F32) + pair_in[i, :, local:].astype(F32)).astype(BF16)
        total[i, :, local : 2 * local] = (
            pair[i, :, local:].astype(F32) + pair_in[i, :, : local].astype(F32)
        ).astype(BF16)
        total_copy(i).start()

    arrived(2)
    arrived(3)
    for i in range(count):
        here_copy(1, i).wait()
        core_copy(1, i).wait_recv()
        hand_copy(1, i).wait_recv()
    later = ((fc1_full, fc1_out), (fc2_full, fc2_out), (cot, cot_out))
    for k, (here, there) in enumerate(later):
        pltpu.make_async_copy(here, there, out_sem.at[len(outs) + k]).start()
    for i in range(count):
        total_copy(i).wait_recv()
    last = len(outs) + len(later)
    pltpu.make_async_copy(total, total_out, out_sem.at[last]).start()
    for w in range(4):
        for d in range(1, row_count):
            row_copy(w, d).wait_send()
            dp_copy(w, d).wait_send()
    for i in range(count):
        for a in range(2):
            y_copy(a, i).wait_send()
            core_copy(a, i).wait_send()
            hand_copy(a, i).wait_send()
        given_copy(i).wait_send()
        pair_copy(i).wait_send()
        total_copy(i).wait_send()
    for k, (here, there) in enumerate((*outs, *later, (total, total_out))):
        pltpu.make_async_copy(here, there, out_sem.at[k]).wait()


def front(images, cotangent, qkv_block, out_block, fc1_block, fc2_block, gain, shift, qkv_bias, seq):
    count, rows, local = images.shape
    row_count = lax.axis_size("row")
    width = 4 * local
    heads = local // HEAD_DIM
    hidden = fc1_block.shape[1]
    qkv_width = qkv_block.shape[1]

    def wide(*shape):
        return shape, BF16

    outs = [
        wide(count, rows, width), wide(count, rows, width), wide(count, rows, width), wide(count, rows, qkv_width),
        wide(count, heads, rows, rows), wide(count, rows, local), wide(count, rows, width),
        wide(width, qkv_width), wide(width, local), wide(width, hidden), wide(width, hidden),
    ]
    scratch = [
        wide(count, rows, width), wide(count, rows, width), wide(count, rows, width), wide(count, rows, qkv_width),
        wide(count, heads, rows, rows), wide(count, rows, local),
        wide(count, rows, 2 * local), wide(count, rows, 2 * local), ((rows, 2 * local), F32),
        wide(count, rows, 2 * local), wide(count, rows, 2 * local), wide(count, rows, width),
        wide(width, qkv_width), wide(width, local), wide(width, hidden), wide(width, hidden),
    ]
    dma = pltpu.SemaphoreType.DMA
    whole = pl.BlockSpec(memory_space=pl.ANY)
    vmem = pl.BlockSpec(memory_space=pltpu.VMEM)
    return pl.pallas_call(
        functools.partial(front_kernel, (count, seq, rows, local, row_count)),
        out_shape=[jax.ShapeDtypeStruct(*s) for s in outs],
        in_specs=[whole] * 6 + [vmem] * 3,
        out_specs=[whole] * len(outs),
        scratch_shapes=[pltpu.VMEM(*s) for s in scratch]
        + [dma((4, row_count))] * 4
        + [dma((4,)), dma((2, 4, count)), dma((2, 3, count)), dma((3, count)), dma((3, count)), dma((11,))],
        name="front",
        compiler_params=pltpu.CompilerParams(
            vmem_limit_bytes=62 * 2**20, collective_id=0, has_side_effects=True
        ),
    )(images, cotangent, qkv_block, out_block, fc1_block, fc2_block, gain, shift, qkv_bias)


def attend_back_kernel(heads, mixed_ref, att_ref, grad_ref, probs_ref, mixed_grad_ref, bias_ref, k_turned, v_turned):
    rows = mixed_ref.shape[0]
    two = 2 * HEAD_DIM
    lane = lax.broadcasted_iota(jnp.int32, (1, two), 1)
    down = lax.broadcasted_iota(jnp.int32, (two, two), 0)
    across = lax.broadcasted_iota(jnp.int32, (two, two), 1)
    eye = (down == across).astype(BF16)
    scale = HEAD_DIM**-0.5
    for pair in range(heads // 2):
        base = pair * 3 * two
        queries = mixed_ref[:, base : base + two]
        key_rows = mixed_ref[:, base + two : base + 2 * two]
        value_rows = mixed_ref[:, base + 2 * two : base + 3 * two]
        grad = grad_ref[:, pair * two : (pair + 1) * two]
        q_turned = lax.dot_general(eye, queries, NT, preferred_element_type=F32).astype(BF16)
        grad_turned = lax.dot_general(eye, grad, NT, preferred_element_type=F32).astype(BF16)
        product = grad.astype(F32) * att_ref[:, pair * two : (pair + 1) * two].astype(F32)
        parts = []
        for side in range(2):
            mask = (lane // HEAD_DIM) == side
            span = slice(side * HEAD_DIM, (side + 1) * HEAD_DIM)
            head_grad = jnp.where(mask, grad, jnp.zeros_like(grad))
            grad_probs = lax.dot_general(head_grad, value_rows, NT, preferred_element_type=F32)
            delta = jnp.sum(jnp.where(mask, product, 0.0), axis=1, keepdims=True)
            probs_low = probs_ref[2 * pair + side]
            grad_scores = (probs_low.astype(F32) * (grad_probs - delta)).astype(BF16)
            parts.append(jnp.dot(grad_scores, key_rows, preferred_element_type=F32))
            k_turned[span, :] = jnp.dot(q_turned[span, :], grad_scores, preferred_element_type=F32)
            v_turned[span, :] = jnp.dot(grad_turned[span, :], probs_low, preferred_element_type=F32)
        q_grad = jnp.where((lane // HEAD_DIM) == 0, parts[0], parts[1]) * scale
        v_grad = v_turned[...].T
        mixed_grad_ref[:, base : base + two] = q_grad.astype(BF16)
        mixed_grad_ref[:, base + two : base + 2 * two] = (k_turned[...].T * scale).astype(BF16)
        mixed_grad_ref[:, base + 2 * two : base + 3 * two] = v_grad.astype(BF16)
        bias_ref[0:1, pair * two : (pair + 1) * two] = jnp.sum(q_grad, axis=0, keepdims=True)
        bias_ref[1:2, pair * two : (pair + 1) * two] = jnp.sum(v_grad, axis=0, keepdims=True)


def attend_back(mixed, attended, grad_att, probs):
    rows, width3 = mixed.shape
    width = width3 // 3
    heads = width // HEAD_DIM
    return pl.pallas_call(
        functools.partial(attend_back_kernel, heads),
        out_shape=(
            jax.ShapeDtypeStruct((rows, width3), BF16),
            jax.ShapeDtypeStruct((2, width), F32),
        ),
        scratch_shapes=[pltpu.VMEM((2 * HEAD_DIM, rows), F32)] * 2,
        name="attend_back",
        compiler_params=pltpu.CompilerParams(vmem_limit_bytes=40 * 2**20),
        cost_estimate=pl.CostEstimate(
            flops=8 * rows * rows * width * heads,
            transcendentals=0,
            bytes_accessed=2 * rows * (2 * width3 + 2 * width + heads * rows),
        ),
    )(mixed, attended, grad_att, probs)


def adam_step(weight, grad, momentum, variance):
    moment_new = BETA_FIRST * momentum + (1.0 - BETA_FIRST) * grad
    second_new = BETA_SECOND * variance + (1.0 - BETA_SECOND) * grad * grad
    corrected = moment_new / (1.0 - BETA_FIRST**STEP)
    second_corrected = second_new / (1.0 - BETA_SECOND**STEP)
    master = weight.astype(jnp.float32)
    updated = master - LEARN_RATE * (
        corrected / (jnp.sqrt(second_corrected) + ADAM_EPS) + WEIGHT_DECAY * master
    )
    return (updated, moment_new, second_new)


def replica_sum(value):
    for axis in ("dp", "row"):
        size = lax.axis_size(axis)
        step = 1
        while step < size:
            value = value + swap(value, axis, step)
            step *= 2
    return value


def block_total(grad, place):
    block = lax.psum_scatter(abs_rows(grad.astype(BF16), place), "row", scatter_dimension=0, tiled=True)
    return block.astype(F32) + swap(block, "dp", 1).astype(F32)


def mm(left, right):
    return jnp.dot(left, right, preferred_element_type=F32)


def mm_nt(left, right):
    return lax.dot_general(left, right, NT, preferred_element_type=F32)


def mm_tn(left, right):
    return lax.dot_general(left, right, (((0,), (0,)), ((), ())), preferred_element_type=F32)


def per_device(
    images_in,
    cotangent,
    first_gain,
    first_shift,
    second_gain,
    second_shift,
    qkv_weight,
    qv_bias,
    out_weight,
    out_bias,
    fc1_weight,
    fc1_bias,
    fc2_weight,
    fc2_bias,
    qkv_momentum,
    qkv_variance,
    out_momentum,
    out_variance,
    fc1_momentum,
    fc1_variance,
    fc2_momentum,
    fc2_variance,
):
    image_count, seq, local = images_in.shape
    width = 4 * local
    rows = -(-seq // ROW_TILE) * ROW_TILE
    place = lax.axis_index("col")

    def paired(value):
        lead = value.shape[:-2]
        value = value.reshape(*lead, 3, local // 128, 128)
        return jnp.swapaxes(value, -3, -2).reshape(*lead, 3 * local)

    def unpaired(value):
        value = value.reshape(value.shape[0], local // 128, 3, 128)
        return jnp.swapaxes(value, 1, 2).reshape(value.shape[0], 3, local)

    vectors = whole_width(jnp.stack([first_gain, first_shift, second_gain, second_shift, out_bias]))
    gain1, shift1, gain2, shift2, bias_out = (vectors[i] for i in range(5))
    qkv_shift = paired(jnp.stack([qv_bias[0], jnp.zeros_like(qv_bias[0]), qv_bias[1]]))
    images = range(image_count)
    (source_all, cot_all, low_all, mixed_all, probs_all, att_all, total_all, qkv_full, out_full, fc1_full, fc2_full) = front(
        jnp.pad(images_in, ((0, 0), (0, rows - seq), (0, 0))),
        jnp.pad(cotangent, ((0, 0), (0, rows - seq), (0, 0))),
        paired(qkv_weight),
        out_weight,
        fc1_weight,
        fc2_weight,
        gain1[None],
        shift1[None],
        qkv_shift[None],
        seq,
    )
    source = [source_all[i] for i in images]
    cot = [cot_all[i] for i in images]
    low1 = [low_all[i] for i in images]
    mixed = [mixed_all[i] for i in images]
    attended = [att_all[i] for i in images]
    probs = [probs_all[i] for i in images]
    hidden1 = [source[i].astype(F32) + total_all[i].astype(F32) + bias_out for i in images]
    stats1 = [norm_stats(source[i].astype(F32)) for i in images]
    normed1 = [(source[i].astype(F32) - stats1[i][0]) * stats1[i][1] for i in images]
    normed2, inverse2, low2 = [], [], []
    for i in images:
        middle, inverse = norm_stats(hidden1[i])
        normed2.append((hidden1[i] - middle) * inverse)
        inverse2.append(inverse)
        low2.append((normed2[i] * gain2 + shift2).astype(BF16))
    out_rows, active, grad_pre, grad_pre_low, grad_low2 = [], [], [], [], []
    for i in images:
        pre_act = mm(low2[i], fc1_full) + fc1_bias
        active.append(gelu_value(pre_act).astype(BF16))
        grad_pre.append(mm(cot[i], fc2_full) * gelu_slope(pre_act))
        grad_pre_low.append(grad_pre[i].astype(BF16))
        grad_low2.append(all_sum(mm_nt(grad_pre_low[i], fc1_full)))
        moved = own_sum(mm_nt(active[i], fc2_full))
        out_rows.append((hidden1[i][:, :local] + moved + fc2_bias).astype(BF16)[:seq])
    fc2_grad = sum(mm_tn(cot[i], active[i]) for i in images)
    fc1_grad = sum(mm_tn(low2[i], grad_pre_low[i]) for i in images)
    grad_hidden, hidden_low, mixed_grad, bias_pair = [], [], [], []
    for i in images:
        scaled = grad_low2[i] * gain2
        first = jnp.mean(scaled, axis=1, keepdims=True)
        second = jnp.mean(scaled * normed2[i], axis=1, keepdims=True)
        grad_hidden.append(cot[i].astype(F32) + inverse2[i] * (scaled - first - normed2[i] * second))
        hidden_low.append(grad_hidden[i].astype(BF16))
        grad_att = mm(hidden_low[i], out_full).astype(BF16)
        grads, biases = attend_back(mixed[i], attended[i], grad_att, probs[i])
        mixed_grad.append(grads)
        bias_pair.append(biases)
    out_grad = sum(mm_tn(hidden_low[i], attended[i]) for i in images)
    qkv_grad = sum(mm_tn(low1[i], mixed_grad[i]) for i in images)
    images_grad, grad_low1 = [], []
    for i in images:
        partial = mm_nt(mixed_grad[i], qkv_full)
        scaled = partial * gain1
        sums = col_sum(jnp.stack([jnp.sum(scaled, axis=1), jnp.sum(scaled * normed1[i], axis=1)]))
        grad_low1.append(own_sum(partial))
        mine = grad_low1[i] * first_gain
        back = stats1[i][1] * (
            mine - (sums[0] / width)[:, None] - normed1[i][:, :local] * (sums[1] / width)[:, None]
        )
        images_grad.append((grad_hidden[i][:, :local] + back)[:seq])

    def token_sum(terms):
        return sum(jnp.sum(term, axis=0) for term in terms)

    small = jnp.concatenate(
        [
            sum(bias_pair).reshape(-1),
            token_sum([grad_hidden[i][:, :local] for i in images]),
            token_sum(grad_pre),
            token_sum([cot[i][:, :local].astype(F32) for i in images]),
            token_sum([grad_low1[i] * normed1[i][:, :local] for i in images]),
            token_sum(grad_low1),
            token_sum([grad_low2[i][:, :local] * normed2[i][:, :local] for i in images]),
            token_sum([grad_low2[i][:, :local] for i in images]),
        ]
    ).reshape(-1, 128)
    small = replica_sum(small).reshape(-1)
    sizes = [local, local, local, fc1_bias.shape[0], local, local, local, local, local]
    cuts, at = [], 0
    for size in sizes:
        cuts.append(small[at : at + size])
        at += size
    fc2_total = block_total(fc2_grad, place)
    fc1_total = block_total(fc1_grad, place)
    out_total = block_total(out_grad, place)
    qkv_total = unpaired(block_total(qkv_grad, place))
    qkv_new = adam_step(qkv_weight, qkv_total, qkv_momentum, qkv_variance)
    out_new = adam_step(out_weight, out_total, out_momentum, out_variance)
    fc1_new = adam_step(fc1_weight, fc1_total, fc1_momentum, fc1_variance)
    fc2_new = adam_step(fc2_weight, fc2_total, fc2_momentum, fc2_variance)
    return (
        jnp.stack(out_rows),
        jnp.stack(images_grad),
        qkv_total,
        out_total,
        fc1_total,
        fc2_total,
        jnp.stack([cuts[0], cuts[1]]),
        cuts[2],
        cuts[3],
        cuts[4],
        cuts[5],
        cuts[6],
        cuts[7],
        cuts[8],
        qkv_new[0],
        out_new[0],
        fc1_new[0],
        fc2_new[0],
        qkv_new[1],
        out_new[1],
        fc1_new[1],
        fc2_new[1],
        qkv_new[2],
        out_new[2],
        fc1_new[2],
        fc2_new[2],
    )


def solution(mesh):
    return jax.shard_map(
        per_device,
        mesh=mesh,
        in_specs=(
            P(("dp", "row"), None, "col"),
            P(("dp", "row"), None, "col"),
            P("col"),
            P("col"),
            P("col"),
            P("col"),
            P("row", None, "col"),
            P(None, "col"),
            P("row", "col"),
            P("col"),
            P("row", "col"),
            P("col"),
            P("row", "col"),
            P("col"),
            P("row", None, "col"),
            P("row", None, "col"),
            P("row", "col"),
            P("row", "col"),
            P("row", "col"),
            P("row", "col"),
            P("row", "col"),
            P("row", "col"),
        ),
        out_specs=(
            P(("dp", "row"), None, "col"),
            P(("dp", "row"), None, "col"),
            P("row", None, "col"),
            P("row", "col"),
            P("row", "col"),
            P("row", "col"),
            P(None, "col"),
            P("col"),
            P("col"),
            P("col"),
            P("col"),
            P("col"),
            P("col"),
            P("col"),
            P("row", None, "col"),
            P("row", "col"),
            P("row", "col"),
            P("row", "col"),
            P("row", None, "col"),
            P("row", "col"),
            P("row", "col"),
            P("row", "col"),
            P("row", None, "col"),
            P("row", "col"),
            P("row", "col"),
            P("row", "col"),
        ),
        check_vma=False,
    )
```

```python
import functools

import jax
import jax.numpy as jnp
from jax import lax
from jax.experimental import pallas as pl
from jax.experimental.pallas import tpu as pltpu
from jax.sharding import PartitionSpec as P

HEAD_DIM = 64
STEP = 3


NORM_EPS = 1e-06
LEARN_RATE = 0.02
BETA_FIRST = 0.9
BETA_SECOND = 0.999
ADAM_EPS = 1e-08
WEIGHT_DECAY = 0.05
ROOT_HALF = 0.7071067811865476
ROOT_TWO_PI = 2.5066282746310002
LOG2E = 1.4426950408889634
ROW_TILE = 16
MESH = pl.DeviceIdType.MESH
NT = (((1,), (1,)), ((), ()))
TN = (((0,), (0,)), ((), ()))
F32 = jnp.float32
BF16 = jnp.bfloat16


def swap(value, axis, distance):
    pairs = [(i, i ^ distance) for i in range(lax.axis_size(axis))]
    return lax.ppermute(value, axis, pairs)


def over_y(value):
    return swap(value, "col", 2)


def over_core(value):
    return swap(value, "col", 1)


def whole_width(own):
    pair = jnp.concatenate([own, over_y(own)], axis=1)
    return jnp.concatenate([pair, over_core(pair)], axis=1)


def copy_to(src, dst, send, recv, where):
    return pltpu.make_async_remote_copy(
        src_ref=src, dst_ref=dst, send_sem=send, recv_sem=recv, device_id=where, device_id_type=MESH
    )


def rel_place(quarter, place):
    return (quarter // 2 + place // 2) % 2 + 2 * ((quarter % 2 + place % 2) % 2)


def front_kernel(
    sizes,
    images_ref, cot_ref, qkv_ref, out_ref, fc1_ref, fc2_ref, gain_ref, shift_ref, qkv_bias_ref,
    source_out, cot_out, low_out, mixed_out, probs_out, att_out, total_out, qkv_out, outw_out, fc1_out, fc2_out,
    source, cot, low, mixed, probs, att, theirs, given, mine, pair, pair_in, total, qkv_full, out_full, fc1_full, fc2_full,
    row_send, row_recv, dp_send, dp_recv, own_sem, in_send, in_recv, sum_send, sum_recv, out_sem,
):
    count, seq, rows, local, row_count = sizes
    dp, row, place = lax.axis_index("dp"), lax.axis_index("row"), lax.axis_index("col")
    core_at = {"col": place + 1 - 2 * (place % 2)}
    y_at = {"col": (place + 2) % 4}
    dp_at = {"dp": 1 - dp}
    barrier = pltpu.get_barrier_semaphore()
    partners = [core_at, y_at, dp_at] + [{"row": (row + d) % row_count} for d in range(1, row_count)]
    for partner in partners:
        pl.semaphore_signal(barrier, inc=1, device_id=partner, device_id_type=MESH)
    pl.semaphore_wait(barrier, len(partners))

    block = qkv_ref.shape[0]
    per = row_count // 4

    def rows_of(owner):
        at = (rel_place(owner // per, place) * per + owner % per) * block
        return pl.ds(pl.multiple_of(at, block), block)

    weights = ((qkv_ref, qkv_full), (out_ref, out_full), (fc1_ref, fc1_full), (fc2_ref, fc2_full))

    def half_of(full):
        half = full.shape[1] // 2
        return pl.ds(pl.multiple_of(dp * half, half), half)

    def row_copy(w, d):
        ref, full = weights[w]
        cols = half_of(full)
        return copy_to(
            ref.at[:, cols], full.at[rows_of(row), cols], row_send.at[w, d], row_recv.at[w, d], {"row": (row + d) % row_count}
        )

    def dp_copy(w, d):
        _, full = weights[w]
        part = full.at[rows_of((row + row_count - d) % row_count), half_of(full)]
        return copy_to(part, part, dp_send.at[w, d], dp_recv.at[w, d], dp_at)

    def own_copy(w):
        ref, full = weights[w]
        return pltpu.make_async_copy(ref, full.at[rows_of(row), :], own_sem.at[w])

    inputs = ((images_ref, source), (cot_ref, cot))

    def y_copy(a, i):
        ref, full = inputs[a]
        return copy_to(ref.at[i], full.at[i, :, pl.ds(local, local)], in_send.at[a, 0, i], in_recv.at[a, 0, i], y_at)

    def core_copy(a, i):
        ref, full = inputs[a]
        return copy_to(ref.at[i], full.at[i, :, pl.ds(2 * local, local)], in_send.at[a, 1, i], in_recv.at[a, 1, i], core_at)

    def hand_copy(a, i):
        _, full = inputs[a]
        return copy_to(
            full.at[i, :, pl.ds(local, local)],
            full.at[i, :, pl.ds(3 * local, local)],
            in_send.at[a, 2, i],
            in_recv.at[a, 2, i],
            core_at,
        )

    def here_copy(a, i):
        ref, full = inputs[a]
        return pltpu.make_async_copy(ref.at[i], full.at[i, :, pl.ds(0, local)], in_send.at[a, 3, i])

    def given_copy(i):
        return copy_to(theirs.at[i], given.at[i], sum_send.at[0, i], sum_recv.at[0, i], core_at)

    def pair_copy(i):
        return copy_to(pair.at[i], pair_in.at[i], sum_send.at[1, i], sum_recv.at[1, i], y_at)

    def total_copy(i):
        return copy_to(
            total.at[i, :, pl.ds(0, 2 * local)],
            total.at[i, :, pl.ds(2 * local, 2 * local)],
            sum_send.at[2, i],
            sum_recv.at[2, i],
            core_at,
        )

    for w in range(4):
        for d in range(1, row_count):
            row_copy(w, d).start()
        own_copy(w).start()
    for a in range(2):
        for i in range(count):
            y_copy(a, i).start()
            core_copy(a, i).start()
            here_copy(a, i).start()

    def forward(w):
        for d in range(1, row_count):
            row_copy(w, d).wait_recv()
            dp_copy(w, d).start()

    def arrived(w):
        for d in range(1, row_count):
            dp_copy(w, d).wait_recv()
        own_copy(w).wait()

    forward(0)
    y_copy(0, 0).wait_recv()
    hand_copy(0, 0).start()
    forward(1)
    arrived(0)
    arrived(1)

    width = 4 * local
    lane = lax.broadcasted_iota(jnp.int32, (1, 2 * HEAD_DIM), 1)
    key_at = lax.broadcasted_iota(jnp.int32, (1, rows), 1)
    pairs = local // (2 * HEAD_DIM)

    @pl.loop(0, count)
    def _(i):
        @pl.when(i > 0)
        def _():
            y_copy(0, i).wait_recv()
            hand_copy(0, i).start()

        here_copy(0, i).wait()
        core_copy(0, i).wait_recv()
        hand_copy(0, i).wait_recv()
        values = source[i].astype(F32)
        middle = jnp.sum(values, axis=1, keepdims=True) / width
        square = jnp.sum(values * values, axis=1, keepdims=True) / width
        inverse = lax.rsqrt(square - middle * middle + NORM_EPS)
        low[i] = ((values - middle) * inverse * gain_ref[...] + shift_ref[...]).astype(BF16)
        mixed[i] = (jnp.dot(low[i], qkv_full[...], preferred_element_type=F32) + qkv_bias_ref[...]).astype(BF16)
        for pair_at in range(pairs):
            base = pair_at * 6 * HEAD_DIM
            queries = mixed[i, :, base : base + 2 * HEAD_DIM]
            key_rows = mixed[i, :, base + 2 * HEAD_DIM : base + 4 * HEAD_DIM]
            value_rows = mixed[i, :, base + 4 * HEAD_DIM : base + 6 * HEAD_DIM]
            parts = []
            for side in range(2):
                mask = (lane // HEAD_DIM) == side
                head_q = jnp.where(mask, queries, jnp.zeros_like(queries))
                scores = lax.dot_general(head_q, key_rows, NT, preferred_element_type=F32)
                scores = jnp.where(key_at < seq, scores, -1e30)
                peak = jnp.max(scores, axis=1, keepdims=True)
                powers = jnp.exp2((scores - peak) * (HEAD_DIM**-0.5 * LOG2E))
                share = 1.0 / jnp.sum(powers, axis=1, keepdims=True)
                probs_low = (powers * share).astype(BF16)
                probs[i, 2 * pair_at + side] = probs_low
                parts.append(jnp.dot(probs_low, value_rows, preferred_element_type=F32))
            joined = jnp.where((lane // HEAD_DIM) == 0, parts[0], parts[1])
            att[i, :, 2 * HEAD_DIM * pair_at : 2 * HEAD_DIM * (pair_at + 1)] = joined.astype(BF16)
        attended = att[i]
        theirs[i] = lax.dot_general(attended, out_full[2 * local :, :], NT, preferred_element_type=F32).astype(BF16)
        given_copy(i).start()
        mine[...] = lax.dot_general(attended, out_full[: 2 * local, :], NT, preferred_element_type=F32)
        given_copy(i).wait_recv()
        pair[i] = (mine[...] + given[i].astype(F32)).astype(BF16)
        pair_copy(i).start()

    outs = (
        (source, source_out), (low, low_out), (mixed, mixed_out), (probs, probs_out), (att, att_out),
        (qkv_full, qkv_out), (out_full, outw_out),
    )
    for k, (here, there) in enumerate(outs):
        pltpu.make_async_copy(here, there, out_sem.at[k]).start()
    forward(2)
    forward(3)
    for i in range(count):
        y_copy(1, i).wait_recv()
        hand_copy(1, i).start()

    @pl.loop(0, count)
    def _(i):
        pair_copy(i).wait_recv()
        total[i, :, : local] = (pair[i, :, : local].astype(F32) + pair_in[i, :, local:].astype(F32)).astype(BF16)
        total[i, :, local : 2 * local] = (
            pair[i, :, local:].astype(F32) + pair_in[i, :, : local].astype(F32)
        ).astype(BF16)
        total_copy(i).start()

    arrived(2)
    arrived(3)
    for i in range(count):
        here_copy(1, i).wait()
        core_copy(1, i).wait_recv()
        hand_copy(1, i).wait_recv()
    later = ((fc1_full, fc1_out), (fc2_full, fc2_out), (cot, cot_out))
    for k, (here, there) in enumerate(later):
        pltpu.make_async_copy(here, there, out_sem.at[len(outs) + k]).start()
    for i in range(count):
        total_copy(i).wait_recv()
    last = len(outs) + len(later)
    pltpu.make_async_copy(total, total_out, out_sem.at[last]).start()
    for w in range(4):
        for d in range(1, row_count):
            row_copy(w, d).wait_send()
            dp_copy(w, d).wait_send()
    for i in range(count):
        for a in range(2):
            y_copy(a, i).wait_send()
            core_copy(a, i).wait_send()
            hand_copy(a, i).wait_send()
        given_copy(i).wait_send()
        pair_copy(i).wait_send()
        total_copy(i).wait_send()
    for k, (here, there) in enumerate((*outs, *later, (total, total_out))):
        pltpu.make_async_copy(here, there, out_sem.at[k]).wait()


def front(images, cotangent, qkv_block, out_block, fc1_block, fc2_block, gain, shift, qkv_bias, seq):
    count, rows, local = images.shape
    row_count = lax.axis_size("row")
    width = 4 * local
    heads = local // HEAD_DIM
    hidden = fc1_block.shape[1]
    qkv_width = qkv_block.shape[1]

    def wide(*shape):
        return shape, BF16

    outs = [
        wide(count, rows, width), wide(count, rows, width), wide(count, rows, width), wide(count, rows, qkv_width),
        wide(count, heads, rows, rows), wide(count, rows, local), wide(count, rows, width),
        wide(width, qkv_width), wide(width, local), wide(width, hidden), wide(width, hidden),
    ]
    scratch = [
        wide(count, rows, width), wide(count, rows, width), wide(count, rows, width), wide(count, rows, qkv_width),
        wide(count, heads, rows, rows), wide(count, rows, local),
        wide(count, rows, 2 * local), wide(count, rows, 2 * local), ((rows, 2 * local), F32),
        wide(count, rows, 2 * local), wide(count, rows, 2 * local), wide(count, rows, width),
        wide(width, qkv_width), wide(width, local), wide(width, hidden), wide(width, hidden),
    ]
    dma = pltpu.SemaphoreType.DMA
    whole = pl.BlockSpec(memory_space=pl.ANY)
    vmem = pl.BlockSpec(memory_space=pltpu.VMEM)
    return pl.pallas_call(
        functools.partial(front_kernel, (count, seq, rows, local, row_count)),
        out_shape=[jax.ShapeDtypeStruct(*s) for s in outs],
        in_specs=[whole] * 6 + [vmem] * 3,
        out_specs=[whole] * len(outs),
        scratch_shapes=[pltpu.VMEM(*s) for s in scratch]
        + [dma((4, row_count))] * 4
        + [dma((4,)), dma((2, 4, count)), dma((2, 3, count)), dma((3, count)), dma((3, count)), dma((11,))],
        name="front",
        compiler_params=pltpu.CompilerParams(
            vmem_limit_bytes=62 * 2**20, collective_id=0, has_side_effects=True
        ),
    )(images, cotangent, qkv_block, out_block, fc1_block, fc2_block, gain, shift, qkv_bias)


def half_of(dp, full_width):
    half = full_width // 2
    return pl.ds(pl.multiple_of(dp * half, half), half)


def other_half_of(dp, full_width):
    half = full_width // 2
    return pl.ds(pl.multiple_of((1 - dp) * half, half), half)


def row_place(owner, row_count, place, block):
    per = row_count // 4
    at = (rel_place(owner // per, place) * per + owner % per) * block
    return pl.ds(pl.multiple_of(at, block), block)


def greet(partners):
    barrier = pltpu.get_barrier_semaphore()
    for partner in partners:
        pl.semaphore_signal(barrier, inc=1, device_id=partner, device_id_type=MESH)
    pl.semaphore_wait(barrier, len(partners))


def mlp_kernel(
    sizes,
    source_ref, total_ref, cot_ref, fc1_ref, fc2_ref, bias_ref, gain_ref, shift_ref, fc1_bias_ref, fc2_bias_ref,
    grad_out, move_out, kept_out, fc1_grad_out, fc2_half_out, bias_out,
    source, total, cot, fc1, fc2, low, active, gelu_grad, theirs, given, mine, pair, pair_in, grad_low,
    move_theirs, move_given, kept, move, fc1_grad, fc2_grad, dp_in, fc2_half,
    load_sem, sum_send, sum_recv, move_send, move_recv, dp_send, dp_recv, out_sem,
):
    count, rows, local, row_count = sizes
    dp, row, place = lax.axis_index("dp"), lax.axis_index("row"), lax.axis_index("col")
    core_at = {"col": place + 1 - 2 * (place % 2)}
    y_at = {"col": (place + 2) % 4}
    dp_at = {"dp": 1 - dp}
    greet([core_at, y_at, dp_at])
    width = 4 * local
    hidden_width = fc1.shape[1]
    block = width // row_count

    def load(k, i):
        here, there = ((source_ref, source), (total_ref, total), (cot_ref, cot))[k]
        return pltpu.make_async_copy(here.at[i], there.at[i], load_sem.at[k, i])

    fc1_load = pltpu.make_async_copy(fc1_ref, fc1, load_sem.at[3, 0])
    fc2_load = pltpu.make_async_copy(fc2_ref, fc2, load_sem.at[3, 1])
    for i in range(count):
        for k in range(3):
            load(k, i).start()
        if i == 0:
            fc1_load.start()
            fc2_load.start()

    def given_copy(i):
        return copy_to(theirs.at[i], given.at[i], sum_send.at[0, i], sum_recv.at[0, i], core_at)

    def pair_copy(i):
        return copy_to(pair.at[i], pair_in.at[i], sum_send.at[1, i], sum_recv.at[1, i], y_at)

    def total_copy(i):
        return copy_to(
            grad_low.at[i, :, pl.ds(0, 2 * local)],
            grad_low.at[i, :, pl.ds(2 * local, 2 * local)],
            sum_send.at[2, i],
            sum_recv.at[2, i],
            core_at,
        )

    def move_copy(i):
        return copy_to(move_theirs.at[i], move_given.at[i], move_send.at[i], move_recv.at[i], core_at)

    def dp_copy(d):
        there = row_place((row + d) % row_count, row_count, place, block)
        return copy_to(
            fc2_grad.at[there, other_half_of(dp, hidden_width)], dp_in.at[there, :], dp_send.at[d], dp_recv.at[d], dp_at
        )

    bias_out[...] = jnp.zeros_like(bias_out)
    step = hidden_width // 4
    fc1_load.wait()
    fc2_load.wait()

    @pl.loop(0, count)
    def _(i):
        for k in range(3):
            load(k, i).wait()
        values = source[i].astype(F32) + total[i].astype(F32) + bias_ref[...]
        kept[i] = values[:, :local] + fc2_bias_ref[...]
        middle = jnp.sum(values, axis=1, keepdims=True) / width
        square = jnp.sum(values * values, axis=1, keepdims=True) / width
        inverse = lax.rsqrt(square - middle * middle + NORM_EPS)
        low[i] = ((values - middle) * inverse * gain_ref[...] + shift_ref[...]).astype(BF16)
        bias_out[1:2, :local] += jnp.sum(cot[i, :, :local].astype(F32), axis=0, keepdims=True)
        for part in range(4):
            cols = slice(part * step, (part + 1) * step)
            pre_act = jnp.dot(low[i], fc1[:, cols], preferred_element_type=F32) + fc1_bias_ref[:, cols]
            gate = 0.5 * (1.0 + lax.erf(pre_act * ROOT_HALF))
            active[i, :, cols] = (pre_act * gate).astype(BF16)
            slope = gate + pre_act * jnp.exp(-0.5 * pre_act * pre_act) / ROOT_TWO_PI
            grad_pre = jnp.dot(cot[i], fc2[:, cols], preferred_element_type=F32) * slope
            bias_out[0:1, cols] += jnp.sum(grad_pre, axis=0, keepdims=True)
            gelu_grad[i, :, cols] = grad_pre.astype(BF16)
        theirs[i] = lax.dot_general(gelu_grad[i], fc1[2 * local :, :], NT, preferred_element_type=F32).astype(BF16)
        given_copy(i).start()
        mine[...] = lax.dot_general(gelu_grad[i], fc1[: 2 * local, :], NT, preferred_element_type=F32)
        given_copy(i).wait_recv()
        pair[i] = (mine[...] + given[i].astype(F32)).astype(BF16)
        pair_copy(i).start()

    def weight_grad(out, left, right):
        for part in range(4):
            span = slice(part * local, (part + 1) * local)
            terms = [
                lax.dot_general(left[i, :, span], right[i], TN, preferred_element_type=F32) for i in range(count)
            ]
            out[span, :] = sum(terms[1:], terms[0]).astype(BF16)

    weight_grad(fc2_grad, cot, active)
    for d in range(row_count):
        dp_copy((d + 1) % row_count).start()

    @pl.loop(0, count)
    def _(i):
        move_theirs[i] = lax.dot_general(active[i], fc2[2 * local :, :], NT, preferred_element_type=F32).astype(BF16)
        move_copy(i).start()
        mine[...] = lax.dot_general(active[i], fc2[: 2 * local, :], NT, preferred_element_type=F32)
        move_copy(i).wait_recv()
        kept[i] += mine[:, :local] + move_given[i, :, :local].astype(F32)
        move[i] = (mine[:, local:] + move_given[i, :, local:].astype(F32)).astype(BF16)

    weight_grad(fc1_grad, low, gelu_grad)
    outs = ((move, move_out), (kept, kept_out), (fc1_grad, fc1_grad_out))
    for k, (here, there) in enumerate(outs):
        pltpu.make_async_copy(here, there, out_sem.at[k]).start()

    @pl.loop(0, count)
    def _(i):
        pair_copy(i).wait_recv()
        grad_low[i, :, :local] = (pair[i, :, :local].astype(F32) + pair_in[i, :, local:].astype(F32)).astype(BF16)
        grad_low[i, :, local : 2 * local] = (
            pair[i, :, local:].astype(F32) + pair_in[i, :, :local].astype(F32)
        ).astype(BF16)
        total_copy(i).start()

    for d in range(row_count):
        dp_copy((d + 1) % row_count).wait_recv()
    fc2_half[...] = (
        fc2_grad[:, half_of(dp, hidden_width)].astype(F32) + dp_in[...].astype(F32)
    ).astype(BF16)
    for i in range(count):
        total_copy(i).wait_recv()
    more = ((fc2_half, fc2_half_out), (grad_low, grad_out))
    for k, (here, there) in enumerate(more):
        pltpu.make_async_copy(here, there, out_sem.at[len(outs) + k]).start()
    for i in range(count):
        given_copy(i).wait_send()
        pair_copy(i).wait_send()
        total_copy(i).wait_send()
        move_copy(i).wait_send()
    for d in range(row_count):
        dp_copy(d).wait_send()
    for k, (here, there) in enumerate((*outs, *more)):
        pltpu.make_async_copy(here, there, out_sem.at[k]).wait()


def mlp(source, total, cot, fc1, fc2, bias, gain, shift, fc1_bias, fc2_bias):
    count, rows, width = source.shape
    local = width // 4
    row_count = lax.axis_size("row")
    hidden = fc1.shape[1]
    outs = [
        ((count, rows, width), BF16), ((count, rows, local), BF16), ((count, rows, local), F32),
        ((width, hidden), BF16), ((width, hidden // 2), BF16), ((2, hidden), F32),
    ]
    all_wide = ((count, rows, width), BF16)
    all_pair = ((count, rows, 2 * local), BF16)
    scratch = [
        all_wide, all_wide, all_wide, ((width, hidden), BF16), ((width, hidden), BF16), all_wide,
        ((count, rows, hidden), BF16), ((count, rows, hidden), BF16),
        all_pair, all_pair, ((rows, 2 * local), F32), all_pair, all_pair, all_wide,
        all_pair, all_pair, ((count, rows, local), F32), ((count, rows, local), BF16),
        ((width, hidden), BF16), ((width, hidden), BF16), ((width, hidden // 2), BF16), ((width, hidden // 2), BF16),
    ]
    dma = pltpu.SemaphoreType.DMA
    whole = pl.BlockSpec(memory_space=pl.ANY)
    vmem = pl.BlockSpec(memory_space=pltpu.VMEM)
    return pl.pallas_call(
        functools.partial(mlp_kernel, (count, rows, local, row_count)),
        out_shape=[jax.ShapeDtypeStruct(*s) for s in outs],
        in_specs=[whole] * 5 + [vmem] * 5,
        out_specs=[whole] * 5 + [vmem],
        scratch_shapes=[pltpu.VMEM(*s) for s in scratch]
        + [dma((4, count)), dma((3, count)), dma((3, count)), dma((count,)), dma((count,))]
        + [dma((row_count,)), dma((row_count,)), dma((5,))],
        name="mlp",
        compiler_params=pltpu.CompilerParams(
            vmem_limit_bytes=62 * 2**20, collective_id=1, has_side_effects=True
        ),
    )(source, total, cot, fc1, fc2, bias, gain, shift, fc1_bias, fc2_bias)


def back_kernel(
    sizes,
    source_ref, total_ref, cot_ref, grad_ref, mixed_ref, probs_ref, att_ref, low_ref, move_ref, kept_ref,
    qkv_ref, outw_ref, fc1_grad_ref, fc2_half_ref, bias_ref, gain1_ref, gain2_ref, mlp_bias_ref,
    images_out, images_grad_out, small_out, qkv_out, outw_out, fc1_out, fc2_out,
    source, total, cot, grad_in, mixed, probs, att, low,
    hidden_low, mixed_grad, grad_hidden, normed1, inverse1, qkv_sum, outw_sum, k_turned, v_turned,
    theirs, given, mine, kept_grad, send, got, stat, stat_given, stat_pair, stat_in,
    move_in, kept, finished, qkv, outw, qkv_grad, outw_grad, small, small_in,
    half_fc2, half_fc1, half_outw, half_qkv, dp_fc1, dp_outw, dp_qkv,
    row_fc2, row_fc1, row_outw, row_qkv, tot_fc2, tot_fc1, tot_outw, tot_qkv,
    early_sem, late_sem, once_sem, sum_send, sum_recv, move_send, move_recv, small_send, small_recv,
    dp_send, dp_recv, row_send, row_recv, tot_send, tot_recv, out_sem,
):
    count, rows, local, row_count = sizes
    dp, row, place = lax.axis_index("dp"), lax.axis_index("row"), lax.axis_index("col")
    core_at = {"col": place + 1 - 2 * (place % 2)}
    y_at = {"col": (place + 2) % 4}
    dp_at = {"dp": 1 - dp}
    greet([core_at, y_at, dp_at] + [{"row": (row + d) % row_count} for d in range(1, row_count)])
    width = 4 * local
    block = width // row_count
    two = 2 * HEAD_DIM
    scale = HEAD_DIM**-0.5

    early = ((source_ref, source), (total_ref, total), (cot_ref, cot), (grad_ref, grad_in))
    late = ((mixed_ref, mixed), (probs_ref, probs), (att_ref, att), (low_ref, low))

    def early_load(k, i):
        here, there = early[k]
        return pltpu.make_async_copy(here.at[i], there.at[i % 2] if k == 0 else there, early_sem.at[k])

    def late_load(k, i):
        here, there = late[k]
        return pltpu.make_async_copy(here.at[i], there, late_sem.at[k])

    once = (
        (outw_ref, outw), (qkv_ref, qkv), (fc2_half_ref, half_fc2),
        (fc1_grad_ref.at[:, half_of(dp, fc1_grad_ref.shape[1])], half_fc1), (kept_ref, kept),
    )

    def once_load(k):
        return pltpu.make_async_copy(once[k][0], once[k][1], once_sem.at[k])

    grads = (None, fc1_grad_ref, outw_grad, qkv_grad)
    halves = (half_fc2, half_fc1, half_outw, half_qkv)
    dp_ins = (None, dp_fc1, dp_outw, dp_qkv)
    row_ins = (row_fc2, row_fc1, row_outw, row_qkv)
    tots = (tot_fc2, tot_fc1, tot_outw, tot_qkv)

    def rows_at(d):
        return row_place((row + d) % row_count, row_count, place, block)

    def dp_copy(w, d):
        full = grads[w]
        return copy_to(
            full.at[rows_at(d), other_half_of(dp, full.shape[1])],
            dp_ins[w].at[rows_at(d), :],
            dp_send.at[w, d],
            dp_recv.at[w, d],
            dp_at,
        )

    def row_copy(w, d):
        return copy_to(
            halves[w].at[rows_at(d), :],
            row_ins[w].at[d],
            row_send.at[w, d],
            row_recv.at[w, d],
            {"row": (row + d) % row_count},
        )

    def tot_copy(w):
        part = tots[w].at[:, half_of(dp, tots[w].shape[1])]
        return copy_to(part, part, tot_send.at[w], tot_recv.at[w], dp_at)

    def given_copy(i):
        return copy_to(theirs.at[i], given.at[i], sum_send.at[0, i], sum_recv.at[0, i], core_at)

    def stat_copy(i):
        return copy_to(stat.at[i], stat_given.at[i], sum_send.at[1, i], sum_recv.at[1, i], core_at)

    def got_copy(i):
        return copy_to(send.at[i], got.at[i], sum_send.at[2, i], sum_recv.at[2, i], y_at)

    def stat_pair_copy(i):
        return copy_to(stat_pair.at[i], stat_in.at[i], sum_send.at[3, i], sum_recv.at[3, i], y_at)

    def move_copy(i):
        return copy_to(move_ref.at[i], move_in.at[i], move_send.at[i], move_recv.at[i], y_at)

    rounds = [dp_at]
    distance = 1
    while distance < row_count:
        rounds.append({"row": row + distance * (1 - 2 * ((row // distance) % 2))})
        distance *= 2

    def small_copy(s):
        return copy_to(small.at[s], small_in.at[s], small_send.at[s], small_recv.at[s], rounds[s])

    for k in range(4):
        early_load(k, 0).start()
    for k in range(len(once)):
        once_load(k).start()
    for k in range(4):
        late_load(k, 0).start()
    for i in range(count):
        move_copy(i).start()
    for d in range(1, row_count + 1):
        dp_copy(1, d % row_count).start()

    small[0] = jnp.zeros_like(small[0])
    small[0, 7:8, :] = mlp_bias_ref[1:2, :local]
    for part in range(mlp_bias_ref.shape[1] // local):
        small[0, 8 + part : 9 + part, :] = mlp_bias_ref[0:1, part * local : (part + 1) * local]
    qkv_sum[...] = jnp.zeros_like(qkv_sum)
    outw_sum[...] = jnp.zeros_like(outw_sum)
    once_load(0).wait()
    once_load(1).wait()
    once_load(2).wait()
    for d in range(1, row_count):
        row_copy(0, d).start()
    lane = lax.broadcasted_iota(jnp.int32, (1, two), 1)
    down = lax.broadcasted_iota(jnp.int32, (two, two), 0)
    across = lax.broadcasted_iota(jnp.int32, (two, two), 1)
    eye = (down == across).astype(BF16)

    @pl.loop(0, count)
    def _(i):
        for k in range(4):
            early_load(k, i).wait()
        values = source[i % 2].astype(F32) + total[...].astype(F32) + bias_ref[...]
        middle = jnp.sum(values, axis=1, keepdims=True) / width
        square = jnp.sum(values * values, axis=1, keepdims=True) / width
        inverse = lax.rsqrt(square - middle * middle + NORM_EPS)
        normed = (values - middle) * inverse
        grad = grad_in[...].astype(F32)
        small[0, 5:6, :] += jnp.sum(grad[:, :local] * normed[:, :local], axis=0, keepdims=True)
        small[0, 6:7, :] += jnp.sum(grad[:, :local], axis=0, keepdims=True)
        scaled = grad * gain2_ref[...]
        first = jnp.sum(scaled, axis=1, keepdims=True) / width
        second = jnp.sum(scaled * normed, axis=1, keepdims=True) / width
        whole_grad = cot[...].astype(F32) + inverse * (scaled - first - normed * second)
        grad_hidden[i] = whole_grad[:, :local]
        small[0, 2:3, :] += jnp.sum(whole_grad[:, :local], axis=0, keepdims=True)
        hidden_low[...] = whole_grad.astype(BF16)

        @pl.when(i + 1 < count)
        def _():
            for k in range(4):
                early_load(k, i + 1).start()

        for k in range(4):
            late_load(k, i).wait()
        grad_att = jnp.dot(hidden_low[...], outw[...], preferred_element_type=F32).astype(BF16)
        for part in range(4):
            span = slice(part * local, (part + 1) * local)
            outw_sum[span, :] += lax.dot_general(hidden_low[:, span], att[...], TN, preferred_element_type=F32)
        for pair in range(local // two):
            base = pair * 3 * two
            cols = slice(pair * two, (pair + 1) * two)
            queries = mixed[:, base : base + two]
            key_rows = mixed[:, base + two : base + 2 * two]
            value_rows = mixed[:, base + 2 * two : base + 3 * two]
            pair_grad = grad_att[:, cols]
            q_turned = lax.dot_general(eye, queries, NT, preferred_element_type=F32).astype(BF16)
            grad_turned = lax.dot_general(eye, pair_grad, NT, preferred_element_type=F32).astype(BF16)
            product = pair_grad.astype(F32) * att[:, cols].astype(F32)
            parts = []
            for side in range(2):
                mask = (lane // HEAD_DIM) == side
                turn = slice(side * HEAD_DIM, (side + 1) * HEAD_DIM)
                head_grad = jnp.where(mask, pair_grad, jnp.zeros_like(pair_grad))
                grad_probs = lax.dot_general(head_grad, value_rows, NT, preferred_element_type=F32)
                delta = jnp.sum(jnp.where(mask, product, 0.0), axis=1, keepdims=True)
                probs_low = probs[2 * pair + side]
                grad_scores = (probs_low.astype(F32) * (grad_probs - delta)).astype(BF16)
                parts.append(jnp.dot(grad_scores, key_rows, preferred_element_type=F32))
                k_turned[turn, :] = jnp.dot(q_turned[turn, :], grad_scores, preferred_element_type=F32)
                v_turned[turn, :] = jnp.dot(grad_turned[turn, :], probs_low, preferred_element_type=F32)
            q_grad = jnp.where((lane // HEAD_DIM) == 0, parts[0], parts[1]) * scale
            v_grad = v_turned[...].T
            mixed_grad[:, base : base + two] = q_grad.astype(BF16)
            mixed_grad[:, base + two : base + 2 * two] = (k_turned[...].T * scale).astype(BF16)
            mixed_grad[:, base + 2 * two : base + 3 * two] = v_grad.astype(BF16)
            small[0, 0:1, cols] += jnp.sum(q_grad, axis=0, keepdims=True)
            small[0, 1:2, cols] += jnp.sum(v_grad, axis=0, keepdims=True)
        values = source[i % 2].astype(F32)
        middle = jnp.sum(values, axis=1, keepdims=True) / width
        square = jnp.sum(values * values, axis=1, keepdims=True) / width
        inverse = lax.rsqrt(square - middle * middle + NORM_EPS)
        normed = (values - middle) * inverse
        normed1[i] = normed[:, :local]
        inverse1[i] = inverse
        scaled_in = normed * gain1_ref[...]
        far = lax.dot_general(mixed_grad[...], qkv[2 * local :, :], NT, preferred_element_type=F32)
        theirs[i] = far.astype(BF16)
        given_copy(i).start()
        near = lax.dot_general(mixed_grad[...], qkv[: 2 * local, :], NT, preferred_element_type=F32)
        mine[...] = near
        first = jnp.sum(far * gain1_ref[:, 2 * local :], axis=1, keepdims=True) + jnp.sum(
            near * gain1_ref[:, : 2 * local], axis=1, keepdims=True
        )
        second = jnp.sum(far * scaled_in[:, 2 * local :], axis=1, keepdims=True) + jnp.sum(
            near * scaled_in[:, : 2 * local], axis=1, keepdims=True
        )
        spread = jnp.where(lane == 0, first, jnp.where(lane == 1, second, 0.0))
        stat[i] = spread.T[:8, :]
        stat_copy(i).start()
        for part in range(4):
            span = slice(part * local, (part + 1) * local)
            qkv_sum[span, :] += lax.dot_general(low[:, span], mixed_grad[...], TN, preferred_element_type=F32)

        @pl.when(i + 1 < count)
        def _():
            for k in range(4):
                late_load(k, i + 1).start()

        given_copy(i).wait_recv()
        kept_grad[i] = mine[:, :local] + given[i, :, :local].astype(F32)
        send[i] = (mine[:, local:] + given[i, :, local:].astype(F32)).astype(BF16)
        got_copy(i).start()
        stat_copy(i).wait_recv()
        stat_pair[i] = stat[i] + stat_given[i]
        stat_pair_copy(i).start()

    outw_grad[...] = outw_sum[...].astype(BF16)
    for d in range(1, row_count + 1):
        dp_copy(2, d % row_count).start()
    qkv_grad[...] = qkv_sum[...].astype(BF16)
    for d in range(1, row_count + 1):
        dp_copy(3, d % row_count).start()
    once_load(3).wait()
    for d in range(1, row_count + 1):
        at = d % row_count
        dp_copy(1, at).wait_recv()
        half_fc1[rows_at(at), :] = (
            half_fc1[rows_at(at), :].astype(F32) + dp_fc1[rows_at(at), :].astype(F32)
        ).astype(BF16)
        if at:
            row_copy(1, at).start()

    once_load(4).wait()

    @pl.loop(0, count)
    def _(i):
        move_copy(i).wait_recv()
        finished[i] = (kept[i] + move_in[i].astype(F32)).astype(BF16)

    for w in (2, 3):
        for d in range(1, row_count + 1):
            at = d % row_count
            dp_copy(w, at).wait_recv()
            halves[w][rows_at(at), :] = (
                grads[w][rows_at(at), half_of(dp, grads[w].shape[1])].astype(F32) + dp_ins[w][rows_at(at), :].astype(F32)
            ).astype(BF16)
            if at:
                row_copy(w, at).start()

    @pl.loop(0, count)
    def _(i):
        got_copy(i).wait_recv()
        stat_pair_copy(i).wait_recv()
        sums = stat_pair[i] + stat_in[i]
        spread = jnp.concatenate([sums, jnp.zeros((two - 8, rows), F32)], axis=0).T / width
        grad = kept_grad[i] + got[i].astype(F32)
        small[0, 3:4, :] += jnp.sum(grad * normed1[i], axis=0, keepdims=True)
        small[0, 4:5, :] += jnp.sum(grad, axis=0, keepdims=True)
        scaled = grad * gain1_ref[:, :local]
        grad_hidden[i] += inverse1[i] * (scaled - spread[:, 0:1] - normed1[i] * spread[:, 1:2])

    pltpu.make_async_copy(finished, images_out, out_sem.at[0]).start()
    pltpu.make_async_copy(grad_hidden, images_grad_out, out_sem.at[1]).start()
    small_copy(0).start()
    for w in range(4):
        sums = halves[w][rows_at(0), :].astype(F32)
        for d in range(1, row_count):
            row_copy(w, d).wait_recv()
            sums += row_ins[w][d].astype(F32)
        tots[w][:, half_of(dp, tots[w].shape[1])] = sums.astype(BF16)
        tot_copy(w).start()
        if w < len(rounds):
            small_copy(w).wait_recv()
            small[w + 1] = small[w] + small_in[w]
            if w + 1 < len(rounds):
                small_copy(w + 1).start()
    for s in range(4, len(rounds)):
        small_copy(s).wait_recv()
        small[s + 1] = small[s] + small_in[s]
        if s + 1 < len(rounds):
            small_copy(s + 1).start()
    outs = ((tot_fc2, fc2_out), (tot_fc1, fc1_out), (tot_outw, outw_out), (tot_qkv, qkv_out))
    for w, (here, there) in enumerate(outs):
        tot_copy(w).wait_recv()
        pltpu.make_async_copy(here, there, out_sem.at[2 + w]).start()
    small_out[...] = small[len(rounds)]
    for i in range(count):
        given_copy(i).wait_send()
        stat_copy(i).wait_send()
        got_copy(i).wait_send()
        stat_pair_copy(i).wait_send()
        move_copy(i).wait_send()
    for s in range(len(rounds)):
        small_copy(s).wait_send()
    for w in range(4):
        tot_copy(w).wait_send()
        for d in range(row_count):
            if w:
                dp_copy(w, d).wait_send()
            if d:
                row_copy(w, d).wait_send()
    for k, (here, there) in enumerate(((finished, images_out), (grad_hidden, images_grad_out), *outs)):
        pltpu.make_async_copy(here, there, out_sem.at[k]).wait()


def back(
    source, total, cot, grad_low, mixed, probs, att, low, move, kept, qkv, outw, fc1_grad, fc2_half, bias, gain1, gain2, mlp_bias
):
    count, rows, width = source.shape
    local = width // 4
    row_count = lax.axis_size("row")
    block = width // row_count
    hidden = fc1_grad.shape[1]
    qkv_width = qkv.shape[1]
    heads = local // HEAD_DIM
    rounds = row_count.bit_length()
    outs = [
        ((count, rows, local), BF16), ((count, rows, local), F32), ((16, local), F32),
        ((block, qkv_width), BF16), ((block, local), BF16), ((block, hidden), BF16), ((block, hidden), BF16),
    ]
    own_f32 = ((count, rows, local), F32)
    own_low = ((count, rows, local), BF16)
    pair_low = ((count, rows, 2 * local), BF16)
    stat = ((count, 8, rows), F32)
    wide = ((rows, width), BF16)
    turned = ((2 * HEAD_DIM, rows), F32)
    columns = (hidden, hidden, local, qkv_width)
    scratch = [
        ((2, rows, width), BF16), wide, wide, wide, ((rows, qkv_width), BF16), ((heads, rows, rows), BF16), ((rows, local), BF16), wide,
        wide, ((rows, qkv_width), BF16), own_f32, own_f32, ((count, rows, 1), F32),
        ((width, qkv_width), F32), ((width, local), F32), turned, turned,
        pair_low, pair_low, ((rows, 2 * local), F32), own_f32, own_low, own_low, stat, stat, stat, stat,
        own_low, own_f32, own_low, ((width, qkv_width), BF16), ((width, local), BF16),
        ((width, qkv_width), BF16), ((width, local), BF16), ((rounds + 1, 16, local), F32), ((rounds, 16, local), F32),
        *[((width, c // 2), BF16) for c in columns],
        *[((width, c // 2), BF16) for c in columns[1:]],
        *[((row_count, block, c // 2), BF16) for c in columns],
        *[((block, c), BF16) for c in columns],
    ]
    dma = pltpu.SemaphoreType.DMA
    whole = pl.BlockSpec(memory_space=pl.ANY)
    vmem = pl.BlockSpec(memory_space=pltpu.VMEM)
    return pl.pallas_call(
        functools.partial(back_kernel, (count, rows, local, row_count)),
        out_shape=[jax.ShapeDtypeStruct(*s) for s in outs],
        in_specs=[whole] * 14 + [vmem] * 4,
        out_specs=[whole, whole, vmem] + [whole] * 4,
        scratch_shapes=[pltpu.VMEM(*s) for s in scratch]
        + [dma((4,)), dma((4,)), dma((5,)), dma((4, count)), dma((4, count)), dma((count,)), dma((count,)), dma((rounds,)), dma((rounds,))]
        + [dma((4, row_count))] * 4
        + [dma((4,)), dma((4,)), dma((6,))],
        name="back",
        compiler_params=pltpu.CompilerParams(
            vmem_limit_bytes=63 * 2**20, collective_id=2, has_side_effects=True
        ),
    )(source, total, cot, grad_low, mixed, probs, att, low, move, kept, qkv, outw, fc1_grad, fc2_half, bias, gain1, gain2, mlp_bias)


def adam_step(weight, grad, momentum, variance):
    moment_new = BETA_FIRST * momentum + (1.0 - BETA_FIRST) * grad
    second_new = BETA_SECOND * variance + (1.0 - BETA_SECOND) * grad * grad
    corrected = moment_new / (1.0 - BETA_FIRST**STEP)
    second_corrected = second_new / (1.0 - BETA_SECOND**STEP)
    master = weight.astype(jnp.float32)
    updated = master - LEARN_RATE * (
        corrected / (jnp.sqrt(second_corrected) + ADAM_EPS) + WEIGHT_DECAY * master
    )
    return (updated, moment_new, second_new)


def per_device(
    images_in,
    cotangent,
    first_gain,
    first_shift,
    second_gain,
    second_shift,
    qkv_weight,
    qv_bias,
    out_weight,
    out_bias,
    fc1_weight,
    fc1_bias,
    fc2_weight,
    fc2_bias,
    qkv_momentum,
    qkv_variance,
    out_momentum,
    out_variance,
    fc1_momentum,
    fc1_variance,
    fc2_momentum,
    fc2_variance,
):
    image_count, seq, local = images_in.shape
    width = 4 * local
    rows = -(-seq // ROW_TILE) * ROW_TILE
    place = lax.axis_index("col")

    def paired(value):
        lead = value.shape[:-2]
        value = value.reshape(*lead, 3, local // 128, 128)
        return jnp.swapaxes(value, -3, -2).reshape(*lead, 3 * local)

    def unpaired(value):
        value = value.reshape(value.shape[0], local // 128, 3, 128)
        return jnp.swapaxes(value, 1, 2).reshape(value.shape[0], 3, local)

    vectors = whole_width(jnp.stack([first_gain, first_shift, second_gain, second_shift, out_bias]))
    gain1, shift1, gain2, shift2, bias_out = (vectors[i] for i in range(5))
    qkv_shift = paired(jnp.stack([qv_bias[0], jnp.zeros_like(qv_bias[0]), qv_bias[1]]))
    (source_all, cot_all, low_all, mixed_all, probs_all, att_all, total_all, qkv_full, out_full, fc1_full, fc2_full) = front(
        jnp.pad(images_in, ((0, 0), (0, rows - seq), (0, 0))),
        jnp.pad(cotangent, ((0, 0), (0, rows - seq), (0, 0))),
        paired(qkv_weight),
        out_weight,
        fc1_weight,
        fc2_weight,
        gain1[None],
        shift1[None],
        qkv_shift[None],
        seq,
    )
    grad_low2, move, kept, fc1_grad, fc2_half, mlp_bias = mlp(
        source_all, total_all, cot_all, fc1_full, fc2_full,
        bias_out[None], gain2[None], shift2[None], fc1_bias[None], fc2_bias[None],
    )
    images_out, images_grad, small, qkv_total, out_total, fc1_total, fc2_total = back(
        source_all, total_all, cot_all, grad_low2, mixed_all, probs_all, att_all, low_all, move, kept,
        qkv_full, out_full, fc1_grad, fc2_half, bias_out[None], gain1[None], gain2[None], mlp_bias,
    )
    qkv_total = unpaired(qkv_total).astype(F32)
    out_total, fc1_total, fc2_total = (t.astype(F32) for t in (out_total, fc1_total, fc2_total))
    qkv_new = adam_step(qkv_weight, qkv_total, qkv_momentum, qkv_variance)
    out_new = adam_step(out_weight, out_total, out_momentum, out_variance)
    fc1_new = adam_step(fc1_weight, fc1_total, fc1_momentum, fc1_variance)
    fc2_new = adam_step(fc2_weight, fc2_total, fc2_momentum, fc2_variance)
    return (
        images_out[:, :seq],
        images_grad[:, :seq],
        qkv_total,
        out_total,
        fc1_total,
        fc2_total,
        small[0:2],
        small[2],
        small[8:12].reshape(-1),
        small[7],
        small[3],
        small[4],
        small[5],
        small[6],
        qkv_new[0],
        out_new[0],
        fc1_new[0],
        fc2_new[0],
        qkv_new[1],
        out_new[1],
        fc1_new[1],
        fc2_new[1],
        qkv_new[2],
        out_new[2],
        fc1_new[2],
        fc2_new[2],
    )


def solution(mesh):
    return jax.shard_map(
        per_device,
        mesh=mesh,
        in_specs=(
            P(("dp", "row"), None, "col"),
            P(("dp", "row"), None, "col"),
            P("col"),
            P("col"),
            P("col"),
            P("col"),
            P("row", None, "col"),
            P(None, "col"),
            P("row", "col"),
            P("col"),
            P("row", "col"),
            P("col"),
            P("row", "col"),
            P("col"),
            P("row", None, "col"),
            P("row", None, "col"),
            P("row", "col"),
            P("row", "col"),
            P("row", "col"),
            P("row", "col"),
            P("row", "col"),
            P("row", "col"),
        ),
        out_specs=(
            P(("dp", "row"), None, "col"),
            P(("dp", "row"), None, "col"),
            P("row", None, "col"),
            P("row", "col"),
            P("row", "col"),
            P("row", "col"),
            P(None, "col"),
            P("col"),
            P("col"),
            P("col"),
            P("col"),
            P("col"),
            P("col"),
            P("col"),
            P("row", None, "col"),
            P("row", "col"),
            P("row", "col"),
            P("row", "col"),
            P("row", None, "col"),
            P("row", "col"),
            P("row", "col"),
            P("row", "col"),
            P("row", None, "col"),
            P("row", "col"),
            P("row", "col"),
            P("row", "col"),
        ),
        check_vma=False,
    )
```

```python
import functools

import jax
import jax.numpy as jnp
from jax import lax
from jax.experimental import pallas as pl
from jax.experimental.pallas import tpu as pltpu
from jax.sharding import PartitionSpec as P

HEAD_DIM = 64
STEP = 3


NORM_EPS = 1e-06
LEARN_RATE = 0.02
BETA_FIRST = 0.9
BETA_SECOND = 0.999
ADAM_EPS = 1e-08
WEIGHT_DECAY = 0.05
ROOT_HALF = 0.7071067811865476
ROOT_TWO_PI = 2.5066282746310002
LOG2E = 1.4426950408889634
ROW_TILE = 16
MESH = pl.DeviceIdType.MESH
NT = (((1,), (1,)), ((), ()))
TN = (((0,), (0,)), ((), ()))
F32 = jnp.float32
BF16 = jnp.bfloat16


def copy_to(src, dst, send, recv, where):
    return pltpu.make_async_remote_copy(
        src_ref=src, dst_ref=dst, send_sem=send, recv_sem=recv, device_id=where, device_id_type=MESH
    )


def rel_place(quarter, place):
    return (quarter // 2 + place // 2) % 2 + 2 * ((quarter % 2 + place % 2) % 2)


def crossed(row, code):
    distance = 1
    while distance <= code:
        if code & distance:
            row = row + distance * (1 - 2 * ((row // distance) % 2))
        distance *= 2
    return row


def half_of(dp, full_width):
    half = full_width // 2
    return pl.ds(pl.multiple_of(dp * half, half), half)


def other_half_of(dp, full_width):
    half = full_width // 2
    return pl.ds(pl.multiple_of((1 - dp) * half, half), half)


def row_place(owner, row_count, place, block):
    per = row_count // 4
    at = (rel_place(owner // per, place) * per + owner % per) * block
    return pl.ds(pl.multiple_of(at, block), block)


def part_at(full, rows, cols):
    return full.at[:, rows, cols] if len(full.shape) == 3 else full.at[rows, cols]


def greet(partners):
    barrier = pltpu.get_barrier_semaphore()
    for partner in partners:
        pl.semaphore_signal(barrier, inc=1, device_id=partner, device_id_type=MESH)
    pl.semaphore_wait(barrier, len(partners))


def front_kernel(
    sizes,
    images_ref, cot_ref, qkv_ref, out_ref, fc1_ref, fc2_ref, vectors_ref, qkv_bias_ref,
    source_out, cot_out, low_out, mixed_out, probs_out, att_out, total_out, qkv_out, outw_out, fc1_out, fc2_out, vectors_out,
    source, cot, low, mixed, probs, att, theirs, given, mine, pair, pair_in, total, qkv_full, out_full, fc1_full, fc2_full, vectors,
    row_send, row_recv, dp_send, dp_recv, own_sem, in_send, in_recv, vec_send, vec_recv, sum_send, sum_recv, image_sem, out_sem,
):
    count, cot_count, seq, rows, local, row_count = sizes
    dp, row, place = lax.axis_index("dp"), lax.axis_index("row"), lax.axis_index("col")
    core_at = {"col": place + 1 - 2 * (place % 2)}
    y_at = {"col": (place + 2) % 4}
    dp_at = {"dp": 1 - dp}
    codes = sorted(range(1, row_count), key=lambda code: -(code & -code))
    fars = [code for code in codes if code & -code == code]
    greet([core_at, y_at, dp_at] + [{"row": crossed(row, far)} for far in fars])
    block = out_ref.shape[0]
    width = 4 * local
    weights = ((qkv_ref, qkv_full), (out_ref, out_full), (fc1_ref, fc1_full), (fc2_ref, fc2_full))

    def row_copy(w, code):
        ref, full = weights[w]
        cols = half_of(dp, full.shape[-1])
        far = code & -code
        held = part_at(full, row_place(crossed(row, code - far), row_count, place, block), cols)
        return copy_to(
            part_at(ref, slice(None), cols) if code == far else held, held, row_send.at[w, code], row_recv.at[w, code], {"row": crossed(row, far)}
        )

    def dp_copy(w, code):
        _, full = weights[w]
        part = part_at(full, row_place(crossed(row, code), row_count, place, block), half_of(dp, full.shape[-1]))
        return copy_to(part, part, dp_send.at[w, code], dp_recv.at[w, code], dp_at)

    def own_copy(w):
        ref, full = weights[w]
        return pltpu.make_async_copy(ref, part_at(full, row_place(row, row_count, place, block), slice(None)), own_sem.at[w])

    inputs = ((images_ref, source), (cot_ref, cot))

    def y_copy(a, i):
        ref, full = inputs[a]
        return copy_to(ref.at[i], full.at[i, :, pl.ds(local, local)], in_send.at[a, 0, i], in_recv.at[a, 0, i], y_at)

    def core_copy(a, i):
        ref, full = inputs[a]
        return copy_to(ref.at[i], full.at[i, :, pl.ds(2 * local, local)], in_send.at[a, 1, i], in_recv.at[a, 1, i], core_at)

    def hand_copy(a, i):
        _, full = inputs[a]
        return copy_to(
            full.at[i, :, pl.ds(local, local)],
            full.at[i, :, pl.ds(3 * local, local)],
            in_send.at[a, 2, i],
            in_recv.at[a, 2, i],
            core_at,
        )

    def here_copy(a, i):
        ref, full = inputs[a]
        return pltpu.make_async_copy(ref.at[i], full.at[i, :, pl.ds(0, local)], in_send.at[a, 3, i])

    def vector_copy(k):
        src = vectors.at[:, pl.ds(local, local)] if k == 2 else vectors_ref
        at = (local, 2 * local, 3 * local)[k]
        return copy_to(
            src, vectors.at[:, pl.ds(at, local)], vec_send.at[k], vec_recv.at[k], (y_at, core_at, core_at)[k]
        )

    vector_here = pltpu.make_async_copy(vectors_ref, vectors.at[:, pl.ds(0, local)], vec_send.at[3])

    def given_copy(i):
        return copy_to(theirs.at[i], given.at[i], sum_send.at[0, i], sum_recv.at[0, i], core_at)

    def pair_copy(i):
        return copy_to(pair.at[i], pair_in.at[i], sum_send.at[1, i], sum_recv.at[1, i], y_at)

    def total_copy(i):
        return copy_to(
            total.at[i, :, pl.ds(0, 2 * local)],
            total.at[i, :, pl.ds(2 * local, 2 * local)],
            sum_send.at[2, i],
            sum_recv.at[2, i],
            core_at,
        )

    def start_own(w):
        for far in fars:
            row_copy(w, far).start()

    def relay(w, code):
        row_copy(w, code).wait_recv()
        for far in fars:
            if far < code & -code:
                row_copy(w, code + far).start()
        dp_copy(w, code).start()

    def arrived(w):
        for code in codes:
            dp_copy(w, code).wait_recv()
        own_copy(w).wait()

    kinds = ((source, source_out), (low, low_out), (mixed, mixed_out), (probs, probs_out), (att, att_out))

    def image_copy(k, i):
        here, there = kinds[k]
        return pltpu.make_async_copy(here.at[i], there.at[i], image_sem.at[k, i])

    wanted = [(0, i) for i in range(count)] + [(1, i) for i in range(cot_count)]
    start_own(0)
    start_own(1)
    vector_copy(0).start()
    for a, i in wanted:
        y_copy(a, i).start()
    vector_copy(1).start()
    vector_here.start()
    for a, i in wanted:
        core_copy(a, i).start()
        here_copy(a, i).start()
    for w in range(4):
        own_copy(w).start()
    vector_copy(0).wait_recv()
    vector_copy(2).start()
    relay(0, codes[0])
    relay(1, codes[0])
    start_own(2)
    vector_here.wait()
    vector_copy(1).wait_recv()
    vector_copy(2).wait_recv()

    @pl.loop(0, count)
    def _(i):
        y_copy(0, i).wait_recv()
        hand_copy(0, i).start()
        here_copy(0, i).wait()
        core_copy(0, i).wait_recv()
        hand_copy(0, i).wait_recv()
        image_copy(0, i).start()
        values = source[i].astype(F32)
        middle = jnp.sum(values, axis=1, keepdims=True) / width
        square = jnp.sum(values * values, axis=1, keepdims=True) / width
        inverse = lax.rsqrt(square - middle * middle + NORM_EPS)
        low[i] = ((values - middle) * inverse * vectors[0:1, :] + vectors[1:2, :]).astype(BF16)
        image_copy(1, i).start()

        @pl.when(i == 0)
        def _():
            for code in codes[1:]:
                relay(0, code)
                relay(1, code)

    arrived(0)
    arrived(1)

    lane = lax.broadcasted_iota(jnp.int32, (1, 2 * HEAD_DIM), 1)
    key_at = lax.broadcasted_iota(jnp.int32, (1, rows), 1)
    pairs = local // (2 * HEAD_DIM)

    @pl.loop(0, count)
    def _(i):
        for c in range(3):
            cols = slice(c * local, (c + 1) * local)
            rows_out = jnp.dot(low[i], qkv_full[c], preferred_element_type=F32) + qkv_bias_ref[c : c + 1, :]
            mixed[i, :, cols] = rows_out.astype(BF16)
        image_copy(2, i).start()
        for pair_at in range(pairs):
            base = pair_at * 2 * HEAD_DIM
            queries = mixed[i, :, base : base + 2 * HEAD_DIM]
            key_rows = mixed[i, :, local + base : local + base + 2 * HEAD_DIM]
            value_rows = mixed[i, :, 2 * local + base : 2 * local + base + 2 * HEAD_DIM]
            parts = []
            for side in range(2):
                mask = (lane // HEAD_DIM) == side
                head_q = jnp.where(mask, queries, jnp.zeros_like(queries))
                scores = lax.dot_general(head_q, key_rows, NT, preferred_element_type=F32)
                scores = jnp.where(key_at < seq, scores, -1e30)
                peak = jnp.max(scores, axis=1, keepdims=True)
                powers = jnp.exp2((scores - peak) * (HEAD_DIM**-0.5 * LOG2E))
                share = 1.0 / jnp.sum(powers, axis=1, keepdims=True)
                probs_low = (powers * share).astype(BF16)
                probs[i, 2 * pair_at + side] = probs_low
                parts.append(jnp.dot(probs_low, value_rows, preferred_element_type=F32))
            joined = jnp.where((lane // HEAD_DIM) == 0, parts[0], parts[1])
            att[i, :, 2 * HEAD_DIM * pair_at : 2 * HEAD_DIM * (pair_at + 1)] = joined.astype(BF16)
        attended = att[i]
        theirs[i] = lax.dot_general(attended, out_full[2 * local :, :], NT, preferred_element_type=F32).astype(BF16)
        given_copy(i).start()
        mine[...] = lax.dot_general(attended, out_full[: 2 * local, :], NT, preferred_element_type=F32)
        given_copy(i).wait_recv()
        pair[i] = (mine[...] + given[i].astype(F32)).astype(BF16)
        pair_copy(i).start()
        image_copy(3, i).start()
        image_copy(4, i).start()

        @pl.when(i == 0)
        def _():
            relay(2, codes[0])
            start_own(3)
            relay(2, codes[1])

        @pl.when(i == 1)
        def _():
            for code in codes[2:]:
                relay(2, code)
            relay(3, codes[0])
            relay(3, codes[1])

    for code in codes[2:]:
        relay(3, code)
    outs = ((qkv_full, qkv_out), (out_full, outw_out), (vectors, vectors_out), (fc1_full, fc1_out), (fc2_full, fc2_out), (cot, cot_out), (total, total_out))

    def out_copy(k):
        return pltpu.make_async_copy(outs[k][0], outs[k][1], out_sem.at[k])

    for k in range(3):
        out_copy(k).start()
    for i in range(cot_count):
        y_copy(1, i).wait_recv()
        hand_copy(1, i).start()

    @pl.loop(0, count)
    def _(i):
        pair_copy(i).wait_recv()
        total[i, :, :local] = (pair[i, :, :local].astype(F32) + pair_in[i, :, local:].astype(F32)).astype(BF16)
        total[i, :, local : 2 * local] = (pair[i, :, local:].astype(F32) + pair_in[i, :, :local].astype(F32)).astype(BF16)
        total_copy(i).start()

        @pl.when(i == count - 2)
        def _():
            arrived(2)
            arrived(3)
            for k in range(cot_count):
                here_copy(1, k).wait()
                core_copy(1, k).wait_recv()
                hand_copy(1, k).wait_recv()
            for k in (3, 4, 5):
                out_copy(k).start()

    for i in range(count):
        total_copy(i).wait_recv()
    out_copy(6).start()
    for w in range(4):
        for code in codes:
            row_copy(w, code).wait_send()
            dp_copy(w, code).wait_send()
    for a, i in wanted:
        y_copy(a, i).wait_send()
        core_copy(a, i).wait_send()
        hand_copy(a, i).wait_send()
    for k in range(3):
        vector_copy(k).wait_send()
    for i in range(count):
        given_copy(i).wait_send()
        pair_copy(i).wait_send()
        total_copy(i).wait_send()
        for k in range(len(kinds)):
            image_copy(k, i).wait()
    for k in range(len(outs)):
        out_copy(k).wait()


def front(images, cotangent, qkv_block, out_block, fc1_block, fc2_block, vectors, qkv_bias, seq, cot_count):
    count, rows, local = images.shape
    row_count = lax.axis_size("row")
    width = 4 * local
    heads = local // HEAD_DIM
    hidden = fc1_block.shape[1]
    qkv_width = 3 * local

    def wide(*shape):
        return shape, BF16

    outs = [
        wide(count, rows, width), wide(cot_count, rows, width), wide(count, rows, width), wide(count, rows, qkv_width),
        wide(count, heads, rows, rows), wide(count, rows, local), wide(count, rows, width),
        wide(3, width, local), wide(width, local), wide(width, hidden), wide(width, hidden), ((vectors.shape[0], width), F32),
    ]
    scratch = [
        *outs[:6],
        wide(count, rows, 2 * local), wide(count, rows, 2 * local), ((rows, 2 * local), F32),
        wide(count, rows, 2 * local), wide(count, rows, 2 * local), *outs[6:],
    ]
    dma = pltpu.SemaphoreType.DMA
    whole = pl.BlockSpec(memory_space=pl.ANY)
    vmem = pl.BlockSpec(memory_space=pltpu.VMEM)
    return pl.pallas_call(
        functools.partial(front_kernel, (count, cot_count, seq, rows, local, row_count)),
        out_shape=[jax.ShapeDtypeStruct(*s) for s in outs],
        in_specs=[whole] * 7 + [vmem],
        out_specs=[whole] * len(outs),
        scratch_shapes=[pltpu.VMEM(*s) for s in scratch]
        + [dma((4, row_count))] * 4
        + [dma((4,)), dma((2, 4, count)), dma((2, 3, count)), dma((4,)), dma((3,))]
        + [dma((3, count)), dma((3, count)), dma((5, count)), dma((7,))],
        name="front",
        compiler_params=pltpu.CompilerParams(
            vmem_limit_bytes=62 * 2**20, collective_id=0, has_side_effects=True
        ),
    )(images, cotangent, qkv_block, out_block, fc1_block, fc2_block, vectors, qkv_bias)


def mlp_kernel(
    sizes,
    source_ref, total_ref, cot_ref, own_cot_ref, fc1_ref, fc2_ref, vectors_ref, fc1_bias_ref, fc2_bias_ref,
    grad_out, cot_out, move_out, kept_out, fc1_grad_out, fc2_half_out, bias_out,
    source, total, cot, fc1, fc2, low, active, gelu_grad, theirs, given, mine, pair, pair_in, grad_low,
    move_theirs, move_given, kept, move, fc1_grad, fc2_grad, dp_in, fc2_half,
    load_sem, in_send, in_recv, sum_send, sum_recv, move_send, move_recv, dp_send, dp_recv, out_sem,
):
    count, rows, local, row_count = sizes
    dp, row, place = lax.axis_index("dp"), lax.axis_index("row"), lax.axis_index("col")
    core_at = {"col": place + 1 - 2 * (place % 2)}
    y_at = {"col": (place + 2) % 4}
    dp_at = {"dp": 1 - dp}
    greet([core_at, y_at, dp_at])
    width = 4 * local
    hidden_width = fc1.shape[1]
    block = width // row_count

    cot_count = cot_ref.shape[0]

    def load(k, i):
        here, there = ((source_ref, source), (total_ref, total), (cot_ref, cot))[k]
        return pltpu.make_async_copy(here.at[i], there.at[i], load_sem.at[k, i])

    fc1_load = pltpu.make_async_copy(fc1_ref, fc1, load_sem.at[3, 0])
    fc2_load = pltpu.make_async_copy(fc2_ref, fc2, load_sem.at[3, 1])
    def y_copy(i):
        return copy_to(own_cot_ref.at[i], cot.at[i, :, pl.ds(local, local)], in_send.at[0, i], in_recv.at[0, i], y_at)

    def core_copy(i):
        return copy_to(own_cot_ref.at[i], cot.at[i, :, pl.ds(2 * local, local)], in_send.at[1, i], in_recv.at[1, i], core_at)

    def hand_copy(i):
        return copy_to(
            cot.at[i, :, pl.ds(local, local)],
            cot.at[i, :, pl.ds(3 * local, local)],
            in_send.at[2, i],
            in_recv.at[2, i],
            core_at,
        )

    def here_copy(i):
        return pltpu.make_async_copy(own_cot_ref.at[i], cot.at[i, :, pl.ds(0, local)], load_sem.at[2, i])

    for i in range(cot_count, count):
        y_copy(i).start()
    for i in range(count):
        for k in range(2 + (i < cot_count)):
            load(k, i).start()
        if i == 0:
            fc1_load.start()
            fc2_load.start()
        if i >= cot_count:
            core_copy(i).start()
            here_copy(i).start()

    def given_copy(i):
        return copy_to(theirs.at[i], given.at[i], sum_send.at[0, i], sum_recv.at[0, i], core_at)

    def pair_copy(i):
        return copy_to(pair.at[i], pair_in.at[i], sum_send.at[1, i], sum_recv.at[1, i], y_at)

    def total_copy(i):
        return copy_to(
            grad_low.at[i, :, pl.ds(0, 2 * local)],
            grad_low.at[i, :, pl.ds(2 * local, 2 * local)],
            sum_send.at[2, i],
            sum_recv.at[2, i],
            core_at,
        )

    def move_copy(i):
        return copy_to(move_theirs.at[i], move_given.at[i], move_send.at[i], move_recv.at[i], core_at)

    def dp_copy(d):
        there = row_place((row + d) % row_count, row_count, place, block)
        return copy_to(
            fc2_grad.at[there, other_half_of(dp, hidden_width)], dp_in.at[there, :], dp_send.at[d], dp_recv.at[d], dp_at
        )

    bias_out[...] = jnp.zeros_like(bias_out)
    step = hidden_width // 4
    fc1_load.wait()
    fc2_load.wait()

    @pl.loop(0, count)
    def _(i):
        for k in range(2):
            load(k, i).wait()

        @pl.when(i < cot_count)
        def _():
            load(2, i).wait()

        @pl.when(i >= cot_count)
        def _():
            y_copy(i).wait_recv()
            hand_copy(i).start()
            here_copy(i).wait()
            core_copy(i).wait_recv()
            hand_copy(i).wait_recv()

        values = source[i].astype(F32) + total[i].astype(F32) + vectors_ref[4:5, :]
        kept[i] = values[:, :local] + fc2_bias_ref[...]
        middle = jnp.sum(values, axis=1, keepdims=True) / width
        square = jnp.sum(values * values, axis=1, keepdims=True) / width
        inverse = lax.rsqrt(square - middle * middle + NORM_EPS)
        low[i] = ((values - middle) * inverse * vectors_ref[2:3, :] + vectors_ref[3:4, :]).astype(BF16)
        bias_out[1:2, :local] += jnp.sum(cot[i, :, :local].astype(F32), axis=0, keepdims=True)
        for part in range(4):
            cols = slice(part * step, (part + 1) * step)
            pre_act = jnp.dot(low[i], fc1[:, cols], preferred_element_type=F32) + fc1_bias_ref[:, cols]
            gate = 0.5 * (1.0 + lax.erf(pre_act * ROOT_HALF))
            active[i, :, cols] = (pre_act * gate).astype(BF16)
            slope = gate + pre_act * jnp.exp(-0.5 * pre_act * pre_act) / ROOT_TWO_PI
            grad_pre = jnp.dot(cot[i], fc2[:, cols], preferred_element_type=F32) * slope
            bias_out[0:1, cols] += jnp.sum(grad_pre, axis=0, keepdims=True)
            gelu_grad[i, :, cols] = grad_pre.astype(BF16)
        theirs[i] = lax.dot_general(gelu_grad[i], fc1[2 * local :, :], NT, preferred_element_type=F32).astype(BF16)
        given_copy(i).start()
        mine[...] = lax.dot_general(gelu_grad[i], fc1[: 2 * local, :], NT, preferred_element_type=F32)
        given_copy(i).wait_recv()
        pair[i] = (mine[...] + given[i].astype(F32)).astype(BF16)
        pair_copy(i).start()

    def weight_grad(out, left, right):
        for part in range(4):
            span = slice(part * local, (part + 1) * local)
            terms = [
                lax.dot_general(left[i, :, span], right[i], TN, preferred_element_type=F32) for i in range(count)
            ]
            out[span, :] = sum(terms[1:], terms[0]).astype(BF16)

    weight_grad(fc2_grad, cot, active)
    for d in range(row_count):
        dp_copy((d + 1) % row_count).start()

    @pl.loop(0, count)
    def _(i):
        move_theirs[i] = lax.dot_general(active[i], fc2[2 * local :, :], NT, preferred_element_type=F32).astype(BF16)
        move_copy(i).start()
        mine[...] = lax.dot_general(active[i], fc2[: 2 * local, :], NT, preferred_element_type=F32)
        move_copy(i).wait_recv()
        kept[i] += mine[:, :local] + move_given[i, :, :local].astype(F32)
        move[i] = (mine[:, local:] + move_given[i, :, local:].astype(F32)).astype(BF16)

    weight_grad(fc1_grad, low, gelu_grad)
    outs = ((move, move_out), (kept, kept_out), (fc1_grad, fc1_grad_out), (cot, cot_out))
    for k, (here, there) in enumerate(outs):
        pltpu.make_async_copy(here, there, out_sem.at[k]).start()

    @pl.loop(0, count)
    def _(i):
        pair_copy(i).wait_recv()
        grad_low[i, :, :local] = (pair[i, :, :local].astype(F32) + pair_in[i, :, local:].astype(F32)).astype(BF16)
        grad_low[i, :, local : 2 * local] = (
            pair[i, :, local:].astype(F32) + pair_in[i, :, :local].astype(F32)
        ).astype(BF16)
        total_copy(i).start()

    for d in range(row_count):
        dp_copy((d + 1) % row_count).wait_recv()
    fc2_half[...] = (
        fc2_grad[:, half_of(dp, hidden_width)].astype(F32) + dp_in[...].astype(F32)
    ).astype(BF16)
    for i in range(count):
        total_copy(i).wait_recv()
    more = ((fc2_half, fc2_half_out), (grad_low, grad_out))
    for k, (here, there) in enumerate(more):
        pltpu.make_async_copy(here, there, out_sem.at[len(outs) + k]).start()
    for i in range(count):
        given_copy(i).wait_send()
        pair_copy(i).wait_send()
        total_copy(i).wait_send()
        move_copy(i).wait_send()
    for i in range(cot_count, count):
        y_copy(i).wait_send()
        core_copy(i).wait_send()
        hand_copy(i).wait_send()
    for d in range(row_count):
        dp_copy(d).wait_send()
    for k, (here, there) in enumerate((*outs, *more)):
        pltpu.make_async_copy(here, there, out_sem.at[k]).wait()


def mlp(source, total, cot, own_cot, fc1, fc2, vectors, fc1_bias, fc2_bias):
    count, rows, width = source.shape
    local = width // 4
    row_count = lax.axis_size("row")
    hidden = fc1.shape[1]
    outs = [
        ((count, rows, width), BF16), ((count, rows, width), BF16), ((count, rows, local), BF16), ((count, rows, local), F32),
        ((width, hidden), BF16), ((width, hidden // 2), BF16), ((2, hidden), F32),
    ]
    all_wide = ((count, rows, width), BF16)
    all_pair = ((count, rows, 2 * local), BF16)
    scratch = [
        all_wide, all_wide, all_wide, ((width, hidden), BF16), ((width, hidden), BF16), all_wide,
        ((count, rows, hidden), BF16), ((count, rows, hidden), BF16),
        all_pair, all_pair, ((rows, 2 * local), F32), all_pair, all_pair, all_wide,
        all_pair, all_pair, ((count, rows, local), F32), ((count, rows, local), BF16),
        ((width, hidden), BF16), ((width, hidden), BF16), ((width, hidden // 2), BF16), ((width, hidden // 2), BF16),
    ]
    dma = pltpu.SemaphoreType.DMA
    whole = pl.BlockSpec(memory_space=pl.ANY)
    vmem = pl.BlockSpec(memory_space=pltpu.VMEM)
    return pl.pallas_call(
        functools.partial(mlp_kernel, (count, rows, local, row_count)),
        out_shape=[jax.ShapeDtypeStruct(*s) for s in outs],
        in_specs=[whole] * 6 + [vmem] * 3,
        out_specs=[whole] * 6 + [vmem],
        scratch_shapes=[pltpu.VMEM(*s) for s in scratch]
        + [dma((4, count))] + [dma((3, count))] * 4 + [dma((count,)), dma((count,))]
        + [dma((row_count,)), dma((row_count,)), dma((6,))],
        name="mlp",
        compiler_params=pltpu.CompilerParams(
            vmem_limit_bytes=62 * 2**20, collective_id=1, has_side_effects=True
        ),
    )(source, total, cot, own_cot, fc1, fc2, vectors, fc1_bias, fc2_bias)


def back_kernel(
    sizes,
    source_ref, total_ref, cot_ref, grad_ref, mixed_ref, probs_ref, att_ref, low_ref, move_ref, kept_ref,
    qkv_ref, outw_ref, fc1_grad_ref, fc2_half_ref, vectors_ref, mlp_bias_ref,
    images_out, images_grad_out, small_out, qkv_out, outw_out, fc1_out, fc2_out,
    source, total, cot, grad_in, mixed, probs, att, low,
    hidden_low, mixed_grad, grad_hidden, normed1, inverse1, qkv_sum, outw_sum, k_turned, v_turned,
    theirs, given, mine, kept_grad, send, got, stat, stat_given, stat_pair, stat_in,
    move_in, kept, finished, qkv, outw, qkv_grad, outw_grad, small, small_in,
    half_fc2, half_fc1, half_outw, half_qkv, dp_fc1, dp_outw, dp_qkv,
    row_fc2, row_fc1, row_outw, row_qkv, tot_fc2, tot_fc1, tot_outw, tot_qkv,
    early_sem, late_sem, once_sem, sum_send, sum_recv, move_send, move_recv, small_send, small_recv,
    dp_send, dp_recv, row_send, row_recv, tot_send, tot_recv, out_sem,
):
    count, rows, local, row_count = sizes
    dp, row, place = lax.axis_index("dp"), lax.axis_index("row"), lax.axis_index("col")
    core_at = {"col": place + 1 - 2 * (place % 2)}
    y_at = {"col": (place + 2) % 4}
    dp_at = {"dp": 1 - dp}
    rounds = [dp_at]
    distance = 1
    while distance < row_count:
        rounds.append({"row": crossed(row, distance)})
        distance *= 2
    greet([core_at, y_at] + rounds)
    width = 4 * local
    block = width // row_count
    two = 2 * HEAD_DIM
    scale = HEAD_DIM**-0.5

    early = ((source_ref, source), (total_ref, total), (cot_ref, cot), (grad_ref, grad_in))
    late = ((mixed_ref, mixed), (probs_ref, probs), (att_ref, att), (low_ref, low))

    def early_load(k, i):
        here, there = early[k]
        return pltpu.make_async_copy(here.at[i], there.at[i % 2] if k == 0 else there, early_sem.at[k])

    def late_load(k, i):
        here, there = late[k]
        return pltpu.make_async_copy(here.at[i], there, late_sem.at[k])

    once = (
        (outw_ref, outw), (qkv_ref, qkv), (fc2_half_ref, half_fc2),
        (fc1_grad_ref.at[:, half_of(dp, fc1_grad_ref.shape[1])], half_fc1), (kept_ref, kept),
    )

    def once_load(k):
        return pltpu.make_async_copy(once[k][0], once[k][1], once_sem.at[k])

    grads = (None, fc1_grad_ref, outw_grad, qkv_grad)
    halves = (half_fc2, half_fc1, half_outw, half_qkv)
    dp_ins = (None, dp_fc1, dp_outw, dp_qkv)
    row_ins = (row_fc2, row_fc1, row_outw, row_qkv)
    tots = (tot_fc2, tot_fc1, tot_outw, tot_qkv)

    codes = sorted(range(1, row_count), key=lambda code: (code & -code, -code)) + [0]

    def rows_at(code):
        return row_place(crossed(row, code), row_count, place, block)

    def dp_copy(w, code):
        full = grads[w]
        return copy_to(
            part_at(full, rows_at(code), other_half_of(dp, full.shape[-1])),
            part_at(dp_ins[w], rows_at(code), slice(None)),
            dp_send.at[w, code],
            dp_recv.at[w, code],
            dp_at,
        )

    def row_copy(w, code):
        return copy_to(
            part_at(halves[w], rows_at(code), slice(None)),
            row_ins[w].at[code],
            row_send.at[w, code],
            row_recv.at[w, code],
            {"row": crossed(row, code & -code)},
        )

    def tot_copy(w):
        part = part_at(tots[w], slice(None), half_of(dp, tots[w].shape[-1]))
        return copy_to(part, part, tot_send.at[w], tot_recv.at[w], dp_at)

    def add_to(w, code, term):
        at = (slice(None), rows_at(code), slice(None)) if len(halves[w].shape) == 3 else (rows_at(code), slice(None))
        halves[w][at] = (halves[w][at].astype(F32) + term.astype(F32)).astype(BF16)

    def dp_sum(w, code):
        dp_copy(w, code).wait_recv()
        at = (slice(None), rows_at(code), slice(None)) if len(halves[w].shape) == 3 else (rows_at(code), slice(None))
        add_to(w, code, dp_ins[w][at])

    def row_take(w, code):
        row_copy(w, code).wait_recv()
        add_to(w, code - (code & -code), row_ins[w][code])

    def row_first(w):
        for code in codes[:-1]:
            if code % 2:
                row_copy(w, code).start()

    def row_next(w):
        for code in codes[:-1]:
            if code % 2 == 0:
                far = 1
                while far < code & -code:
                    row_take(w, code + far)
                    far *= 2
                row_copy(w, code).start()

    def row_last(w):
        far = 1
        while far < row_count:
            row_take(w, far)
            far *= 2
        own = halves[w][:, rows_at(0), :] if len(halves[w].shape) == 3 else halves[w][rows_at(0), :]
        cols = half_of(dp, tots[w].shape[-1])
        if len(halves[w].shape) == 3:
            tots[w][:, :, cols] = own
        else:
            tots[w][:, cols] = own
        tot_copy(w).start()

    def given_copy(i):
        return copy_to(theirs.at[i], given.at[i], sum_send.at[0, i], sum_recv.at[0, i], core_at)

    def stat_copy(i):
        return copy_to(stat.at[i], stat_given.at[i], sum_send.at[1, i], sum_recv.at[1, i], core_at)

    def got_copy(i):
        return copy_to(send.at[i], got.at[i], sum_send.at[2, i], sum_recv.at[2, i], y_at)

    def stat_pair_copy(i):
        return copy_to(stat_pair.at[i], stat_in.at[i], sum_send.at[3, i], sum_recv.at[3, i], y_at)

    def move_copy(i):
        return copy_to(move_ref.at[i], move_in.at[i], move_send.at[i], move_recv.at[i], y_at)

    def small_copy(s):
        return copy_to(small.at[s], small_in.at[s], small_send.at[s], small_recv.at[s], rounds[s])

    for k in range(4):
        early_load(k, 0).start()
    for k in range(len(once)):
        once_load(k).start()
    for k in range(4):
        late_load(k, 0).start()
    for i in range(count):
        move_copy(i).start()
    for code in codes:
        dp_copy(1, code).start()

    small[0] = jnp.zeros_like(small[0])
    small[0, 7:8, :] = mlp_bias_ref[1:2, :local]
    for part in range(mlp_bias_ref.shape[1] // local):
        small[0, 8 + part : 9 + part, :] = mlp_bias_ref[0:1, part * local : (part + 1) * local]
    qkv_sum[...] = jnp.zeros_like(qkv_sum)
    outw_sum[...] = jnp.zeros_like(outw_sum)
    once_load(0).wait()
    once_load(1).wait()
    once_load(2).wait()
    row_first(0)

    def product_of(span):
        terms = [
            lax.dot_general(mixed_grad[:, c * local : (c + 1) * local], qkv[c, span, :], NT, preferred_element_type=F32)
            for c in range(3)
        ]
        return terms[0] + terms[1] + terms[2]

    lane = lax.broadcasted_iota(jnp.int32, (1, two), 1)
    down = lax.broadcasted_iota(jnp.int32, (two, two), 0)
    across = lax.broadcasted_iota(jnp.int32, (two, two), 1)
    eye = (down == across).astype(BF16)

    @pl.loop(0, count)
    def _(i):
        for k in range(4):
            early_load(k, i).wait()
        values = source[i % 2].astype(F32) + total[...].astype(F32) + vectors_ref[4:5, :]
        middle = jnp.sum(values, axis=1, keepdims=True) / width
        square = jnp.sum(values * values, axis=1, keepdims=True) / width
        inverse = lax.rsqrt(square - middle * middle + NORM_EPS)
        normed = (values - middle) * inverse
        grad = grad_in[...].astype(F32)
        small[0, 5:6, :] += jnp.sum(grad[:, :local] * normed[:, :local], axis=0, keepdims=True)
        small[0, 6:7, :] += jnp.sum(grad[:, :local], axis=0, keepdims=True)
        scaled = grad * vectors_ref[2:3, :]
        first = jnp.sum(scaled, axis=1, keepdims=True) / width
        second = jnp.sum(scaled * normed, axis=1, keepdims=True) / width
        whole_grad = cot[...].astype(F32) + inverse * (scaled - first - normed * second)
        grad_hidden[i] = whole_grad[:, :local]
        small[0, 2:3, :] += jnp.sum(whole_grad[:, :local], axis=0, keepdims=True)
        hidden_low[...] = whole_grad.astype(BF16)

        @pl.when(i + 1 < count)
        def _():
            for k in range(4):
                early_load(k, i + 1).start()

        for k in range(4):
            late_load(k, i).wait()
        grad_att = jnp.dot(hidden_low[...], outw[...], preferred_element_type=F32).astype(BF16)
        for part in range(4):
            span = slice(part * local, (part + 1) * local)
            outw_sum[span, :] += lax.dot_general(hidden_low[:, span], att[...], TN, preferred_element_type=F32)
        for pair in range(local // two):
            base = pair * two
            cols = slice(pair * two, (pair + 1) * two)
            queries = mixed[:, cols]
            key_rows = mixed[:, local + base : local + base + two]
            value_rows = mixed[:, 2 * local + base : 2 * local + base + two]
            pair_grad = grad_att[:, cols]
            q_turned = lax.dot_general(eye, queries, NT, preferred_element_type=F32).astype(BF16)
            grad_turned = lax.dot_general(eye, pair_grad, NT, preferred_element_type=F32).astype(BF16)
            product = pair_grad.astype(F32) * att[:, cols].astype(F32)
            parts = []
            for side in range(2):
                mask = (lane // HEAD_DIM) == side
                turn = slice(side * HEAD_DIM, (side + 1) * HEAD_DIM)
                head_grad = jnp.where(mask, pair_grad, jnp.zeros_like(pair_grad))
                grad_probs = lax.dot_general(head_grad, value_rows, NT, preferred_element_type=F32)
                delta = jnp.sum(jnp.where(mask, product, 0.0), axis=1, keepdims=True)
                probs_low = probs[2 * pair + side]
                grad_scores = (probs_low.astype(F32) * (grad_probs - delta)).astype(BF16)
                parts.append(jnp.dot(grad_scores, key_rows, preferred_element_type=F32))
                k_turned[turn, :] = jnp.dot(q_turned[turn, :], grad_scores, preferred_element_type=F32)
                v_turned[turn, :] = jnp.dot(grad_turned[turn, :], probs_low, preferred_element_type=F32)
            q_grad = jnp.where((lane // HEAD_DIM) == 0, parts[0], parts[1]) * scale
            v_grad = v_turned[...].T
            mixed_grad[:, cols] = q_grad.astype(BF16)
            mixed_grad[:, local + base : local + base + two] = (k_turned[...].T * scale).astype(BF16)
            mixed_grad[:, 2 * local + base : 2 * local + base + two] = v_grad.astype(BF16)
            small[0, 0:1, cols] += jnp.sum(q_grad, axis=0, keepdims=True)
            small[0, 1:2, cols] += jnp.sum(v_grad, axis=0, keepdims=True)
        values = source[i % 2].astype(F32)
        middle = jnp.sum(values, axis=1, keepdims=True) / width
        square = jnp.sum(values * values, axis=1, keepdims=True) / width
        inverse = lax.rsqrt(square - middle * middle + NORM_EPS)
        normed = (values - middle) * inverse
        normed1[i] = normed[:, :local]
        inverse1[i] = inverse
        scaled_in = normed * vectors_ref[0:1, :]
        far = product_of(slice(2 * local, 4 * local))
        theirs[i] = far.astype(BF16)
        given_copy(i).start()
        near = product_of(slice(0, 2 * local))
        mine[...] = near
        first = jnp.sum(far * vectors_ref[0:1, 2 * local :], axis=1, keepdims=True) + jnp.sum(
            near * vectors_ref[0:1, : 2 * local], axis=1, keepdims=True
        )
        second = jnp.sum(far * scaled_in[:, 2 * local :], axis=1, keepdims=True) + jnp.sum(
            near * scaled_in[:, : 2 * local], axis=1, keepdims=True
        )
        spread = jnp.where(lane == 0, first, jnp.where(lane == 1, second, 0.0))
        stat[i] = spread.T[:8, :]
        stat_copy(i).start()
        for part in range(4):
            span = slice(part * local, (part + 1) * local)
            term = lax.dot_general(low[:, span], mixed_grad[...], TN, preferred_element_type=F32)
            for c in range(3):
                qkv_sum[c, span, :] += term[:, c * local : (c + 1) * local]

        @pl.when(i + 1 < count)
        def _():
            for k in range(4):
                late_load(k, i + 1).start()

        given_copy(i).wait_recv()
        kept_grad[i] = mine[:, :local] + given[i, :, :local].astype(F32)
        send[i] = (mine[:, local:] + given[i, :, local:].astype(F32)).astype(BF16)
        got_copy(i).start()
        stat_copy(i).wait_recv()
        stat_pair[i] = stat[i] + stat_given[i]
        stat_pair_copy(i).start()

        @pl.when(i == 0)
        def _():
            row_next(0)
            once_load(3).wait()

        @pl.when(i == 1)
        def _():
            for code in codes:
                dp_sum(1, code)
                if code % 2:
                    row_copy(1, code).start()
            row_last(0)

    outw_grad[...] = outw_sum[...].astype(BF16)
    half_outw[...] = outw_grad[:, half_of(dp, local)]
    for code in codes:
        dp_copy(2, code).start()
    qkv_grad[...] = qkv_sum[...].astype(BF16)
    half_qkv[...] = qkv_grad[:, :, half_of(dp, local)]
    for code in codes:
        dp_copy(3, code).start()
    row_next(1)
    once_load(4).wait()

    @pl.loop(0, count)
    def _(i):
        move_copy(i).wait_recv()
        finished[i] = (kept[i] + move_in[i].astype(F32)).astype(BF16)

    for w in (2, 3):
        for code in codes:
            if code % 2:
                dp_sum(w, code)
                row_copy(w, code).start()
    row_last(1)

    @pl.loop(0, count)
    def _(i):
        got_copy(i).wait_recv()
        stat_pair_copy(i).wait_recv()
        sums = stat_pair[i] + stat_in[i]
        spread = jnp.concatenate([sums, jnp.zeros((two - 8, rows), F32)], axis=0).T / width
        grad = kept_grad[i] + got[i].astype(F32)
        small[0, 3:4, :] += jnp.sum(grad * normed1[i], axis=0, keepdims=True)
        small[0, 4:5, :] += jnp.sum(grad, axis=0, keepdims=True)
        scaled = grad * vectors_ref[0:1, :local]
        grad_hidden[i] += inverse1[i] * (scaled - spread[:, 0:1] - normed1[i] * spread[:, 1:2])

    pltpu.make_async_copy(finished, images_out, out_sem.at[0]).start()
    pltpu.make_async_copy(grad_hidden, images_grad_out, out_sem.at[1]).start()
    small_copy(0).start()
    for w in (2, 3):
        for code in codes:
            if code % 2 == 0:
                dp_sum(w, code)
        row_next(w)
    for s in range(len(rounds)):
        small_copy(s).wait_recv()
        small[s + 1] = small[s] + small_in[s]
        if s + 1 < len(rounds):
            small_copy(s + 1).start()
    row_last(2)
    row_last(3)
    outs = ((tot_fc2, fc2_out), (tot_fc1, fc1_out), (tot_outw, outw_out), (tot_qkv, qkv_out))
    for w, (here, there) in enumerate(outs):
        tot_copy(w).wait_recv()
        pltpu.make_async_copy(here, there, out_sem.at[2 + w]).start()
    small_out[...] = small[len(rounds)]
    for i in range(count):
        given_copy(i).wait_send()
        stat_copy(i).wait_send()
        got_copy(i).wait_send()
        stat_pair_copy(i).wait_send()
        move_copy(i).wait_send()
    for s in range(len(rounds)):
        small_copy(s).wait_send()
    for w in range(4):
        tot_copy(w).wait_send()
        for code in codes:
            if w:
                dp_copy(w, code).wait_send()
            if code:
                row_copy(w, code).wait_send()
    for k, (here, there) in enumerate(((finished, images_out), (grad_hidden, images_grad_out), *outs)):
        pltpu.make_async_copy(here, there, out_sem.at[k]).wait()


def back(
    source, total, cot, grad_low, mixed, probs, att, low, move, kept, qkv, outw, fc1_grad, fc2_half, vectors, mlp_bias
):
    count, rows, width = source.shape
    local = width // 4
    row_count = lax.axis_size("row")
    block = width // row_count
    hidden = fc1_grad.shape[1]
    qkv_width = 3 * local
    heads = local // HEAD_DIM
    rounds = row_count.bit_length()
    outs = [
        ((count, rows, local), BF16), ((count, rows, local), F32), ((16, local), F32),
        ((3, block, local), BF16), ((block, local), BF16), ((block, hidden), BF16), ((block, hidden), BF16),
    ]
    own_f32 = ((count, rows, local), F32)
    own_low = ((count, rows, local), BF16)
    pair_low = ((count, rows, 2 * local), BF16)
    stat = ((count, 8, rows), F32)
    wide = ((rows, width), BF16)
    turned = ((2 * HEAD_DIM, rows), F32)
    columns = (((), hidden), ((), hidden), ((), local), ((3,), local))
    scratch = [
        ((2, rows, width), BF16), wide, wide, wide, ((rows, qkv_width), BF16), ((heads, rows, rows), BF16), ((rows, local), BF16), wide,
        wide, ((rows, qkv_width), BF16), own_f32, own_f32, ((count, rows, 1), F32),
        ((3, width, local), F32), ((width, local), F32), turned, turned,
        pair_low, pair_low, ((rows, 2 * local), F32), own_f32, own_low, own_low, stat, stat, stat, stat,
        own_low, own_f32, own_low, ((3, width, local), BF16), ((width, local), BF16),
        ((3, width, local), BF16), ((width, local), BF16), ((rounds + 1, 16, local), F32), ((rounds, 16, local), F32),
        *[((*lead, width, c // 2), BF16) for lead, c in columns],
        *[((*lead, width, c // 2), BF16) for lead, c in columns[1:]],
        *[((row_count, *lead, block, c // 2), BF16) for lead, c in columns],
        *[((*lead, block, c), BF16) for lead, c in columns],
    ]
    dma = pltpu.SemaphoreType.DMA
    whole = pl.BlockSpec(memory_space=pl.ANY)
    vmem = pl.BlockSpec(memory_space=pltpu.VMEM)
    return pl.pallas_call(
        functools.partial(back_kernel, (count, rows, local, row_count)),
        out_shape=[jax.ShapeDtypeStruct(*s) for s in outs],
        in_specs=[whole] * 14 + [vmem] * 2,
        out_specs=[whole, whole, vmem] + [whole] * 4,
        scratch_shapes=[pltpu.VMEM(*s) for s in scratch]
        + [dma((4,)), dma((4,)), dma((5,)), dma((4, count)), dma((4, count)), dma((count,)), dma((count,)), dma((rounds,)), dma((rounds,))]
        + [dma((4, row_count))] * 4
        + [dma((4,)), dma((4,)), dma((6,))],
        name="back",
        compiler_params=pltpu.CompilerParams(
            vmem_limit_bytes=63 * 2**20, collective_id=2, has_side_effects=True
        ),
    )(source, total, cot, grad_low, mixed, probs, att, low, move, kept, qkv, outw, fc1_grad, fc2_half, vectors, mlp_bias)


def adam_step(weight, grad, momentum, variance):
    moment_new = BETA_FIRST * momentum + (1.0 - BETA_FIRST) * grad
    second_new = BETA_SECOND * variance + (1.0 - BETA_SECOND) * grad * grad
    corrected = moment_new / (1.0 - BETA_FIRST**STEP)
    second_corrected = second_new / (1.0 - BETA_SECOND**STEP)
    master = weight.astype(jnp.float32)
    updated = master - LEARN_RATE * (
        corrected / (jnp.sqrt(second_corrected) + ADAM_EPS) + WEIGHT_DECAY * master
    )
    return (updated, moment_new, second_new)


def per_device(
    images_in,
    cotangent,
    first_gain,
    first_shift,
    second_gain,
    second_shift,
    qkv_weight,
    qv_bias,
    out_weight,
    out_bias,
    fc1_weight,
    fc1_bias,
    fc2_weight,
    fc2_bias,
    qkv_momentum,
    qkv_variance,
    out_momentum,
    out_variance,
    fc1_momentum,
    fc1_variance,
    fc2_momentum,
    fc2_variance,
):
    image_count, seq, local = images_in.shape
    width = 4 * local
    rows = -(-seq // ROW_TILE) * ROW_TILE
    place = lax.axis_index("col")

    vectors = jnp.pad(jnp.stack([first_gain, first_shift, second_gain, second_shift, out_bias]), ((0, 3), (0, 0)))
    qkv_shift = jnp.stack([qv_bias[0], jnp.zeros_like(qv_bias[0]), qv_bias[1]])
    own_cot = jnp.pad(cotangent, ((0, 0), (0, rows - seq), (0, 0)))
    (source_all, cot_first, low_all, mixed_all, probs_all, att_all, total_all, qkv_full, out_full, fc1_full, fc2_full, vectors) = front(
        jnp.pad(images_in, ((0, 0), (0, rows - seq), (0, 0))),
        own_cot,
        qkv_weight.transpose(1, 0, 2),
        out_weight,
        fc1_weight,
        fc2_weight,
        vectors,
        qkv_shift,
        seq,
        min(2, image_count),
    )
    grad_low2, cot_all, move, kept, fc1_grad, fc2_half, mlp_bias = mlp(
        source_all, total_all, cot_first, own_cot, fc1_full, fc2_full,
        vectors, fc1_bias[None], fc2_bias[None],
    )
    images_out, images_grad, small, qkv_total, out_total, fc1_total, fc2_total = back(
        source_all, total_all, cot_all, grad_low2, mixed_all, probs_all, att_all, low_all, move, kept,
        qkv_full, out_full, fc1_grad, fc2_half, vectors, mlp_bias,
    )
    qkv_total = qkv_total.transpose(1, 0, 2).astype(F32)
    out_total, fc1_total, fc2_total = (t.astype(F32) for t in (out_total, fc1_total, fc2_total))
    qkv_new = adam_step(qkv_weight, qkv_total, qkv_momentum, qkv_variance)
    out_new = adam_step(out_weight, out_total, out_momentum, out_variance)
    fc1_new = adam_step(fc1_weight, fc1_total, fc1_momentum, fc1_variance)
    fc2_new = adam_step(fc2_weight, fc2_total, fc2_momentum, fc2_variance)
    return (
        images_out[:, :seq],
        images_grad[:, :seq],
        qkv_total,
        out_total,
        fc1_total,
        fc2_total,
        small[0:2],
        small[2],
        small[8:12].reshape(-1),
        small[7],
        small[3],
        small[4],
        small[5],
        small[6],
        qkv_new[0],
        out_new[0],
        fc1_new[0],
        fc2_new[0],
        qkv_new[1],
        out_new[1],
        fc1_new[1],
        fc2_new[1],
        qkv_new[2],
        out_new[2],
        fc1_new[2],
        fc2_new[2],
    )


def solution(mesh):
    return jax.shard_map(
        per_device,
        mesh=mesh,
        in_specs=(
            P(("dp", "row"), None, "col"),
            P(("dp", "row"), None, "col"),
            P("col"),
            P("col"),
            P("col"),
            P("col"),
            P("row", None, "col"),
            P(None, "col"),
            P("row", "col"),
            P("col"),
            P("row", "col"),
            P("col"),
            P("row", "col"),
            P("col"),
            P("row", None, "col"),
            P("row", None, "col"),
            P("row", "col"),
            P("row", "col"),
            P("row", "col"),
            P("row", "col"),
            P("row", "col"),
            P("row", "col"),
        ),
        out_specs=(
            P(("dp", "row"), None, "col"),
            P(("dp", "row"), None, "col"),
            P("row", None, "col"),
            P("row", "col"),
            P("row", "col"),
            P("row", "col"),
            P(None, "col"),
            P("col"),
            P("col"),
            P("col"),
            P("col"),
            P("col"),
            P("col"),
            P("col"),
            P("row", None, "col"),
            P("row", "col"),
            P("row", "col"),
            P("row", "col"),
            P("row", None, "col"),
            P("row", "col"),
            P("row", "col"),
            P("row", "col"),
            P("row", None, "col"),
            P("row", "col"),
            P("row", "col"),
            P("row", "col"),
        ),
        check_vma=False,
    )
```

```python
import functools

import jax
import jax.numpy as jnp
from jax import lax
from jax.experimental import pallas as pl
from jax.experimental.pallas import tpu as pltpu
from jax.sharding import PartitionSpec as P

HEAD_DIM = 64
STEP = 3


NORM_EPS = 1e-06
LEARN_RATE = 0.02
BETA_FIRST = 0.9
BETA_SECOND = 0.999
ADAM_EPS = 1e-08
WEIGHT_DECAY = 0.05
ROOT_HALF = 0.7071067811865476
ROOT_TWO_PI = 2.5066282746310002
LOG2E = 1.4426950408889634
ROW_TILE = 16
MESH = pl.DeviceIdType.MESH
NT = (((1,), (1,)), ((), ()))
TN = (((0,), (0,)), ((), ()))
F32 = jnp.float32
BF16 = jnp.bfloat16


def copy_to(src, dst, send, recv, where):
    return pltpu.make_async_remote_copy(
        src_ref=src, dst_ref=dst, send_sem=send, recv_sem=recv, device_id=where, device_id_type=MESH
    )


def rel_place(quarter, place):
    return (quarter // 2 + place // 2) % 2 + 2 * ((quarter % 2 + place % 2) % 2)


def crossed(row, code):
    distance = 1
    while distance <= code:
        if code & distance:
            row = row + distance * (1 - 2 * ((row // distance) % 2))
        distance *= 2
    return row


def half_of(dp, full_width):
    half = full_width // 2
    return pl.ds(pl.multiple_of(dp * half, half), half)


def other_half_of(dp, full_width):
    half = full_width // 2
    return pl.ds(pl.multiple_of((1 - dp) * half, half), half)


def row_place(owner, row_count, place, block):
    per = row_count // 4
    at = (rel_place(owner // per, place) * per + owner % per) * block
    return pl.ds(pl.multiple_of(at, block), block)


def part_at(full, rows, cols):
    return full.at[:, rows, cols] if len(full.shape) == 3 else full.at[rows, cols]


def greet(partners):
    barrier = pltpu.get_barrier_semaphore()
    for partner in partners:
        pl.semaphore_signal(barrier, inc=1, device_id=partner, device_id_type=MESH)
    pl.semaphore_wait(barrier, len(partners))


def ahead_kernel(
    sizes,
    images_ref, cot_ref, qkv_ref, out_ref, fc1_ref, fc2_ref, vectors_ref, qkv_bias_ref, fc1_bias_ref, fc2_bias_ref,
    source_out, cot_out, low_out, mixed_out, probs_out, att_out, total_out, grad_out, qkv_out, outw_out, vectors_out,
    move_out, kept_out, fc1_grad_out, fc2_half_out, bias_out,
    source, cot, low, mixed, probs, att, theirs, given, mine, pair, pair_in, total, qkv_full, out_full, fc1_full, fc2_full, vectors,
    active, gelu_grad, grad_in, move_given, kept, move, fc1_grad, fc2_grad, dp_in, fc2_half,
    row_send, row_recv, dp_send, dp_recv, own_sem, in_send, in_recv, vec_send, vec_recv, sum_send, sum_recv, image_sem, out_sem,
    back_send, back_recv, half_send, half_recv,
):
    count, seq, rows, local, row_count = sizes
    dp, row, place = lax.axis_index("dp"), lax.axis_index("row"), lax.axis_index("col")
    core_at = {"col": place + 1 - 2 * (place % 2)}
    y_at = {"col": (place + 2) % 4}
    dp_at = {"dp": 1 - dp}
    codes = sorted(range(1, row_count), key=lambda code: -(code & -code))
    fars = [code for code in codes if code & -code == code]
    greet([core_at, y_at, dp_at] + [{"row": crossed(row, far)} for far in fars])
    block = out_ref.shape[0]
    width = 4 * local
    weights = ((qkv_ref, qkv_full), (out_ref, out_full), (fc1_ref, fc1_full), (fc2_ref, fc2_full))

    def row_copy(w, code):
        ref, full = weights[w]
        cols = half_of(dp, full.shape[-1])
        far = code & -code
        held = part_at(full, row_place(crossed(row, code - far), row_count, place, block), cols)
        return copy_to(
            part_at(ref, slice(None), cols) if code == far else held, held, row_send.at[w, code], row_recv.at[w, code], {"row": crossed(row, far)}
        )

    def dp_copy(w, code):
        _, full = weights[w]
        part = part_at(full, row_place(crossed(row, code), row_count, place, block), half_of(dp, full.shape[-1]))
        return copy_to(part, part, dp_send.at[w, code], dp_recv.at[w, code], dp_at)

    def own_copy(w):
        ref, full = weights[w]
        return pltpu.make_async_copy(ref, part_at(full, row_place(row, row_count, place, block), slice(None)), own_sem.at[w])

    inputs = ((images_ref, source), (cot_ref, cot))

    def y_copy(a, i):
        ref, full = inputs[a]
        return copy_to(ref.at[i], full.at[i, :, pl.ds(local, local)], in_send.at[a, 0, i], in_recv.at[a, 0, i], y_at)

    def core_copy(a, i):
        ref, full = inputs[a]
        return copy_to(ref.at[i], full.at[i, :, pl.ds(2 * local, local)], in_send.at[a, 1, i], in_recv.at[a, 1, i], core_at)

    def hand_copy(a, i):
        _, full = inputs[a]
        return copy_to(
            full.at[i, :, pl.ds(local, local)],
            full.at[i, :, pl.ds(3 * local, local)],
            in_send.at[a, 2, i],
            in_recv.at[a, 2, i],
            core_at,
        )

    def here_copy(a, i):
        ref, full = inputs[a]
        return pltpu.make_async_copy(ref.at[i], full.at[i, :, pl.ds(0, local)], in_send.at[a, 3, i])

    def vector_copy(k):
        src = vectors.at[:, pl.ds(local, local)] if k == 2 else vectors_ref
        at = (local, 2 * local, 3 * local)[k]
        return copy_to(
            src, vectors.at[:, pl.ds(at, local)], vec_send.at[k], vec_recv.at[k], (y_at, core_at, core_at)[k]
        )

    vector_here = pltpu.make_async_copy(vectors_ref, vectors.at[:, pl.ds(0, local)], vec_send.at[3])

    def given_copy(i):
        return copy_to(theirs, given.at[i], sum_send.at[0, i], sum_recv.at[0, i], core_at)

    def given_back(i):
        return copy_to(theirs, given.at[i], back_send.at[0, i], back_recv.at[0, i], core_at)

    def pair_back(i):
        return copy_to(pair.at[i], grad_in.at[i], back_send.at[1, i], back_recv.at[1, i], y_at)

    def total_back(i):
        return copy_to(
            total.at[i, :, pl.ds(0, 2 * local)],
            total.at[i, :, pl.ds(2 * local, 2 * local)],
            back_send.at[2, i],
            back_recv.at[2, i],
            core_at,
        )

    def move_copy(i):
        return copy_to(theirs, move_given.at[i], back_send.at[3, i], back_recv.at[3, i], core_at)

    hidden_width = fc1_full.shape[1]

    def half_copy(d):
        there = row_place((row + d) % row_count, row_count, place, block)
        return copy_to(
            fc2_grad.at[there, other_half_of(dp, hidden_width)], dp_in.at[there, :], half_send.at[d], half_recv.at[d], dp_at
        )

    def pair_copy(i):
        return copy_to(pair.at[i], pair_in.at[i], sum_send.at[1, i], sum_recv.at[1, i], y_at)

    def total_copy(i):
        return copy_to(
            total.at[i, :, pl.ds(0, 2 * local)],
            total.at[i, :, pl.ds(2 * local, 2 * local)],
            sum_send.at[2, i],
            sum_recv.at[2, i],
            core_at,
        )

    def start_own(w):
        for far in fars:
            row_copy(w, far).start()

    def relay(w, code):
        row_copy(w, code).wait_recv()
        for far in fars:
            if far < code & -code:
                row_copy(w, code + far).start()
        dp_copy(w, code).start()

    def arrived(w):
        for code in codes:
            dp_copy(w, code).wait_recv()
        own_copy(w).wait()

    kinds = ((source, source_out), (low, low_out), (mixed, mixed_out), (probs, probs_out), (att, att_out), (total, total_out))

    def image_copy(k, i):
        here, there = kinds[k]
        return pltpu.make_async_copy(here if k in (2, 3) else here.at[i], there.at[i], image_sem.at[k, i])

    wanted = [(a, i) for a in range(2) for i in range(count)]
    start_own(0)
    start_own(1)
    vector_copy(0).start()
    for a, i in wanted:
        y_copy(a, i).start()
    vector_copy(1).start()
    vector_here.start()
    for a, i in wanted:
        core_copy(a, i).start()
        here_copy(a, i).start()
    for w in range(4):
        own_copy(w).start()
    vector_copy(0).wait_recv()
    vector_copy(2).start()
    relay(0, codes[0])
    relay(1, codes[0])
    start_own(2)
    vector_here.wait()
    vector_copy(1).wait_recv()
    vector_copy(2).wait_recv()

    @pl.loop(0, count)
    def _(i):
        y_copy(0, i).wait_recv()
        hand_copy(0, i).start()
        here_copy(0, i).wait()
        core_copy(0, i).wait_recv()
        hand_copy(0, i).wait_recv()
        image_copy(0, i).start()
        values = source[i].astype(F32)
        middle = jnp.sum(values, axis=1, keepdims=True) / width
        square = jnp.sum(values * values, axis=1, keepdims=True) / width
        inverse = lax.rsqrt(square - middle * middle + NORM_EPS)
        low[i] = ((values - middle) * inverse * vectors[0:1, :] + vectors[1:2, :]).astype(BF16)
        image_copy(1, i).start()

        @pl.when(i == 0)
        def _():
            for code in codes[1:]:
                relay(0, code)
                relay(1, code)

    arrived(0)
    arrived(1)

    lane = lax.broadcasted_iota(jnp.int32, (1, 2 * HEAD_DIM), 1)
    key_at = lax.broadcasted_iota(jnp.int32, (1, rows), 1)
    pairs = local // (2 * HEAD_DIM)

    @pl.loop(0, count)
    def _(i):
        @pl.when(i > 0)
        def _():
            image_copy(2, i - 1).wait()

        for c in range(3):
            cols = slice(c * local, (c + 1) * local)
            rows_out = jnp.dot(low[i], qkv_full[c], preferred_element_type=F32) + qkv_bias_ref[c : c + 1, :]
            mixed[:, cols] = rows_out.astype(BF16)
        image_copy(2, i).start()

        @pl.when(i > 0)
        def _():
            image_copy(3, i - 1).wait()

        for pair_at in range(pairs):
            base = pair_at * 2 * HEAD_DIM
            queries = mixed[:, base : base + 2 * HEAD_DIM]
            key_rows = mixed[:, local + base : local + base + 2 * HEAD_DIM]
            value_rows = mixed[:, 2 * local + base : 2 * local + base + 2 * HEAD_DIM]
            parts = []
            for side in range(2):
                mask = (lane // HEAD_DIM) == side
                head_q = jnp.where(mask, queries, jnp.zeros_like(queries))
                scores = lax.dot_general(head_q, key_rows, NT, preferred_element_type=F32)
                scores = jnp.where(key_at < seq, scores, -1e30)
                peak = jnp.max(scores, axis=1, keepdims=True)
                powers = jnp.exp2((scores - peak) * (HEAD_DIM**-0.5 * LOG2E))
                share = 1.0 / jnp.sum(powers, axis=1, keepdims=True)
                probs_low = (powers * share).astype(BF16)
                probs[2 * pair_at + side] = probs_low
                parts.append(jnp.dot(probs_low, value_rows, preferred_element_type=F32))
            joined = jnp.where((lane // HEAD_DIM) == 0, parts[0], parts[1])
            att[i, :, 2 * HEAD_DIM * pair_at : 2 * HEAD_DIM * (pair_at + 1)] = joined.astype(BF16)
        image_copy(3, i).start()
        image_copy(4, i).start()
        attended = att[i]

        @pl.when(i > 0)
        def _():
            given_copy(i - 1).wait_send()

        theirs[...] = lax.dot_general(attended, out_full[2 * local :, :], NT, preferred_element_type=F32).astype(BF16)
        given_copy(i).start()
        mine[...] = lax.dot_general(attended, out_full[: 2 * local, :], NT, preferred_element_type=F32)
        given_copy(i).wait_recv()
        pair[i] = (mine[...] + given[i].astype(F32)).astype(BF16)
        pair_copy(i).start()

        @pl.when(i == 0)
        def _():
            relay(2, codes[0])
            start_own(3)
            relay(2, codes[1])

        @pl.when(i == 1)
        def _():
            for code in codes[2:]:
                relay(2, code)
            relay(3, codes[0])
            relay(3, codes[1])

    for code in codes[2:]:
        relay(3, code)
    outs = ((qkv_full, qkv_out), (out_full, outw_out), (vectors, vectors_out), (cot, cot_out), (move, move_out), (kept, kept_out), (fc1_grad, fc1_grad_out), (fc2_half, fc2_half_out), (total, grad_out))

    def out_copy(k):
        return pltpu.make_async_copy(outs[k][0], outs[k][1], out_sem.at[k])

    for k in range(3):
        out_copy(k).start()
    bias_out[...] = jnp.zeros_like(bias_out)
    step = hidden_width // 4
    given_copy(count - 1).wait_send()
    arrived(2)
    arrived(3)

    @pl.loop(0, count)
    def _(i):
        y_copy(1, i).wait_recv()
        hand_copy(1, i).start()
        pair_copy(i).wait_recv()
        total[i, :, :local] = (pair[i, :, :local].astype(F32) + pair_in[i, :, local:].astype(F32)).astype(BF16)
        total[i, :, local : 2 * local] = (pair[i, :, local:].astype(F32) + pair_in[i, :, :local].astype(F32)).astype(BF16)
        total_copy(i).start()
        image_copy(1, i).wait()
        pair_copy(i).wait_send()
        here_copy(1, i).wait()
        core_copy(1, i).wait_recv()
        hand_copy(1, i).wait_recv()
        bias_out[1:2, :local] += jnp.sum(cot[i, :, :local].astype(F32), axis=0, keepdims=True)
        total_copy(i).wait_recv()
        image_copy(5, i).start()
        values = source[i].astype(F32) + total[i].astype(F32) + vectors[4:5, :]
        kept[i] = values[:, :local] + fc2_bias_ref[...]
        middle = jnp.sum(values, axis=1, keepdims=True) / width
        square = jnp.sum(values * values, axis=1, keepdims=True) / width
        inverse = lax.rsqrt(square - middle * middle + NORM_EPS)
        low[i] = ((values - middle) * inverse * vectors[2:3, :] + vectors[3:4, :]).astype(BF16)
        for part in range(4):
            cols = slice(part * step, (part + 1) * step)
            pre_act = jnp.dot(low[i], fc1_full[:, cols], preferred_element_type=F32) + fc1_bias_ref[:, cols]
            gate = 0.5 * (1.0 + lax.erf(pre_act * ROOT_HALF))
            active[i, :, cols] = (pre_act * gate).astype(BF16)
            slope = gate + pre_act * jnp.exp(-0.5 * pre_act * pre_act) / ROOT_TWO_PI
            grad_pre = jnp.dot(cot[i], fc2_full[:, cols], preferred_element_type=F32) * slope
            bias_out[0:1, cols] += jnp.sum(grad_pre, axis=0, keepdims=True)
            gelu_grad[i, :, cols] = grad_pre.astype(BF16)

        @pl.when(i > 0)
        def _():
            given_back(i - 1).wait_send()

        theirs[...] = lax.dot_general(gelu_grad[i], fc1_full[2 * local :, :], NT, preferred_element_type=F32).astype(BF16)
        image_copy(5, i).wait()
        given_back(i).start()
        mine[...] = lax.dot_general(gelu_grad[i], fc1_full[: 2 * local, :], NT, preferred_element_type=F32)
        given_back(i).wait_recv()
        pair[i] = (mine[...] + given[i].astype(F32)).astype(BF16)
        pair_back(i).start()

    out_copy(3).start()

    def weight_grad(out, left, right):
        for part in range(4):
            span = slice(part * local, (part + 1) * local)
            terms = [lax.dot_general(left[i, :, span], right[i], TN, preferred_element_type=F32) for i in range(count)]
            out[span, :] = sum(terms[1:], terms[0]).astype(BF16)

    weight_grad(fc2_grad, cot, active)
    for d in range(row_count):
        half_copy((d + 1) % row_count).start()
    given_back(count - 1).wait_send()

    @pl.loop(0, count)
    def _(i):
        @pl.when(i > 0)
        def _():
            move_copy(i - 1).wait_send()

        theirs[...] = lax.dot_general(active[i], fc2_full[2 * local :, :], NT, preferred_element_type=F32).astype(BF16)
        move_copy(i).start()
        mine[...] = lax.dot_general(active[i], fc2_full[: 2 * local, :], NT, preferred_element_type=F32)
        move_copy(i).wait_recv()
        kept[i] += mine[:, :local] + move_given[i, :, :local].astype(F32)
        move[i] = (mine[:, local:] + move_given[i, :, local:].astype(F32)).astype(BF16)

    out_copy(4).start()
    out_copy(5).start()
    weight_grad(fc1_grad, low, gelu_grad)
    out_copy(6).start()

    @pl.loop(0, count)
    def _(i):
        pair_back(i).wait_recv()
        total_copy(i).wait_send()
        total[i, :, :local] = (pair[i, :, :local].astype(F32) + grad_in[i, :, local:].astype(F32)).astype(BF16)
        total[i, :, local : 2 * local] = (pair[i, :, local:].astype(F32) + grad_in[i, :, :local].astype(F32)).astype(BF16)
        total_back(i).start()

        @pl.when(i == count - 2)
        def _():
            for d in range(row_count):
                half_copy(d).wait_recv()
            fc2_half[...] = (fc2_grad[:, half_of(dp, hidden_width)].astype(F32) + dp_in[...].astype(F32)).astype(BF16)
            out_copy(7).start()

    for i in range(count):
        total_back(i).wait_recv()
    out_copy(8).start()
    for w in range(4):
        for code in codes:
            row_copy(w, code).wait_send()
            dp_copy(w, code).wait_send()
    for a, i in wanted:
        y_copy(a, i).wait_send()
        core_copy(a, i).wait_send()
        hand_copy(a, i).wait_send()
    for k in range(3):
        vector_copy(k).wait_send()
    for i in range(count):
        pair_back(i).wait_send()
        total_back(i).wait_send()
        image_copy(0, i).wait()
        image_copy(4, i).wait()
    move_copy(count - 1).wait_send()
    image_copy(2, count - 1).wait()
    image_copy(3, count - 1).wait()
    for d in range(row_count):
        half_copy(d).wait_send()
    for k in range(len(outs)):
        out_copy(k).wait()


def ahead(images, cotangent, qkv_block, out_block, fc1_block, fc2_block, vectors, qkv_bias, fc1_bias, fc2_bias, seq):
    count, rows, local = images.shape
    row_count = lax.axis_size("row")
    width = 4 * local
    heads = local // HEAD_DIM
    hidden = fc1_block.shape[1]

    def wide(*shape):
        return shape, BF16

    all_wide = wide(count, rows, width)
    all_pair = wide(count, rows, 2 * local)
    all_own = wide(count, rows, local)
    own_f32 = ((count, rows, local), F32)
    norm_rows = ((vectors.shape[0], width), F32)
    outs = [
        all_wide, all_wide, all_wide, wide(count, rows, 3 * local), wide(count, heads, rows, rows), all_own, all_wide, all_wide,
        wide(3, width, local), wide(width, local), norm_rows, all_own, own_f32, wide(width, hidden), wide(width, hidden // 2),
        ((2, hidden), F32),
    ]
    scratch = [
        all_wide, all_wide, all_wide, wide(rows, 3 * local), wide(heads, rows, rows), all_own,
        wide(rows, 2 * local), all_pair, ((rows, 2 * local), F32), all_pair, all_pair, all_wide,
        wide(3, width, local), wide(width, local), wide(width, hidden), wide(width, hidden), norm_rows,
        wide(count, rows, hidden), wide(count, rows, hidden), all_pair, all_pair, own_f32, all_own,
        wide(width, hidden), wide(width, hidden), wide(width, hidden // 2), wide(width, hidden // 2),
    ]
    dma = pltpu.SemaphoreType.DMA
    whole = pl.BlockSpec(memory_space=pl.ANY)
    vmem = pl.BlockSpec(memory_space=pltpu.VMEM)
    return pl.pallas_call(
        functools.partial(ahead_kernel, (count, seq, rows, local, row_count)),
        out_shape=[jax.ShapeDtypeStruct(*s) for s in outs],
        in_specs=[whole] * 7 + [vmem] * 3,
        out_specs=[whole] * (len(outs) - 1) + [vmem],
        scratch_shapes=[pltpu.VMEM(*s) for s in scratch]
        + [dma((4, row_count))] * 4
        + [dma((4,)), dma((2, 4, count)), dma((2, 3, count)), dma((4,)), dma((3,))]
        + [dma((3, count)), dma((3, count)), dma((6, count)), dma((9,))]
        + [dma((4, count)), dma((4, count)), dma((row_count,)), dma((row_count,))],
        name="ahead",
        compiler_params=pltpu.CompilerParams(
            vmem_limit_bytes=63 * 2**20, collective_id=0, has_side_effects=True
        ),
    )(images, cotangent, qkv_block, out_block, fc1_block, fc2_block, vectors, qkv_bias, fc1_bias, fc2_bias)


def back_kernel(
    sizes,
    source_ref, total_ref, cot_ref, grad_ref, mixed_ref, probs_ref, att_ref, low_ref, move_ref, kept_ref,
    qkv_ref, outw_ref, fc1_grad_ref, fc2_half_ref, vectors_ref, mlp_bias_ref,
    images_out, images_grad_out, small_out, qkv_out, outw_out, fc1_out, fc2_out,
    source, total, cot, grad_in, mixed, probs, att, low,
    hidden_low, mixed_grad, grad_hidden, normed1, inverse1, qkv_sum, outw_sum, k_turned, v_turned,
    theirs, given, mine, kept_grad, send, got, stat, stat_given, stat_pair, stat_in,
    move_in, kept, finished, qkv, outw, qkv_grad, outw_grad, small, small_in,
    half_fc2, half_fc1, half_outw, half_qkv, dp_fc1, dp_outw, dp_qkv,
    row_fc2, row_fc1, row_outw, row_qkv, tot_fc2, tot_fc1, tot_outw, tot_qkv,
    early_sem, late_sem, once_sem, sum_send, sum_recv, move_send, move_recv, small_send, small_recv,
    dp_send, dp_recv, row_send, row_recv, tot_send, tot_recv, out_sem,
):
    count, rows, local, row_count = sizes
    dp, row, place = lax.axis_index("dp"), lax.axis_index("row"), lax.axis_index("col")
    core_at = {"col": place + 1 - 2 * (place % 2)}
    y_at = {"col": (place + 2) % 4}
    dp_at = {"dp": 1 - dp}
    rounds = [dp_at]
    distance = 1
    while distance < row_count:
        rounds.append({"row": crossed(row, distance)})
        distance *= 2
    greet([core_at, y_at] + rounds)
    width = 4 * local
    block = width // row_count
    two = 2 * HEAD_DIM
    scale = HEAD_DIM**-0.5

    early = ((source_ref, source), (total_ref, total), (cot_ref, cot), (grad_ref, grad_in))
    late = ((mixed_ref, mixed), (probs_ref, probs), (att_ref, att), (low_ref, low))

    def early_load(k, i):
        here, there = early[k]
        return pltpu.make_async_copy(here.at[i], there.at[i % 2] if k == 0 else there, early_sem.at[k])

    def late_load(k, i):
        here, there = late[k]
        return pltpu.make_async_copy(here.at[i], there, late_sem.at[k])

    once = (
        (outw_ref, outw), (qkv_ref, qkv), (fc2_half_ref, half_fc2),
        (fc1_grad_ref.at[:, half_of(dp, fc1_grad_ref.shape[1])], half_fc1), (kept_ref, kept),
    )

    def once_load(k):
        return pltpu.make_async_copy(once[k][0], once[k][1], once_sem.at[k])

    grads = (None, fc1_grad_ref, outw_grad, qkv_grad)
    halves = (half_fc2, half_fc1, half_outw, half_qkv)
    dp_ins = (None, dp_fc1, dp_outw, dp_qkv)
    row_ins = (row_fc2, row_fc1, row_outw, row_qkv)
    tots = (tot_fc2, tot_fc1, tot_outw, tot_qkv)

    codes = sorted(range(1, row_count), key=lambda code: (code & -code, -code)) + [0]

    def rows_at(code):
        return row_place(crossed(row, code), row_count, place, block)

    def dp_copy(w, code):
        full = grads[w]
        return copy_to(
            part_at(full, rows_at(code), other_half_of(dp, full.shape[-1])),
            part_at(dp_ins[w], rows_at(code), slice(None)),
            dp_send.at[w, code],
            dp_recv.at[w, code],
            dp_at,
        )

    def row_copy(w, code):
        return copy_to(
            part_at(halves[w], rows_at(code), slice(None)),
            row_ins[w].at[code],
            row_send.at[w, code],
            row_recv.at[w, code],
            {"row": crossed(row, code & -code)},
        )

    def tot_copy(w):
        part = part_at(tots[w], slice(None), half_of(dp, tots[w].shape[-1]))
        return copy_to(part, part, tot_send.at[w], tot_recv.at[w], dp_at)

    def add_to(w, code, term):
        at = (slice(None), rows_at(code), slice(None)) if len(halves[w].shape) == 3 else (rows_at(code), slice(None))
        halves[w][at] = (halves[w][at].astype(F32) + term.astype(F32)).astype(BF16)

    def dp_sum(w, code):
        dp_copy(w, code).wait_recv()
        at = (slice(None), rows_at(code), slice(None)) if len(halves[w].shape) == 3 else (rows_at(code), slice(None))
        add_to(w, code, dp_ins[w][at])

    def row_take(w, code):
        row_copy(w, code).wait_recv()
        add_to(w, code - (code & -code), row_ins[w][code])

    def row_first(w):
        for code in codes[:-1]:
            if code % 2:
                row_copy(w, code).start()

    def row_next(w):
        for code in codes[:-1]:
            if code % 2 == 0:
                far = 1
                while far < code & -code:
                    row_take(w, code + far)
                    far *= 2
                row_copy(w, code).start()

    def row_last(w):
        far = 1
        while far < row_count:
            row_take(w, far)
            far *= 2
        own = halves[w][:, rows_at(0), :] if len(halves[w].shape) == 3 else halves[w][rows_at(0), :]
        cols = half_of(dp, tots[w].shape[-1])
        if len(halves[w].shape) == 3:
            tots[w][:, :, cols] = own
        else:
            tots[w][:, cols] = own
        tot_copy(w).start()

    def given_copy(i):
        return copy_to(theirs.at[i], given.at[i], sum_send.at[0, i], sum_recv.at[0, i], core_at)

    def stat_copy(i):
        return copy_to(stat.at[i], stat_given.at[i], sum_send.at[1, i], sum_recv.at[1, i], core_at)

    def got_copy(i):
        return copy_to(send.at[i], got.at[i], sum_send.at[2, i], sum_recv.at[2, i], y_at)

    def stat_pair_copy(i):
        return copy_to(stat_pair.at[i], stat_in.at[i], sum_send.at[3, i], sum_recv.at[3, i], y_at)

    def move_copy(i):
        return copy_to(move_ref.at[i], move_in.at[i], move_send.at[i], move_recv.at[i], y_at)

    def small_copy(s):
        return copy_to(small.at[s], small_in.at[s], small_send.at[s], small_recv.at[s], rounds[s])

    for k in range(4):
        early_load(k, 0).start()
    once_load(2).start()
    once_load(0).start()
    for k in range(4):
        late_load(k, 0).start()
    for k in (1, 3, 4):
        once_load(k).start()
    for i in range(count):
        move_copy(i).start()
    for code in codes:
        dp_copy(1, code).start()

    small[0] = jnp.zeros_like(small[0])
    small[0, 7:8, :] = mlp_bias_ref[1:2, :local]
    for part in range(mlp_bias_ref.shape[1] // local):
        small[0, 8 + part : 9 + part, :] = mlp_bias_ref[0:1, part * local : (part + 1) * local]
    qkv_sum[...] = jnp.zeros_like(qkv_sum)
    outw_sum[...] = jnp.zeros_like(outw_sum)
    once_load(2).wait()
    row_first(0)

    def product_of(span):
        terms = [
            lax.dot_general(mixed_grad[:, c * local : (c + 1) * local], qkv[c, span, :], NT, preferred_element_type=F32)
            for c in range(3)
        ]
        return terms[0] + terms[1] + terms[2]

    lane = lax.broadcasted_iota(jnp.int32, (1, two), 1)
    down = lax.broadcasted_iota(jnp.int32, (two, two), 0)
    across = lax.broadcasted_iota(jnp.int32, (two, two), 1)
    eye = (down == across).astype(BF16)

    @pl.loop(0, count)
    def _(i):
        for k in range(4):
            early_load(k, i).wait()
        values = source[i % 2].astype(F32) + total[...].astype(F32) + vectors_ref[4:5, :]
        middle = jnp.sum(values, axis=1, keepdims=True) / width
        square = jnp.sum(values * values, axis=1, keepdims=True) / width
        inverse = lax.rsqrt(square - middle * middle + NORM_EPS)
        normed = (values - middle) * inverse
        grad = grad_in[...].astype(F32)
        small[0, 5:6, :] += jnp.sum(grad[:, :local] * normed[:, :local], axis=0, keepdims=True)
        small[0, 6:7, :] += jnp.sum(grad[:, :local], axis=0, keepdims=True)
        scaled = grad * vectors_ref[2:3, :]
        first = jnp.sum(scaled, axis=1, keepdims=True) / width
        second = jnp.sum(scaled * normed, axis=1, keepdims=True) / width
        whole_grad = cot[...].astype(F32) + inverse * (scaled - first - normed * second)
        grad_hidden[i] = whole_grad[:, :local]
        small[0, 2:3, :] += jnp.sum(whole_grad[:, :local], axis=0, keepdims=True)
        hidden_low[...] = whole_grad.astype(BF16)

        @pl.when(i + 1 < count)
        def _():
            for k in range(4):
                early_load(k, i + 1).start()

        for k in range(4):
            late_load(k, i).wait()

        @pl.when(i == 0)
        def _():
            once_load(0).wait()
            once_load(1).wait()

        grad_att = jnp.dot(hidden_low[...], outw[...], preferred_element_type=F32).astype(BF16)
        for part in range(4):
            span = slice(part * local, (part + 1) * local)
            outw_sum[span, :] += lax.dot_general(hidden_low[:, span], att[...], TN, preferred_element_type=F32)
        for pair in range(local // two):
            base = pair * two
            cols = slice(pair * two, (pair + 1) * two)
            queries = mixed[:, cols]
            key_rows = mixed[:, local + base : local + base + two]
            value_rows = mixed[:, 2 * local + base : 2 * local + base + two]
            pair_grad = grad_att[:, cols]
            q_turned = lax.dot_general(eye, queries, NT, preferred_element_type=F32).astype(BF16)
            grad_turned = lax.dot_general(eye, pair_grad, NT, preferred_element_type=F32).astype(BF16)
            product = pair_grad.astype(F32) * att[:, cols].astype(F32)
            parts = []
            for side in range(2):
                mask = (lane // HEAD_DIM) == side
                turn = slice(side * HEAD_DIM, (side + 1) * HEAD_DIM)
                head_grad = jnp.where(mask, pair_grad, jnp.zeros_like(pair_grad))
                grad_probs = lax.dot_general(head_grad, value_rows, NT, preferred_element_type=F32)
                delta = jnp.sum(jnp.where(mask, product, 0.0), axis=1, keepdims=True)
                probs_low = probs[2 * pair + side]
                grad_scores = (probs_low.astype(F32) * (grad_probs - delta)).astype(BF16)
                parts.append(jnp.dot(grad_scores, key_rows, preferred_element_type=F32))
                k_turned[turn, :] = jnp.dot(q_turned[turn, :], grad_scores, preferred_element_type=F32)
                v_turned[turn, :] = jnp.dot(grad_turned[turn, :], probs_low, preferred_element_type=F32)
            q_grad = jnp.where((lane // HEAD_DIM) == 0, parts[0], parts[1]) * scale
            v_grad = v_turned[...].T
            mixed_grad[:, cols] = q_grad.astype(BF16)
            mixed_grad[:, local + base : local + base + two] = (k_turned[...].T * scale).astype(BF16)
            mixed_grad[:, 2 * local + base : 2 * local + base + two] = v_grad.astype(BF16)
            small[0, 0:1, cols] += jnp.sum(q_grad, axis=0, keepdims=True)
            small[0, 1:2, cols] += jnp.sum(v_grad, axis=0, keepdims=True)
        @pl.when(i + 1 < count)
        def _():
            for k in range(3):
                late_load(k, i + 1).start()

        values = source[i % 2].astype(F32)
        middle = jnp.sum(values, axis=1, keepdims=True) / width
        square = jnp.sum(values * values, axis=1, keepdims=True) / width
        inverse = lax.rsqrt(square - middle * middle + NORM_EPS)
        normed = (values - middle) * inverse
        normed1[i] = normed[:, :local]
        inverse1[i] = inverse
        scaled_in = normed * vectors_ref[0:1, :]
        far = product_of(slice(2 * local, 4 * local))
        theirs[i] = far.astype(BF16)
        given_copy(i).start()
        near = product_of(slice(0, 2 * local))
        mine[...] = near
        first = jnp.sum(far * vectors_ref[0:1, 2 * local :], axis=1, keepdims=True) + jnp.sum(
            near * vectors_ref[0:1, : 2 * local], axis=1, keepdims=True
        )
        second = jnp.sum(far * scaled_in[:, 2 * local :], axis=1, keepdims=True) + jnp.sum(
            near * scaled_in[:, : 2 * local], axis=1, keepdims=True
        )
        spread = jnp.where(lane == 0, first, jnp.where(lane == 1, second, 0.0))
        stat[i] = spread.T[:8, :]
        stat_copy(i).start()
        for part in range(4):
            span = slice(part * local, (part + 1) * local)
            term = lax.dot_general(low[:, span], mixed_grad[...], TN, preferred_element_type=F32)
            for c in range(3):
                qkv_sum[c, span, :] += term[:, c * local : (c + 1) * local]

        @pl.when(i + 1 < count)
        def _():
            late_load(3, i + 1).start()

        given_copy(i).wait_recv()
        kept_grad[i] = mine[:, :local] + given[i, :, :local].astype(F32)
        send[i] = (mine[:, local:] + given[i, :, local:].astype(F32)).astype(BF16)
        got_copy(i).start()
        stat_copy(i).wait_recv()
        stat_pair[i] = stat[i] + stat_given[i]
        stat_pair_copy(i).start()

        @pl.when(i == 0)
        def _():
            row_next(0)
            once_load(3).wait()

        @pl.when(i == 1)
        def _():
            for code in codes:
                dp_sum(1, code)
                if code % 2:
                    row_copy(1, code).start()
            row_last(0)

    outw_grad[...] = outw_sum[...].astype(BF16)
    half_outw[...] = outw_grad[:, half_of(dp, local)]
    for code in codes:
        dp_copy(2, code).start()
    qkv_grad[...] = qkv_sum[...].astype(BF16)
    half_qkv[...] = qkv_grad[:, :, half_of(dp, local)]
    for code in codes:
        dp_copy(3, code).start()
    row_next(1)
    once_load(4).wait()

    @pl.loop(0, count)
    def _(i):
        move_copy(i).wait_recv()
        finished[i] = (kept[i] + move_in[i].astype(F32)).astype(BF16)

    for w in (2, 3):
        for code in codes:
            if code % 2:
                dp_sum(w, code)
                row_copy(w, code).start()
    row_last(1)

    @pl.loop(0, count)
    def _(i):
        got_copy(i).wait_recv()
        stat_pair_copy(i).wait_recv()
        sums = stat_pair[i] + stat_in[i]
        spread = jnp.concatenate([sums, jnp.zeros((two - 8, rows), F32)], axis=0).T / width
        grad = kept_grad[i] + got[i].astype(F32)
        small[0, 3:4, :] += jnp.sum(grad * normed1[i], axis=0, keepdims=True)
        small[0, 4:5, :] += jnp.sum(grad, axis=0, keepdims=True)
        scaled = grad * vectors_ref[0:1, :local]
        grad_hidden[i] += inverse1[i] * (scaled - spread[:, 0:1] - normed1[i] * spread[:, 1:2])

    pltpu.make_async_copy(finished, images_out, out_sem.at[0]).start()
    pltpu.make_async_copy(grad_hidden, images_grad_out, out_sem.at[1]).start()
    small_copy(0).start()
    for w in (2, 3):
        for code in codes:
            if code % 2 == 0:
                dp_sum(w, code)
        row_next(w)
    for s in range(len(rounds)):
        small_copy(s).wait_recv()
        small[s + 1] = small[s] + small_in[s]
        if s + 1 < len(rounds):
            small_copy(s + 1).start()
    row_last(2)
    row_last(3)
    outs = ((tot_fc2, fc2_out), (tot_fc1, fc1_out), (tot_outw, outw_out), (tot_qkv, qkv_out))
    for w, (here, there) in enumerate(outs):
        tot_copy(w).wait_recv()
        pltpu.make_async_copy(here, there, out_sem.at[2 + w]).start()
    small_out[...] = small[len(rounds)]
    for i in range(count):
        given_copy(i).wait_send()
        stat_copy(i).wait_send()
        got_copy(i).wait_send()
        stat_pair_copy(i).wait_send()
        move_copy(i).wait_send()
    for s in range(len(rounds)):
        small_copy(s).wait_send()
    for w in range(4):
        tot_copy(w).wait_send()
        for code in codes:
            if w:
                dp_copy(w, code).wait_send()
            if code:
                row_copy(w, code).wait_send()
    for k, (here, there) in enumerate(((finished, images_out), (grad_hidden, images_grad_out), *outs)):
        pltpu.make_async_copy(here, there, out_sem.at[k]).wait()


def back(
    source, total, cot, grad_low, mixed, probs, att, low, move, kept, qkv, outw, fc1_grad, fc2_half, vectors, mlp_bias
):
    count, rows, width = source.shape
    local = width // 4
    row_count = lax.axis_size("row")
    block = width // row_count
    hidden = fc1_grad.shape[1]
    qkv_width = 3 * local
    heads = local // HEAD_DIM
    rounds = row_count.bit_length()
    outs = [
        ((count, rows, local), BF16), ((count, rows, local), F32), ((16, local), F32),
        ((3, block, local), BF16), ((block, local), BF16), ((block, hidden), BF16), ((block, hidden), BF16),
    ]
    own_f32 = ((count, rows, local), F32)
    own_low = ((count, rows, local), BF16)
    pair_low = ((count, rows, 2 * local), BF16)
    stat = ((count, 8, rows), F32)
    wide = ((rows, width), BF16)
    turned = ((2 * HEAD_DIM, rows), F32)
    columns = (((), hidden), ((), hidden), ((), local), ((3,), local))
    scratch = [
        ((2, rows, width), BF16), wide, wide, wide, ((rows, qkv_width), BF16), ((heads, rows, rows), BF16), ((rows, local), BF16), wide,
        wide, ((rows, qkv_width), BF16), own_f32, own_f32, ((count, rows, 1), F32),
        ((3, width, local), F32), ((width, local), F32), turned, turned,
        pair_low, pair_low, ((rows, 2 * local), F32), own_f32, own_low, own_low, stat, stat, stat, stat,
        own_low, own_f32, own_low, ((3, width, local), BF16), ((width, local), BF16),
        ((3, width, local), BF16), ((width, local), BF16), ((rounds + 1, 16, local), F32), ((rounds, 16, local), F32),
        *[((*lead, width, c // 2), BF16) for lead, c in columns],
        *[((*lead, width, c // 2), BF16) for lead, c in columns[1:]],
        *[((row_count, *lead, block, c // 2), BF16) for lead, c in columns],
        *[((*lead, block, c), BF16) for lead, c in columns],
    ]
    dma = pltpu.SemaphoreType.DMA
    whole = pl.BlockSpec(memory_space=pl.ANY)
    vmem = pl.BlockSpec(memory_space=pltpu.VMEM)
    return pl.pallas_call(
        functools.partial(back_kernel, (count, rows, local, row_count)),
        out_shape=[jax.ShapeDtypeStruct(*s) for s in outs],
        in_specs=[whole] * 14 + [vmem] * 2,
        out_specs=[whole, whole, vmem] + [whole] * 4,
        scratch_shapes=[pltpu.VMEM(*s) for s in scratch]
        + [dma((4,)), dma((4,)), dma((5,)), dma((4, count)), dma((4, count)), dma((count,)), dma((count,)), dma((rounds,)), dma((rounds,))]
        + [dma((4, row_count))] * 4
        + [dma((4,)), dma((4,)), dma((6,))],
        name="back",
        compiler_params=pltpu.CompilerParams(
            vmem_limit_bytes=63 * 2**20, collective_id=2, has_side_effects=True
        ),
    )(source, total, cot, grad_low, mixed, probs, att, low, move, kept, qkv, outw, fc1_grad, fc2_half, vectors, mlp_bias)


def adam_step(weight, grad, momentum, variance):
    moment_new = BETA_FIRST * momentum + (1.0 - BETA_FIRST) * grad
    second_new = BETA_SECOND * variance + (1.0 - BETA_SECOND) * grad * grad
    corrected = moment_new / (1.0 - BETA_FIRST**STEP)
    second_corrected = second_new / (1.0 - BETA_SECOND**STEP)
    master = weight.astype(jnp.float32)
    updated = master - LEARN_RATE * (
        corrected / (jnp.sqrt(second_corrected) + ADAM_EPS) + WEIGHT_DECAY * master
    )
    return (updated, moment_new, second_new)


def per_device(
    images_in,
    cotangent,
    first_gain,
    first_shift,
    second_gain,
    second_shift,
    qkv_weight,
    qv_bias,
    out_weight,
    out_bias,
    fc1_weight,
    fc1_bias,
    fc2_weight,
    fc2_bias,
    qkv_momentum,
    qkv_variance,
    out_momentum,
    out_variance,
    fc1_momentum,
    fc1_variance,
    fc2_momentum,
    fc2_variance,
):
    image_count, seq, local = images_in.shape
    width = 4 * local
    rows = -(-seq // ROW_TILE) * ROW_TILE
    place = lax.axis_index("col")

    vectors = jnp.pad(jnp.stack([first_gain, first_shift, second_gain, second_shift, out_bias]), ((0, 3), (0, 0)))
    qkv_shift = jnp.stack([qv_bias[0], jnp.zeros_like(qv_bias[0]), qv_bias[1]])
    (
        source_all, cot_all, low_all, mixed_all, probs_all, att_all, total_all, grad_low2, qkv_full, out_full, vectors,
        move, kept, fc1_grad, fc2_half, mlp_bias,
    ) = ahead(
        jnp.pad(images_in, ((0, 0), (0, rows - seq), (0, 0))),
        jnp.pad(cotangent, ((0, 0), (0, rows - seq), (0, 0))),
        qkv_weight.transpose(1, 0, 2),
        out_weight,
        fc1_weight,
        fc2_weight,
        vectors,
        qkv_shift,
        fc1_bias[None],
        fc2_bias[None],
        seq,
    )
    images_out, images_grad, small, qkv_total, out_total, fc1_total, fc2_total = back(
        source_all, total_all, cot_all, grad_low2, mixed_all, probs_all, att_all, low_all, move, kept,
        qkv_full, out_full, fc1_grad, fc2_half, vectors, mlp_bias,
    )
    qkv_total = qkv_total.transpose(1, 0, 2).astype(F32)
    out_total, fc1_total, fc2_total = (t.astype(F32) for t in (out_total, fc1_total, fc2_total))
    qkv_new = adam_step(qkv_weight, qkv_total, qkv_momentum, qkv_variance)
    out_new = adam_step(out_weight, out_total, out_momentum, out_variance)
    fc1_new = adam_step(fc1_weight, fc1_total, fc1_momentum, fc1_variance)
    fc2_new = adam_step(fc2_weight, fc2_total, fc2_momentum, fc2_variance)
    return (
        images_out[:, :seq],
        images_grad[:, :seq],
        qkv_total,
        out_total,
        fc1_total,
        fc2_total,
        small[0:2],
        small[2],
        small[8:12].reshape(-1),
        small[7],
        small[3],
        small[4],
        small[5],
        small[6],
        qkv_new[0],
        out_new[0],
        fc1_new[0],
        fc2_new[0],
        qkv_new[1],
        out_new[1],
        fc1_new[1],
        fc2_new[1],
        qkv_new[2],
        out_new[2],
        fc1_new[2],
        fc2_new[2],
    )


def solution(mesh):
    return jax.shard_map(
        per_device,
        mesh=mesh,
        in_specs=(
            P(("dp", "row"), None, "col"),
            P(("dp", "row"), None, "col"),
            P("col"),
            P("col"),
            P("col"),
            P("col"),
            P("row", None, "col"),
            P(None, "col"),
            P("row", "col"),
            P("col"),
            P("row", "col"),
            P("col"),
            P("row", "col"),
            P("col"),
            P("row", None, "col"),
            P("row", None, "col"),
            P("row", "col"),
            P("row", "col"),
            P("row", "col"),
            P("row", "col"),
            P("row", "col"),
            P("row", "col"),
        ),
        out_specs=(
            P(("dp", "row"), None, "col"),
            P(("dp", "row"), None, "col"),
            P("row", None, "col"),
            P("row", "col"),
            P("row", "col"),
            P("row", "col"),
            P(None, "col"),
            P("col"),
            P("col"),
            P("col"),
            P("col"),
            P("col"),
            P("col"),
            P("col"),
            P("row", None, "col"),
            P("row", "col"),
            P("row", "col"),
            P("row", "col"),
            P("row", None, "col"),
            P("row", "col"),
            P("row", "col"),
            P("row", "col"),
            P("row", None, "col"),
            P("row", "col"),
            P("row", "col"),
            P("row", "col"),
        ),
        check_vma=False,
    )
```

```python
import functools

import jax
import jax.numpy as jnp
from jax import lax
from jax.experimental import pallas as pl
from jax.experimental.pallas import tpu as pltpu
from jax.sharding import PartitionSpec as P

HEAD_DIM = 64
STEP = 3


NORM_EPS = 1e-06
LEARN_RATE = 0.02
BETA_FIRST = 0.9
BETA_SECOND = 0.999
ADAM_EPS = 1e-08
WEIGHT_DECAY = 0.05
ROOT_HALF = 0.7071067811865476
ROOT_TWO_PI = 2.5066282746310002
LOG2E = 1.4426950408889634
ROW_TILE = 16
MESH = pl.DeviceIdType.MESH
NT = (((1,), (1,)), ((), ()))
TN = (((0,), (0,)), ((), ()))
F32 = jnp.float32
BF16 = jnp.bfloat16


def copy_to(src, dst, send, recv, where):
    return pltpu.make_async_remote_copy(
        src_ref=src, dst_ref=dst, send_sem=send, recv_sem=recv, device_id=where, device_id_type=MESH
    )


def rel_place(quarter, place):
    return (quarter // 2 + place // 2) % 2 + 2 * ((quarter % 2 + place % 2) % 2)


def crossed(row, code):
    distance = 1
    while distance <= code:
        if code & distance:
            row = row + distance * (1 - 2 * ((row // distance) % 2))
        distance *= 2
    return row


def half_of(dp, full_width):
    half = full_width // 2
    return pl.ds(pl.multiple_of(dp * half, half), half)


def other_half_of(dp, full_width):
    half = full_width // 2
    return pl.ds(pl.multiple_of((1 - dp) * half, half), half)


def row_place(owner, row_count, place, block):
    per = row_count // 4
    at = (rel_place(owner // per, place) * per + owner % per) * block
    return pl.ds(pl.multiple_of(at, block), block)


def part_at(full, rows, cols):
    return full.at[:, rows, cols] if len(full.shape) == 3 else full.at[rows, cols]


def greet(partners):
    barrier = pltpu.get_barrier_semaphore()
    for partner in partners:
        pl.semaphore_signal(barrier, inc=1, device_id=partner, device_id_type=MESH)
    pl.semaphore_wait(barrier, len(partners))


def ahead_kernel(
    sizes,
    images_ref, cot_ref, qkv_ref, out_ref, fc1_ref, fc2_ref,
    gain1_ref, shift1_ref, gain2_ref, shift2_ref, out_bias_ref, qv_bias_ref, fc1_bias_ref, fc2_bias_ref,
    source_out, cot_out, low_out, mixed_out, probs_out, att_out, total_out, grad_out, qkv_out, outw_out, vectors_out,
    move_out, kept_out, fc1_grad_out, fc2_half_out, fc2_grad_out, late_out, bias_out,
    source, cot, low, mixed, probs, att, theirs, given, mine, pair, pair_in, total, qkv_full, out_full, fc1_full, fc2_full, vectors, vectors_ref,
    active, gelu_grad, grad_in, move_given, kept, move, fc1_grad, fc2_grad, dp_in, fc2_half,
    row_send, row_recv, dp_send, dp_recv, own_sem, in_send, in_recv, vec_send, vec_recv, sum_send, sum_recv, image_sem, out_sem,
    back_send, back_recv, half_send, half_recv,
):
    count, seq, rows, local, row_count = sizes
    dp, row, place = lax.axis_index("dp"), lax.axis_index("row"), lax.axis_index("col")
    core_at = {"col": place + 1 - 2 * (place % 2)}
    y_at = {"col": (place + 2) % 4}
    dp_at = {"dp": 1 - dp}
    codes = sorted(range(1, row_count), key=lambda code: -(code & -code))
    fars = [code for code in codes if code & -code == code]
    greet([core_at, y_at, dp_at] + [{"row": crossed(row, far)} for far in fars])
    block = out_ref.shape[0]
    width = 4 * local
    weights = ((qkv_ref, qkv_full), (out_ref, out_full), (fc1_ref, fc1_full), (fc2_ref, fc2_full))

    def row_copy(w, code):
        ref, full = weights[w]
        cols = half_of(dp, full.shape[-1])
        far = code & -code
        held = part_at(full, row_place(crossed(row, code - far), row_count, place, block), cols)
        return copy_to(
            part_at(ref, slice(None), cols) if code == far else held, held, row_send.at[w, code], row_recv.at[w, code], {"row": crossed(row, far)}
        )

    def dp_copy(w, code):
        _, full = weights[w]
        part = part_at(full, row_place(crossed(row, code), row_count, place, block), half_of(dp, full.shape[-1]))
        return copy_to(part, part, dp_send.at[w, code], dp_recv.at[w, code], dp_at)

    def own_copy(w):
        ref, full = weights[w]
        return pltpu.make_async_copy(ref, part_at(full, row_place(row, row_count, place, block), slice(None)), own_sem.at[w])

    inputs = ((images_ref, source), (cot_ref, cot))

    def y_copy(a, i):
        ref, full = inputs[a]
        return copy_to(ref.at[i], full.at[i, :, pl.ds(local, local)], in_send.at[a, 0, i], in_recv.at[a, 0, i], y_at)

    def core_copy(a, i):
        ref, full = inputs[a]
        return copy_to(ref.at[i], full.at[i, :, pl.ds(2 * local, local)], in_send.at[a, 1, i], in_recv.at[a, 1, i], core_at)

    def hand_copy(a, i):
        _, full = inputs[a]
        return copy_to(
            full.at[i, :, pl.ds(local, local)],
            full.at[i, :, pl.ds(3 * local, local)],
            in_send.at[a, 2, i],
            in_recv.at[a, 2, i],
            core_at,
        )

    def here_copy(a, i):
        ref, full = inputs[a]
        return pltpu.make_async_copy(ref.at[i], full.at[i, :, pl.ds(0, local)], in_send.at[a, 3, i])

    def vector_copy(k):
        src = vectors.at[:, pl.ds(local, local)] if k == 2 else vectors_ref
        at = (local, 2 * local, 3 * local)[k]
        return copy_to(
            src, vectors.at[:, pl.ds(at, local)], vec_send.at[k], vec_recv.at[k], (y_at, core_at, core_at)[k]
        )

    for k, vector in enumerate((gain1_ref, shift1_ref, gain2_ref, shift2_ref, out_bias_ref)):
        vectors_ref[k : k + 1, :] = vector[...]
    vectors_ref[5:8, :] = jnp.zeros((3, local), F32)
    vector_here = pltpu.make_async_copy(vectors_ref, vectors.at[:, pl.ds(0, local)], vec_send.at[3])

    def given_copy(i):
        return copy_to(theirs, given.at[i], sum_send.at[0, i], sum_recv.at[0, i], core_at)

    def given_back(i):
        return copy_to(theirs, given.at[i], back_send.at[0, i], back_recv.at[0, i], core_at)

    def pair_back(i):
        return copy_to(pair.at[i], grad_in.at[i], back_send.at[1, i], back_recv.at[1, i], y_at)

    def total_back(i):
        return copy_to(
            total.at[i, :, pl.ds(0, 2 * local)],
            total.at[i, :, pl.ds(2 * local, 2 * local)],
            back_send.at[2, i],
            back_recv.at[2, i],
            core_at,
        )

    def move_copy(i):
        return copy_to(theirs, move_given.at[i], back_send.at[3, i], back_recv.at[3, i], core_at)

    hidden_width = fc1_full.shape[1]

    odd_codes = sorted(range(1, row_count, 2), reverse=True)

    def half_copy(code):
        there = row_place(crossed(row, code), row_count, place, block)
        return copy_to(
            fc2_grad.at[there, other_half_of(dp, hidden_width)], dp_in.at[there, :], half_send.at[code], half_recv.at[code], dp_at
        )

    def pair_copy(i):
        return copy_to(pair.at[i], pair_in.at[i], sum_send.at[1, i], sum_recv.at[1, i], y_at)

    def total_copy(i):
        return copy_to(
            total.at[i, :, pl.ds(0, 2 * local)],
            total.at[i, :, pl.ds(2 * local, 2 * local)],
            sum_send.at[2, i],
            sum_recv.at[2, i],
            core_at,
        )

    def start_own(w):
        for far in fars:
            row_copy(w, far).start()

    def relay(w, code):
        row_copy(w, code).wait_recv()
        for far in fars:
            if far < code & -code:
                row_copy(w, code + far).start()
        dp_copy(w, code).start()

    def arrived(w):
        for code in codes:
            dp_copy(w, code).wait_recv()
        own_copy(w).wait()

    kinds = ((source, source_out), (low, low_out), (mixed, mixed_out), (probs, probs_out), (att, att_out), (total, total_out))

    def image_copy(k, i):
        here, there = kinds[k]
        return pltpu.make_async_copy(here if k in (2, 3) else here.at[i], there.at[i], image_sem.at[k, i])

    wanted = [(a, i) for a in range(2) for i in range(count)]
    start_own(0)
    start_own(1)
    vector_copy(0).start()
    for a, i in wanted:
        y_copy(a, i).start()
    vector_copy(1).start()
    vector_here.start()
    for a, i in wanted:
        core_copy(a, i).start()
        here_copy(a, i).start()
    for w in range(4):
        own_copy(w).start()
    vector_copy(0).wait_recv()
    vector_copy(2).start()
    relay(0, codes[0])
    relay(1, codes[0])
    start_own(2)
    vector_here.wait()
    vector_copy(1).wait_recv()
    vector_copy(2).wait_recv()

    @pl.loop(0, count)
    def _(i):
        y_copy(0, i).wait_recv()
        hand_copy(0, i).start()
        here_copy(0, i).wait()
        core_copy(0, i).wait_recv()
        hand_copy(0, i).wait_recv()
        image_copy(0, i).start()
        values = source[i].astype(F32)
        middle = jnp.sum(values, axis=1, keepdims=True) / width
        square = jnp.sum(values * values, axis=1, keepdims=True) / width
        inverse = lax.rsqrt(square - middle * middle + NORM_EPS)
        low[i] = ((values - middle) * inverse * vectors[0:1, :] + vectors[1:2, :]).astype(BF16)
        image_copy(1, i).start()

        @pl.when(i == 0)
        def _():
            for code in codes[1:]:
                relay(0, code)
                relay(1, code)

    relay(2, codes[0])
    start_own(3)
    arrived(0)
    arrived(1)

    lane = lax.broadcasted_iota(jnp.int32, (1, 2 * HEAD_DIM), 1)
    key_at = lax.broadcasted_iota(jnp.int32, (1, rows), 1)
    pairs = local // (2 * HEAD_DIM)

    @pl.loop(0, count)
    def _(i):
        @pl.when(i > 0)
        def _():
            image_copy(2, i - 1).wait()

        for c in range(3):
            cols = slice(c * local, (c + 1) * local)
            rows_out = jnp.dot(low[i], qkv_full[c], preferred_element_type=F32)
            if c != 1:
                rows_out += qv_bias_ref[c // 2 : c // 2 + 1, :]
            mixed[:, cols] = rows_out.astype(BF16)
        image_copy(2, i).start()

        @pl.when(i > 0)
        def _():
            image_copy(3, i - 1).wait()

        for pair_at in range(pairs):
            base = pair_at * 2 * HEAD_DIM
            queries = mixed[:, base : base + 2 * HEAD_DIM]
            key_rows = mixed[:, local + base : local + base + 2 * HEAD_DIM]
            value_rows = mixed[:, 2 * local + base : 2 * local + base + 2 * HEAD_DIM]
            parts = []
            for side in range(2):
                mask = (lane // HEAD_DIM) == side
                head_q = jnp.where(mask, queries, jnp.zeros_like(queries))
                scores = lax.dot_general(head_q, key_rows, NT, preferred_element_type=F32)
                scores = jnp.where(key_at < seq, scores, -1e30)
                peak = jnp.max(scores, axis=1, keepdims=True)
                powers = jnp.exp2((scores - peak) * (HEAD_DIM**-0.5 * LOG2E))
                share = 1.0 / jnp.sum(powers, axis=1, keepdims=True)
                probs_low = (powers * share).astype(BF16)
                probs[2 * pair_at + side] = probs_low
                parts.append(jnp.dot(probs_low, value_rows, preferred_element_type=F32))
            joined = jnp.where((lane // HEAD_DIM) == 0, parts[0], parts[1])
            att[i, :, 2 * HEAD_DIM * pair_at : 2 * HEAD_DIM * (pair_at + 1)] = joined.astype(BF16)
        image_copy(3, i).start()
        image_copy(4, i).start()
        attended = att[i]

        @pl.when(i > 0)
        def _():
            given_copy(i - 1).wait_send()

        theirs[...] = lax.dot_general(attended, out_full[2 * local :, :], NT, preferred_element_type=F32).astype(BF16)
        given_copy(i).start()
        mine[...] = lax.dot_general(attended, out_full[: 2 * local, :], NT, preferred_element_type=F32)
        given_copy(i).wait_recv()
        pair[i] = (mine[...] + given[i].astype(F32)).astype(BF16)
        pair_copy(i).start()

        @pl.when(i == 0)
        def _():
            for code in codes[1:]:
                relay(2, code)

        @pl.when(i == 1)
        def _():
            for code in codes[:2]:
                relay(3, code)

    for code in codes[2:]:
        relay(3, code)
    outs = ((qkv_full, qkv_out), (out_full, outw_out), (vectors, vectors_out), (cot, cot_out), (move, move_out), (kept, kept_out), (fc1_grad, fc1_grad_out), (fc2_half, fc2_half_out), (fc2_grad, fc2_grad_out), (total.at[pl.ds(0, count - 1)], grad_out))

    def out_copy(k):
        return pltpu.make_async_copy(outs[k][0], outs[k][1], out_sem.at[k])

    for k in range(3):
        out_copy(k).start()
    bias_out[...] = jnp.zeros_like(bias_out)
    step = hidden_width // 4
    given_copy(count - 1).wait_send()
    arrived(2)
    arrived(3)

    @pl.loop(0, count)
    def _(i):
        y_copy(1, i).wait_recv()
        hand_copy(1, i).start()
        pair_copy(i).wait_recv()
        total[i, :, :local] = (pair[i, :, :local].astype(F32) + pair_in[i, :, local:].astype(F32)).astype(BF16)
        total[i, :, local : 2 * local] = (pair[i, :, local:].astype(F32) + pair_in[i, :, :local].astype(F32)).astype(BF16)
        total_copy(i).start()
        image_copy(1, i).wait()
        pair_copy(i).wait_send()
        here_copy(1, i).wait()
        core_copy(1, i).wait_recv()
        hand_copy(1, i).wait_recv()
        bias_out[1:2, :local] += jnp.sum(cot[i, :, :local].astype(F32), axis=0, keepdims=True)
        total_copy(i).wait_recv()
        image_copy(5, i).start()
        values = source[i].astype(F32) + total[i].astype(F32) + vectors[4:5, :]
        kept[i] = values[:, :local] + fc2_bias_ref[...]
        middle = jnp.sum(values, axis=1, keepdims=True) / width
        square = jnp.sum(values * values, axis=1, keepdims=True) / width
        inverse = lax.rsqrt(square - middle * middle + NORM_EPS)
        low[i] = ((values - middle) * inverse * vectors[2:3, :] + vectors[3:4, :]).astype(BF16)
        @pl.loop(0, 4)
        def _(part):
            cols = pl.ds(pl.multiple_of(part * step, step), step)
            pre_act = jnp.dot(low[i], fc1_full[:, cols], preferred_element_type=F32) + fc1_bias_ref[:, cols]
            gate = 0.5 * (1.0 + lax.erf(pre_act * ROOT_HALF))
            active[i, :, cols] = (pre_act * gate).astype(BF16)
            slope = gate + pre_act * jnp.exp(-0.5 * pre_act * pre_act) / ROOT_TWO_PI
            grad_pre = jnp.dot(cot[i], fc2_full[:, cols], preferred_element_type=F32) * slope
            bias_out[0:1, cols] += jnp.sum(grad_pre, axis=0, keepdims=True)
            gelu_grad[i, :, cols] = grad_pre.astype(BF16)

        @pl.when(i > 0)
        def _():
            given_back(i - 1).wait_send()

        theirs[...] = lax.dot_general(gelu_grad[i], fc1_full[2 * local :, :], NT, preferred_element_type=F32).astype(BF16)
        image_copy(5, i).wait()
        given_back(i).start()
        mine[...] = lax.dot_general(gelu_grad[i], fc1_full[: 2 * local, :], NT, preferred_element_type=F32)
        given_back(i).wait_recv()
        pair[i] = (mine[...] + given[i].astype(F32)).astype(BF16)

        @pl.when(i < count - 1)
        def _():
            pair_back(i).start()

    out_copy(3).start()
    late_copy = pltpu.make_async_copy(pair.at[count - 1], late_out, out_sem.at[10])
    late_copy.start()

    def weight_grad(out, left, right):
        @pl.loop(0, 4)
        def _(part):
            span = pl.ds(pl.multiple_of(part * local, local), local)
            terms = [lax.dot_general(left[i, :, span], right[i], TN, preferred_element_type=F32) for i in range(count)]
            out[span, :] = sum(terms[1:], terms[0]).astype(BF16)

    weight_grad(fc2_grad, cot, active)
    for code in odd_codes:
        half_copy(code).start()
    out_copy(8).start()
    given_back(count - 1).wait_send()

    @pl.loop(0, count)
    def _(i):
        @pl.when(i > 0)
        def _():
            move_copy(i - 1).wait_send()

        theirs[...] = lax.dot_general(active[i], fc2_full[2 * local :, :], NT, preferred_element_type=F32).astype(BF16)
        move_copy(i).start()
        mine[...] = lax.dot_general(active[i], fc2_full[: 2 * local, :], NT, preferred_element_type=F32)
        move_copy(i).wait_recv()
        kept[i] += mine[:, :local] + move_given[i, :, :local].astype(F32)
        move[i] = (mine[:, local:] + move_given[i, :, local:].astype(F32)).astype(BF16)

    out_copy(4).start()
    out_copy(5).start()
    weight_grad(fc1_grad, low, gelu_grad)
    out_copy(6).start()

    @pl.loop(0, count - 1)
    def _(i):
        pair_back(i).wait_recv()
        total_copy(i).wait_send()
        total[i, :, :local] = (pair[i, :, :local].astype(F32) + grad_in[i, :, local:].astype(F32)).astype(BF16)
        total[i, :, local : 2 * local] = (pair[i, :, local:].astype(F32) + grad_in[i, :, :local].astype(F32)).astype(BF16)
        total_back(i).start()

        @pl.when(i == count - 2)
        def _():
            for code in odd_codes:
                half_copy(code).wait_recv()
                there = row_place(crossed(row, code), row_count, place, block)
                mine_part = fc2_grad[there, half_of(dp, hidden_width)].astype(F32)
                fc2_half[there, :] = (mine_part + dp_in[there, :].astype(F32)).astype(BF16)
            for code in range(0, row_count, 2):
                there = row_place(crossed(row, code), row_count, place, block)
                fc2_half[there, :] = fc2_grad[there, half_of(dp, hidden_width)]
            out_copy(7).start()

    for i in range(count - 1):
        total_back(i).wait_recv()
    out_copy(9).start()
    for w in range(4):
        for code in codes:
            row_copy(w, code).wait_send()
            dp_copy(w, code).wait_send()
    for a, i in wanted:
        y_copy(a, i).wait_send()
        core_copy(a, i).wait_send()
        hand_copy(a, i).wait_send()
    for k in range(3):
        vector_copy(k).wait_send()
    total_copy(count - 1).wait_send()
    late_copy.wait()
    for i in range(count - 1):
        pair_back(i).wait_send()
        total_back(i).wait_send()
    for i in range(count):
        image_copy(0, i).wait()
        image_copy(4, i).wait()
    move_copy(count - 1).wait_send()
    image_copy(2, count - 1).wait()
    image_copy(3, count - 1).wait()
    for code in odd_codes:
        half_copy(code).wait_send()
    for k in range(len(outs)):
        out_copy(k).wait()


def ahead(images, cotangent, qkv_block, out_block, fc1_block, fc2_block, vectors, qv_bias, fc1_bias, fc2_bias, seq):
    count, rows, local = images.shape
    row_count = lax.axis_size("row")
    width = 4 * local
    heads = local // HEAD_DIM
    hidden = fc1_block.shape[1]

    def wide(*shape):
        return shape, BF16

    all_wide = wide(count, rows, width)
    all_pair = wide(count, rows, 2 * local)
    all_own = wide(count, rows, local)
    own_f32 = ((count, rows, local), F32)
    norm_rows = ((8, width), F32)
    outs = [
        all_wide, all_wide, all_wide, wide(count, rows, 3 * local), wide(count, heads, rows, rows), all_own, all_wide,
        wide(count - 1, rows, width), wide(3, width, local), wide(width, local), norm_rows, all_own, own_f32,
        wide(width, hidden), wide(width, hidden // 2), wide(width, hidden), wide(rows, 2 * local),
        ((2, hidden), F32),
    ]
    scratch = [
        all_wide, all_wide, all_wide, wide(rows, 3 * local), wide(heads, rows, rows), all_own,
        wide(rows, 2 * local), all_pair, ((rows, 2 * local), F32), all_pair, all_pair, all_wide,
        wide(3, width, local), wide(width, local), wide(width, hidden), wide(width, hidden), norm_rows, ((8, local), F32),
        wide(count, rows, hidden), wide(count, rows, hidden), all_pair, all_pair, own_f32, all_own,
        wide(width, hidden), wide(width, hidden), wide(width, hidden // 2), wide(width, hidden // 2),
    ]
    dma = pltpu.SemaphoreType.DMA
    whole = pl.BlockSpec(memory_space=pl.ANY)
    vmem = pl.BlockSpec(memory_space=pltpu.VMEM)
    return pl.pallas_call(
        functools.partial(ahead_kernel, (count, seq, rows, local, row_count)),
        out_shape=[jax.ShapeDtypeStruct(*s) for s in outs],
        in_specs=[whole] * 6 + [vmem] * 8,
        out_specs=[whole] * (len(outs) - 1) + [vmem],
        scratch_shapes=[pltpu.VMEM(*s) for s in scratch]
        + [dma((4, row_count))] * 4
        + [dma((4,)), dma((2, 4, count)), dma((2, 3, count)), dma((4,)), dma((3,))]
        + [dma((3, count)), dma((3, count)), dma((6, count)), dma((11,))]
        + [dma((4, count)), dma((4, count)), dma((row_count,)), dma((row_count,))],
        name="ahead",
        compiler_params=pltpu.CompilerParams(
            vmem_limit_bytes=63 * 2**20, collective_id=0, has_side_effects=True
        ),
    )(images, cotangent, qkv_block, out_block, fc1_block, fc2_block, *vectors, qv_bias, fc1_bias, fc2_bias)


def back_kernel(
    sizes,
    source_ref, total_ref, cot_ref, grad_ref, mixed_ref, probs_ref, att_ref, low_ref, move_ref, kept_ref,
    qkv_ref, outw_ref, fc1_grad_ref, fc2_half_ref, fc2_grad_ref, late_ref, vectors_ref, mlp_bias_ref,
    images_out, images_grad_out, small_out, qkv_out, outw_out, fc1_out, fc2_out,
    source, total, cot, grad_in, mixed, probs, att, low,
    hidden_low, mixed_grad, grad_hidden, normed1, inverse1, qkv_sum, outw_sum, k_turned, v_turned,
    theirs, given, mine, kept_grad, send, got, stat, stat_given, stat_pair, stat_in,
    late_pair, late_in, late_grad, move_in, kept, finished, qkv, outw, qkv_grad, outw_grad, small, small_in,
    half_fc2, half_fc1, half_outw, half_qkv, dp_fc2, dp_fc1, dp_outw, dp_qkv,
    row_fc2, row_fc1, row_outw, row_qkv, tot_fc2, tot_fc1, tot_outw, tot_qkv,
    early_sem, late_sem, once_sem, sum_send, sum_recv, move_send, move_recv, small_send, small_recv,
    dp_send, dp_recv, row_send, row_recv, tot_send, tot_recv, late_send, late_recv, out_sem,
):
    count, rows, local, row_count = sizes
    dp, row, place = lax.axis_index("dp"), lax.axis_index("row"), lax.axis_index("col")
    core_at = {"col": place + 1 - 2 * (place % 2)}
    y_at = {"col": (place + 2) % 4}
    dp_at = {"dp": 1 - dp}
    rounds = [dp_at]
    distance = 1
    while distance < row_count:
        rounds.append({"row": crossed(row, distance)})
        distance *= 2
    greet([core_at, y_at] + rounds)
    width = 4 * local
    block = width // row_count
    two = 2 * HEAD_DIM
    scale = HEAD_DIM**-0.5

    early = ((source_ref, source), (total_ref, total), (cot_ref, cot), (grad_ref, grad_in))
    late = ((mixed_ref, mixed), (probs_ref, probs), (att_ref, att), (low_ref, low))

    def early_load(k, i):
        here, there = early[k]
        return pltpu.make_async_copy(here.at[i], there.at[i % 2] if k == 0 else there, early_sem.at[k])

    def late_load(k, i):
        here, there = late[k]
        return pltpu.make_async_copy(here.at[i], there, late_sem.at[k])

    once = (
        (outw_ref, outw), (qkv_ref, qkv), (fc2_half_ref, half_fc2),
        (fc1_grad_ref.at[:, half_of(dp, fc1_grad_ref.shape[1])], half_fc1), (kept_ref, kept), (late_ref, late_pair),
    )

    def once_load(k):
        return pltpu.make_async_copy(once[k][0], once[k][1], once_sem.at[k])

    grads = (fc2_grad_ref, fc1_grad_ref, outw_grad, qkv_grad)
    halves = (half_fc2, half_fc1, half_outw, half_qkv)
    dp_ins = (dp_fc2, dp_fc1, dp_outw, dp_qkv)
    row_ins = (row_fc2, row_fc1, row_outw, row_qkv)
    tots = (tot_fc2, tot_fc1, tot_outw, tot_qkv)

    codes = sorted(range(1, row_count), key=lambda code: (code & -code, -code)) + [0]

    def rows_at(code):
        return row_place(crossed(row, code), row_count, place, block)

    def dp_copy(w, code):
        full = grads[w]
        return copy_to(
            part_at(full, rows_at(code), other_half_of(dp, full.shape[-1])),
            part_at(dp_ins[w], rows_at(code), slice(None)),
            dp_send.at[w, code],
            dp_recv.at[w, code],
            dp_at,
        )

    def row_copy(w, code):
        return copy_to(
            part_at(halves[w], rows_at(code), slice(None)),
            row_ins[w].at[code],
            row_send.at[w, code],
            row_recv.at[w, code],
            {"row": crossed(row, code & -code)},
        )

    def tot_copy(w):
        part = part_at(tots[w], slice(None), half_of(dp, tots[w].shape[-1]))
        return copy_to(part, part, tot_send.at[w], tot_recv.at[w], dp_at)

    def add_to(w, code, term):
        at = (slice(None), rows_at(code), slice(None)) if len(halves[w].shape) == 3 else (rows_at(code), slice(None))
        halves[w][at] = (halves[w][at].astype(F32) + term.astype(F32)).astype(BF16)

    def dp_sum(w, code):
        dp_copy(w, code).wait_recv()
        at = (slice(None), rows_at(code), slice(None)) if len(halves[w].shape) == 3 else (rows_at(code), slice(None))
        add_to(w, code, dp_ins[w][at])

    def row_take(w, code):
        row_copy(w, code).wait_recv()
        add_to(w, code - (code & -code), row_ins[w][code])

    def row_first(w):
        for code in codes[:-1]:
            if code % 2:
                row_copy(w, code).start()

    def row_next(w):
        for code in codes[:-1]:
            if code % 2 == 0:
                far = 1
                while far < code & -code:
                    row_take(w, code + far)
                    far *= 2
                row_copy(w, code).start()

    def row_last(w):
        far = 1
        while far < row_count:
            row_take(w, far)
            far *= 2
        own = halves[w][:, rows_at(0), :] if len(halves[w].shape) == 3 else halves[w][rows_at(0), :]
        cols = half_of(dp, tots[w].shape[-1])
        if len(halves[w].shape) == 3:
            tots[w][:, :, cols] = own
        else:
            tots[w][:, cols] = own
        tot_copy(w).start()

    def given_copy(i):
        return copy_to(theirs.at[i], given.at[i], sum_send.at[0, i], sum_recv.at[0, i], core_at)

    def stat_copy(i):
        return copy_to(stat.at[i], stat_given.at[i], sum_send.at[1, i], sum_recv.at[1, i], core_at)

    def got_copy(i):
        return copy_to(send.at[i], got.at[i], sum_send.at[2, i], sum_recv.at[2, i], y_at)

    def stat_pair_copy(i):
        return copy_to(stat_pair.at[i], stat_in.at[i], sum_send.at[3, i], sum_recv.at[3, i], y_at)

    late_y = copy_to(late_ref, late_in, late_send.at[0], late_recv.at[0], y_at)
    late_core = copy_to(
        late_grad.at[:, pl.ds(0, 2 * local)], late_grad.at[:, pl.ds(2 * local, 2 * local)], late_send.at[1], late_recv.at[1], core_at
    )

    def move_copy(i):
        return copy_to(move_ref.at[i], move_in.at[i], move_send.at[i], move_recv.at[i], y_at)

    def small_copy(s):
        return copy_to(small.at[s], small_in.at[s], small_send.at[s], small_recv.at[s], rounds[s])

    late_y.start()
    for k in range(4):
        early_load(k, 0).start()
    once_load(2).start()
    once_load(0).start()
    for k in range(4):
        late_load(k, 0).start()
    for k in (1, 3, 5, 4):
        once_load(k).start()
    for i in range(count):
        move_copy(i).start()
    for code in codes:
        if code % 2 == 0:
            dp_copy(0, code).start()
    for code in codes:
        dp_copy(1, code).start()

    small[0] = jnp.zeros_like(small[0])
    small[0, 7:8, :] = mlp_bias_ref[1:2, :local]
    for part in range(mlp_bias_ref.shape[1] // local):
        small[0, 8 + part : 9 + part, :] = mlp_bias_ref[0:1, part * local : (part + 1) * local]
    qkv_sum[...] = jnp.zeros_like(qkv_sum)
    outw_sum[...] = jnp.zeros_like(outw_sum)
    once_load(2).wait()
    row_first(0)

    def product_of(span):
        terms = [
            lax.dot_general(mixed_grad[:, c * local : (c + 1) * local], qkv[c, span, :], NT, preferred_element_type=F32)
            for c in range(3)
        ]
        return terms[0] + terms[1] + terms[2]

    lane = lax.broadcasted_iota(jnp.int32, (1, two), 1)
    down = lax.broadcasted_iota(jnp.int32, (two, two), 0)
    across = lax.broadcasted_iota(jnp.int32, (two, two), 1)
    eye = (down == across).astype(BF16)

    @pl.loop(0, count)
    def _(i):
        for k in range(3):
            early_load(k, i).wait()

        @pl.when(i < count - 1)
        def _():
            early_load(3, i).wait()

        @pl.when(i == count - 1)
        def _():
            late_core.wait_recv()
            grad_in[...] = late_grad[...]

        values = source[i % 2].astype(F32) + total[...].astype(F32) + vectors_ref[4:5, :]
        middle = jnp.sum(values, axis=1, keepdims=True) / width
        square = jnp.sum(values * values, axis=1, keepdims=True) / width
        inverse = lax.rsqrt(square - middle * middle + NORM_EPS)
        normed = (values - middle) * inverse
        grad = grad_in[...].astype(F32)
        small[0, 5:6, :] += jnp.sum(grad[:, :local] * normed[:, :local], axis=0, keepdims=True)
        small[0, 6:7, :] += jnp.sum(grad[:, :local], axis=0, keepdims=True)
        scaled = grad * vectors_ref[2:3, :]
        first = jnp.sum(scaled, axis=1, keepdims=True) / width
        second = jnp.sum(scaled * normed, axis=1, keepdims=True) / width
        whole_grad = cot[...].astype(F32) + inverse * (scaled - first - normed * second)
        grad_hidden[i] = whole_grad[:, :local]
        small[0, 2:3, :] += jnp.sum(whole_grad[:, :local], axis=0, keepdims=True)
        hidden_low[...] = whole_grad.astype(BF16)

        @pl.when(i + 1 < count)
        def _():
            for k in range(3):
                early_load(k, i + 1).start()

        @pl.when(i + 2 < count)
        def _():
            early_load(3, i + 1).start()

        for k in range(4):
            late_load(k, i).wait()

        @pl.when(i == 0)
        def _():
            once_load(0).wait()
            once_load(1).wait()

        grad_att = jnp.dot(hidden_low[...], outw[...], preferred_element_type=F32).astype(BF16)
        for part in range(4):
            span = slice(part * local, (part + 1) * local)
            outw_sum[span, :] += lax.dot_general(hidden_low[:, span], att[...], TN, preferred_element_type=F32)
        for pair in range(local // two):
            base = pair * two
            cols = slice(pair * two, (pair + 1) * two)
            queries = mixed[:, cols]
            key_rows = mixed[:, local + base : local + base + two]
            value_rows = mixed[:, 2 * local + base : 2 * local + base + two]
            pair_grad = grad_att[:, cols]
            q_turned = lax.dot_general(eye, queries, NT, preferred_element_type=F32).astype(BF16)
            grad_turned = lax.dot_general(eye, pair_grad, NT, preferred_element_type=F32).astype(BF16)
            product = pair_grad.astype(F32) * att[:, cols].astype(F32)
            parts = []
            for side in range(2):
                mask = (lane // HEAD_DIM) == side
                turn = slice(side * HEAD_DIM, (side + 1) * HEAD_DIM)
                head_grad = jnp.where(mask, pair_grad, jnp.zeros_like(pair_grad))
                grad_probs = lax.dot_general(head_grad, value_rows, NT, preferred_element_type=F32)
                delta = jnp.sum(jnp.where(mask, product, 0.0), axis=1, keepdims=True)
                probs_low = probs[2 * pair + side]
                grad_scores = (probs_low.astype(F32) * (grad_probs - delta)).astype(BF16)
                parts.append(jnp.dot(grad_scores, key_rows, preferred_element_type=F32))
                k_turned[turn, :] = jnp.dot(q_turned[turn, :], grad_scores, preferred_element_type=F32)
                v_turned[turn, :] = jnp.dot(grad_turned[turn, :], probs_low, preferred_element_type=F32)
            q_grad = jnp.where((lane // HEAD_DIM) == 0, parts[0], parts[1]) * scale
            v_grad = v_turned[...].T
            mixed_grad[:, cols] = q_grad.astype(BF16)
            mixed_grad[:, local + base : local + base + two] = (k_turned[...].T * scale).astype(BF16)
            mixed_grad[:, 2 * local + base : 2 * local + base + two] = v_grad.astype(BF16)
            small[0, 0:1, cols] += jnp.sum(q_grad, axis=0, keepdims=True)
            small[0, 1:2, cols] += jnp.sum(v_grad, axis=0, keepdims=True)
        @pl.when(i + 1 < count)
        def _():
            for k in range(3):
                late_load(k, i + 1).start()

        values = source[i % 2].astype(F32)
        middle = jnp.sum(values, axis=1, keepdims=True) / width
        square = jnp.sum(values * values, axis=1, keepdims=True) / width
        inverse = lax.rsqrt(square - middle * middle + NORM_EPS)
        normed = (values - middle) * inverse
        normed1[i] = normed[:, :local]
        inverse1[i] = inverse
        scaled_in = normed * vectors_ref[0:1, :]
        far = product_of(slice(2 * local, 4 * local))
        theirs[i] = far.astype(BF16)
        given_copy(i).start()
        near = product_of(slice(0, 2 * local))
        mine[...] = near
        first = jnp.sum(far * vectors_ref[0:1, 2 * local :], axis=1, keepdims=True) + jnp.sum(
            near * vectors_ref[0:1, : 2 * local], axis=1, keepdims=True
        )
        second = jnp.sum(far * scaled_in[:, 2 * local :], axis=1, keepdims=True) + jnp.sum(
            near * scaled_in[:, : 2 * local], axis=1, keepdims=True
        )
        spread = jnp.where(lane == 0, first, jnp.where(lane == 1, second, 0.0))
        stat[i] = spread.T[:8, :]
        stat_copy(i).start()
        for part in range(4):
            span = slice(part * local, (part + 1) * local)
            term = lax.dot_general(low[:, span], mixed_grad[...], TN, preferred_element_type=F32)
            for c in range(3):
                qkv_sum[c, span, :] += term[:, c * local : (c + 1) * local]

        @pl.when(i + 1 < count)
        def _():
            late_load(3, i + 1).start()

        given_copy(i).wait_recv()
        kept_grad[i] = mine[:, :local] + given[i, :, :local].astype(F32)
        send[i] = (mine[:, local:] + given[i, :, local:].astype(F32)).astype(BF16)
        got_copy(i).start()
        stat_copy(i).wait_recv()
        stat_pair[i] = stat[i] + stat_given[i]
        stat_pair_copy(i).start()

        @pl.when(i == 0)
        def _():
            for code in codes:
                if code % 2 == 0:
                    dp_sum(0, code)
            row_next(0)
            once_load(3).wait()

        @pl.when(i == 1)
        def _():
            for code in codes:
                if code % 2:
                    dp_sum(1, code)
                    row_copy(1, code).start()

        @pl.when(i == count - 2)
        def _():
            once_load(5).wait()
            late_y.wait_recv()
            late_grad[:, :local] = (late_pair[:, :local].astype(F32) + late_in[:, local:].astype(F32)).astype(BF16)
            late_grad[:, local : 2 * local] = (late_pair[:, local:].astype(F32) + late_in[:, :local].astype(F32)).astype(BF16)
            late_core.start()

    outw_grad[...] = outw_sum[...].astype(BF16)
    half_outw[...] = outw_grad[:, half_of(dp, local)]
    for code in codes:
        dp_copy(2, code).start()
    qkv_grad[...] = qkv_sum[...].astype(BF16)
    half_qkv[...] = qkv_grad[:, :, half_of(dp, local)]
    for code in codes:
        dp_copy(3, code).start()
    for code in codes:
        if code % 2 == 0:
            dp_sum(1, code)
    row_next(1)
    row_last(0)
    once_load(4).wait()

    @pl.loop(0, count)
    def _(i):
        move_copy(i).wait_recv()
        finished[i] = (kept[i] + move_in[i].astype(F32)).astype(BF16)

    for w in (2, 3):
        for code in codes:
            if code % 2:
                dp_sum(w, code)
                row_copy(w, code).start()
    row_last(1)

    for w in (2, 3):
        for code in codes:
            if code % 2 == 0:
                dp_sum(w, code)
        row_next(w)

    @pl.loop(0, count)
    def _(i):
        got_copy(i).wait_recv()
        stat_pair_copy(i).wait_recv()
        sums = stat_pair[i] + stat_in[i]
        spread = jnp.concatenate([sums, jnp.zeros((two - 8, rows), F32)], axis=0).T / width
        grad = kept_grad[i] + got[i].astype(F32)
        small[0, 3:4, :] += jnp.sum(grad * normed1[i], axis=0, keepdims=True)
        small[0, 4:5, :] += jnp.sum(grad, axis=0, keepdims=True)
        scaled = grad * vectors_ref[0:1, :local]
        grad_hidden[i] += inverse1[i] * (scaled - spread[:, 0:1] - normed1[i] * spread[:, 1:2])

    pltpu.make_async_copy(finished, images_out, out_sem.at[0]).start()
    pltpu.make_async_copy(grad_hidden, images_grad_out, out_sem.at[1]).start()
    small_copy(0).start()
    row_last(2)
    row_last(3)
    for s in range(len(rounds)):
        small_copy(s).wait_recv()
        small[s + 1] = small[s] + small_in[s]
        if s + 1 < len(rounds):
            small_copy(s + 1).start()
    outs = ((tot_fc2, fc2_out), (tot_fc1, fc1_out), (tot_outw, outw_out), (tot_qkv, qkv_out))
    for w, (here, there) in enumerate(outs):
        tot_copy(w).wait_recv()
        pltpu.make_async_copy(here, there, out_sem.at[2 + w]).start()
    small_out[...] = small[len(rounds)]
    for i in range(count):
        given_copy(i).wait_send()
        stat_copy(i).wait_send()
        got_copy(i).wait_send()
        stat_pair_copy(i).wait_send()
        move_copy(i).wait_send()
    late_y.wait_send()
    late_core.wait_send()
    for s in range(len(rounds)):
        small_copy(s).wait_send()
    for w in range(4):
        tot_copy(w).wait_send()
        for code in codes:
            if w or code % 2 == 0:
                dp_copy(w, code).wait_send()
            if code:
                row_copy(w, code).wait_send()
    for k, (here, there) in enumerate(((finished, images_out), (grad_hidden, images_grad_out), *outs)):
        pltpu.make_async_copy(here, there, out_sem.at[k]).wait()


def back(
    source, total, cot, grad_low, mixed, probs, att, low, move, kept, qkv, outw, fc1_grad, fc2_half, fc2_grad, late, vectors, mlp_bias
):
    count, rows, width = source.shape
    local = width // 4
    row_count = lax.axis_size("row")
    block = width // row_count
    hidden = fc1_grad.shape[1]
    qkv_width = 3 * local
    heads = local // HEAD_DIM
    rounds = row_count.bit_length()
    outs = [
        ((count, rows, local), BF16), ((count, rows, local), F32), ((16, local), F32),
        ((3, block, local), BF16), ((block, local), BF16), ((block, hidden), BF16), ((block, hidden), BF16),
    ]
    own_f32 = ((count, rows, local), F32)
    own_low = ((count, rows, local), BF16)
    pair_low = ((count, rows, 2 * local), BF16)
    stat = ((count, 8, rows), F32)
    wide = ((rows, width), BF16)
    turned = ((2 * HEAD_DIM, rows), F32)
    columns = (((), hidden), ((), hidden), ((), local), ((3,), local))
    scratch = [
        ((2, rows, width), BF16), wide, wide, wide, ((rows, qkv_width), BF16), ((heads, rows, rows), BF16), ((rows, local), BF16), wide,
        wide, ((rows, qkv_width), BF16), own_f32, own_f32, ((count, rows, 1), F32),
        ((3, width, local), F32), ((width, local), F32), turned, turned,
        pair_low, pair_low, ((rows, 2 * local), F32), own_f32, own_low, own_low, stat, stat, stat, stat,
        ((rows, 2 * local), BF16), ((rows, 2 * local), BF16), wide, own_low, own_f32, own_low, ((3, width, local), BF16), ((width, local), BF16),
        ((3, width, local), BF16), ((width, local), BF16), ((rounds + 1, 16, local), F32), ((rounds, 16, local), F32),
        *[((*lead, width, c // 2), BF16) for lead, c in columns],
        *[((*lead, width, c // 2), BF16) for lead, c in columns],
        *[((row_count, *lead, block, c // 2), BF16) for lead, c in columns],
        *[((*lead, block, c), BF16) for lead, c in columns],
    ]
    dma = pltpu.SemaphoreType.DMA
    whole = pl.BlockSpec(memory_space=pl.ANY)
    vmem = pl.BlockSpec(memory_space=pltpu.VMEM)
    return pl.pallas_call(
        functools.partial(back_kernel, (count, rows, local, row_count)),
        out_shape=[jax.ShapeDtypeStruct(*s) for s in outs],
        in_specs=[whole] * 16 + [vmem] * 2,
        out_specs=[whole, whole, vmem] + [whole] * 4,
        scratch_shapes=[pltpu.VMEM(*s) for s in scratch]
        + [dma((4,)), dma((4,)), dma((6,)), dma((4, count)), dma((4, count)), dma((count,)), dma((count,)), dma((rounds,)), dma((rounds,))]
        + [dma((4, row_count))] * 4
        + [dma((4,)), dma((4,)), dma((2,)), dma((2,)), dma((6,))],
        name="back",
        compiler_params=pltpu.CompilerParams(
            vmem_limit_bytes=63 * 2**20, collective_id=2, has_side_effects=True
        ),
    )(source, total, cot, grad_low, mixed, probs, att, low, move, kept, qkv, outw, fc1_grad, fc2_half, fc2_grad, late, vectors, mlp_bias)


def adam_step(weight, grad, momentum, variance):
    moment_new = BETA_FIRST * momentum + (1.0 - BETA_FIRST) * grad
    second_new = BETA_SECOND * variance + (1.0 - BETA_SECOND) * grad * grad
    corrected = moment_new / (1.0 - BETA_FIRST**STEP)
    second_corrected = second_new / (1.0 - BETA_SECOND**STEP)
    master = weight.astype(jnp.float32)
    updated = master - LEARN_RATE * (
        corrected / (jnp.sqrt(second_corrected) + ADAM_EPS) + WEIGHT_DECAY * master
    )
    return (updated, moment_new, second_new)


def per_device(
    images_in,
    cotangent,
    first_gain,
    first_shift,
    second_gain,
    second_shift,
    qkv_weight,
    qv_bias,
    out_weight,
    out_bias,
    fc1_weight,
    fc1_bias,
    fc2_weight,
    fc2_bias,
    qkv_momentum,
    qkv_variance,
    out_momentum,
    out_variance,
    fc1_momentum,
    fc1_variance,
    fc2_momentum,
    fc2_variance,
):
    image_count, seq, local = images_in.shape
    width = 4 * local
    rows = -(-seq // ROW_TILE) * ROW_TILE
    place = lax.axis_index("col")

    vectors = [v[None] for v in (first_gain, first_shift, second_gain, second_shift, out_bias)]
    (
        source_all, cot_all, low_all, mixed_all, probs_all, att_all, total_all, grad_low2, qkv_full, out_full, vectors,
        move, kept, fc1_grad, fc2_half, fc2_grad, late, mlp_bias,
    ) = ahead(
        jnp.pad(images_in, ((0, 0), (0, rows - seq), (0, 0))),
        jnp.pad(cotangent, ((0, 0), (0, rows - seq), (0, 0))),
        qkv_weight.transpose(1, 0, 2),
        out_weight,
        fc1_weight,
        fc2_weight,
        vectors,
        qv_bias,
        fc1_bias[None],
        fc2_bias[None],
        seq,
    )
    images_out, images_grad, small, qkv_total, out_total, fc1_total, fc2_total = back(
        source_all, total_all, cot_all, grad_low2, mixed_all, probs_all, att_all, low_all, move, kept,
        qkv_full, out_full, fc1_grad, fc2_half, fc2_grad, late, vectors, mlp_bias,
    )
    qkv_total = qkv_total.transpose(1, 0, 2).astype(F32)
    out_total, fc1_total, fc2_total = (t.astype(F32) for t in (out_total, fc1_total, fc2_total))
    qkv_new = adam_step(qkv_weight, qkv_total, qkv_momentum, qkv_variance)
    out_new = adam_step(out_weight, out_total, out_momentum, out_variance)
    fc1_new = adam_step(fc1_weight, fc1_total, fc1_momentum, fc1_variance)
    fc2_new = adam_step(fc2_weight, fc2_total, fc2_momentum, fc2_variance)
    return (
        images_out[:, :seq],
        images_grad[:, :seq],
        qkv_total,
        out_total,
        fc1_total,
        fc2_total,
        small[0:2],
        small[2],
        small[8:12].reshape(-1),
        small[7],
        small[3],
        small[4],
        small[5],
        small[6],
        qkv_new[0],
        out_new[0],
        fc1_new[0],
        fc2_new[0],
        qkv_new[1],
        out_new[1],
        fc1_new[1],
        fc2_new[1],
        qkv_new[2],
        out_new[2],
        fc1_new[2],
        fc2_new[2],
    )


def solution(mesh):
    return jax.shard_map(
        per_device,
        mesh=mesh,
        in_specs=(
            P(("dp", "row"), None, "col"),
            P(("dp", "row"), None, "col"),
            P("col"),
            P("col"),
            P("col"),
            P("col"),
            P("row", None, "col"),
            P(None, "col"),
            P("row", "col"),
            P("col"),
            P("row", "col"),
            P("col"),
            P("row", "col"),
            P("col"),
            P("row", None, "col"),
            P("row", None, "col"),
            P("row", "col"),
            P("row", "col"),
            P("row", "col"),
            P("row", "col"),
            P("row", "col"),
            P("row", "col"),
        ),
        out_specs=(
            P(("dp", "row"), None, "col"),
            P(("dp", "row"), None, "col"),
            P("row", None, "col"),
            P("row", "col"),
            P("row", "col"),
            P("row", "col"),
            P(None, "col"),
            P("col"),
            P("col"),
            P("col"),
            P("col"),
            P("col"),
            P("col"),
            P("col"),
            P("row", None, "col"),
            P("row", "col"),
            P("row", "col"),
            P("row", "col"),
            P("row", None, "col"),
            P("row", "col"),
            P("row", "col"),
            P("row", "col"),
            P("row", None, "col"),
            P("row", "col"),
            P("row", "col"),
            P("row", "col"),
        ),
        check_vma=False,
    )
```

```python
import functools

import jax
import jax.numpy as jnp
from jax import lax
from jax.experimental import pallas as pl
from jax.experimental.pallas import tpu as pltpu
from jax.sharding import PartitionSpec as P

HEAD_DIM = 64
STEP = 3


NORM_EPS = 1e-06
LEARN_RATE = 0.02
BETA_FIRST = 0.9
BETA_SECOND = 0.999
ADAM_EPS = 1e-08
WEIGHT_DECAY = 0.05
ROOT_HALF = 0.7071067811865476
ROOT_TWO_PI = 2.5066282746310002
LOG2E = 1.4426950408889634
ROW_TILE = 16
MESH = pl.DeviceIdType.MESH
NT = (((1,), (1,)), ((), ()))
TN = (((0,), (0,)), ((), ()))
F32 = jnp.float32
BF16 = jnp.bfloat16


def copy_to(src, dst, send, recv, where):
    return pltpu.make_async_remote_copy(
        src_ref=src, dst_ref=dst, send_sem=send, recv_sem=recv, device_id=where, device_id_type=MESH
    )


def rel_place(quarter, place):
    return (quarter // 2 + place // 2) % 2 + 2 * ((quarter % 2 + place % 2) % 2)


def crossed(row, code):
    distance = 1
    while distance <= code:
        if code & distance:
            row = row + distance * (1 - 2 * ((row // distance) % 2))
        distance *= 2
    return row


def half_of(dp, full_width):
    half = full_width // 2
    return pl.ds(pl.multiple_of(dp * half, half), half)


def other_half_of(dp, full_width):
    half = full_width // 2
    return pl.ds(pl.multiple_of((1 - dp) * half, half), half)


def row_place(owner, row_count, place, block):
    per = row_count // 4
    at = (rel_place(owner // per, place) * per + owner % per) * block
    return pl.ds(pl.multiple_of(at, block), block)


def part_at(full, rows, cols):
    return full.at[:, rows, cols] if len(full.shape) == 3 else full.at[rows, cols]


def greet(partners):
    barrier = pltpu.get_barrier_semaphore()
    for partner in partners:
        pl.semaphore_signal(barrier, inc=1, device_id=partner, device_id_type=MESH)
    pl.semaphore_wait(barrier, len(partners))


def ahead_kernel(
    sizes,
    images_ref, cot_ref, qkv_ref, out_ref, fc1_ref, fc2_ref,
    gain1_ref, shift1_ref, gain2_ref, shift2_ref, out_bias_ref, qv_bias_ref, fc1_bias_ref, fc2_bias_ref,
    source_out, cot_out, low_out, mixed_out, probs_out, att_out, total_out, grad_out, qkv_out, outw_out, vectors_out,
    move_out, kept_out, fc1_grad_out, fc2_half_out, fc2_grad_out, late_out, bias_out,
    source, cot, low, mixed, probs, att, theirs, given, mine, pair, pair_in, total, qkv_full, out_full, fc1_full, fc2_full, vectors, vectors_ref,
    active, gelu_grad, grad_in, move_given, kept, move, fc1_grad, fc2_grad, dp_in, fc2_half,
    row_send, row_recv, dp_send, dp_recv, own_sem, in_send, in_recv, vec_send, vec_recv, sum_send, sum_recv, image_sem, out_sem,
    back_send, back_recv, half_send, half_recv,
):
    count, seq, rows, local, row_count = sizes
    dp, row, place = lax.axis_index("dp"), lax.axis_index("row"), lax.axis_index("col")
    core_at = {"col": place + 1 - 2 * (place % 2)}
    y_at = {"col": (place + 2) % 4}
    dp_at = {"dp": 1 - dp}
    codes = sorted(range(1, row_count), key=lambda code: -(code & -code))
    fars = [code for code in codes if code & -code == code]
    greet([core_at, y_at, dp_at] + [{"row": crossed(row, far)} for far in fars])
    block = out_ref.shape[0]
    width = 4 * local
    weights = ((qkv_ref, qkv_full), (out_ref, out_full), (fc1_ref, fc1_full), (fc2_ref, fc2_full))

    def row_copy(w, code):
        ref, full = weights[w]
        cols = half_of(dp, full.shape[-1])
        far = code & -code
        held = part_at(full, row_place(crossed(row, code - far), row_count, place, block), cols)
        return copy_to(
            part_at(ref, slice(None), cols) if code == far else held, held, row_send.at[w, code], row_recv.at[w, code], {"row": crossed(row, far)}
        )

    def dp_copy(w, code):
        _, full = weights[w]
        part = part_at(full, row_place(crossed(row, code), row_count, place, block), half_of(dp, full.shape[-1]))
        return copy_to(part, part, dp_send.at[w, code], dp_recv.at[w, code], dp_at)

    def own_copy(w):
        ref, full = weights[w]
        return pltpu.make_async_copy(ref, part_at(full, row_place(row, row_count, place, block), slice(None)), own_sem.at[w])

    inputs = ((images_ref, source), (cot_ref, cot))

    def y_copy(a, i):
        ref, full = inputs[a]
        return copy_to(ref.at[i], full.at[i, :, pl.ds(local, local)], in_send.at[a, 0, i], in_recv.at[a, 0, i], y_at)

    def core_copy(a, i):
        ref, full = inputs[a]
        return copy_to(ref.at[i], full.at[i, :, pl.ds(2 * local, local)], in_send.at[a, 1, i], in_recv.at[a, 1, i], core_at)

    def hand_copy(a, i):
        _, full = inputs[a]
        return copy_to(
            full.at[i, :, pl.ds(local, local)],
            full.at[i, :, pl.ds(3 * local, local)],
            in_send.at[a, 2, i],
            in_recv.at[a, 2, i],
            core_at,
        )

    def here_copy(a, i):
        ref, full = inputs[a]
        return pltpu.make_async_copy(ref.at[i], full.at[i, :, pl.ds(0, local)], in_send.at[a, 3, i])

    def vector_copy(k):
        src = vectors.at[:, pl.ds(local, local)] if k == 2 else vectors_ref
        at = (local, 2 * local, 3 * local)[k]
        return copy_to(
            src, vectors.at[:, pl.ds(at, local)], vec_send.at[k], vec_recv.at[k], (y_at, core_at, core_at)[k]
        )

    for k, vector in enumerate((gain1_ref, shift1_ref, gain2_ref, shift2_ref, out_bias_ref)):
        vectors_ref[k : k + 1, :] = vector[...]
    vectors_ref[5:8, :] = jnp.zeros((3, local), F32)
    vector_here = pltpu.make_async_copy(vectors_ref, vectors.at[:, pl.ds(0, local)], vec_send.at[3])

    def given_copy(i):
        return copy_to(theirs, given.at[i], sum_send.at[0, i], sum_recv.at[0, i], core_at)

    def given_back(i):
        return copy_to(theirs, given.at[i], back_send.at[0, i], back_recv.at[0, i], core_at)

    def pair_back(i):
        return copy_to(pair.at[i], grad_in.at[i], back_send.at[1, i], back_recv.at[1, i], y_at)

    def total_back(i):
        return copy_to(
            total.at[i, :, pl.ds(0, 2 * local)],
            total.at[i, :, pl.ds(2 * local, 2 * local)],
            back_send.at[2, i],
            back_recv.at[2, i],
            core_at,
        )

    def move_copy(i):
        return copy_to(theirs, move_given.at[i], back_send.at[3, i], back_recv.at[3, i], core_at)

    hidden_width = fc1_full.shape[1]

    odd_codes = sorted(range(1, row_count, 2), reverse=True)

    def half_copy(code):
        there = row_place(crossed(row, code), row_count, place, block)
        return copy_to(
            fc2_grad.at[there, other_half_of(dp, hidden_width)], dp_in.at[there, :], half_send.at[code], half_recv.at[code], dp_at
        )

    def pair_copy(i):
        return copy_to(pair.at[i], pair_in.at[i], sum_send.at[1, i], sum_recv.at[1, i], y_at)

    def total_copy(i):
        return copy_to(
            total.at[i, :, pl.ds(0, 2 * local)],
            total.at[i, :, pl.ds(2 * local, 2 * local)],
            sum_send.at[2, i],
            sum_recv.at[2, i],
            core_at,
        )

    def start_own(w):
        for far in fars:
            row_copy(w, far).start()

    def relay(w, code):
        row_copy(w, code).wait_recv()
        for far in fars:
            if far < code & -code:
                row_copy(w, code + far).start()
        dp_copy(w, code).start()

    def arrived(w):
        for code in codes:
            dp_copy(w, code).wait_recv()
        own_copy(w).wait()

    kinds = ((source, source_out), (low, low_out), (mixed, mixed_out), (probs, probs_out), (att, att_out), (total, total_out))

    def image_copy(k, i):
        here, there = kinds[k]
        return pltpu.make_async_copy(here if k in (2, 3) else here.at[i], there.at[i], image_sem.at[k, i])

    wanted = [(a, i) for a in range(2) for i in range(count)]
    start_own(0)
    start_own(1)
    vector_copy(0).start()
    for a, i in wanted:
        y_copy(a, i).start()
    vector_copy(1).start()
    vector_here.start()
    for a, i in wanted:
        core_copy(a, i).start()
        here_copy(a, i).start()
    for w in range(4):
        own_copy(w).start()
    vector_copy(0).wait_recv()
    vector_copy(2).start()
    relay(0, codes[0])
    relay(1, codes[0])
    start_own(2)
    vector_here.wait()
    vector_copy(1).wait_recv()
    vector_copy(2).wait_recv()

    @pl.loop(0, count)
    def _(i):
        y_copy(0, i).wait_recv()
        hand_copy(0, i).start()
        here_copy(0, i).wait()
        core_copy(0, i).wait_recv()
        hand_copy(0, i).wait_recv()
        image_copy(0, i).start()
        values = source[i].astype(F32)
        middle = jnp.sum(values, axis=1, keepdims=True) / width
        square = jnp.sum(values * values, axis=1, keepdims=True) / width
        inverse = lax.rsqrt(square - middle * middle + NORM_EPS)
        low[i] = ((values - middle) * inverse * vectors[0:1, :] + vectors[1:2, :]).astype(BF16)
        image_copy(1, i).start()

        @pl.when(i == 0)
        def _():
            for code in codes[1:]:
                relay(0, code)
                relay(1, code)

    relay(2, codes[0])
    start_own(3)
    arrived(0)
    arrived(1)

    lane = lax.broadcasted_iota(jnp.int32, (1, 2 * HEAD_DIM), 1)
    key_at = lax.broadcasted_iota(jnp.int32, (1, rows), 1)
    pairs = local // (2 * HEAD_DIM)

    @pl.loop(0, count)
    def _(i):
        @pl.when(i > 0)
        def _():
            image_copy(2, i - 1).wait()

        for c in range(3):
            cols = slice(c * local, (c + 1) * local)
            rows_out = jnp.dot(low[i], qkv_full[c], preferred_element_type=F32)
            if c != 1:
                rows_out += qv_bias_ref[c // 2 : c // 2 + 1, :]
            mixed[:, cols] = rows_out.astype(BF16)
        image_copy(2, i).start()

        @pl.when(i > 0)
        def _():
            image_copy(3, i - 1).wait()

        for pair_at in range(pairs):
            base = pair_at * 2 * HEAD_DIM
            queries = mixed[:, base : base + 2 * HEAD_DIM]
            key_rows = mixed[:, local + base : local + base + 2 * HEAD_DIM]
            value_rows = mixed[:, 2 * local + base : 2 * local + base + 2 * HEAD_DIM]
            parts = []
            for side in range(2):
                mask = (lane // HEAD_DIM) == side
                head_q = jnp.where(mask, queries, jnp.zeros_like(queries))
                scores = lax.dot_general(head_q, key_rows, NT, preferred_element_type=F32)
                scores = jnp.where(key_at < seq, scores, -1e30)
                peak = jnp.max(scores, axis=1, keepdims=True)
                powers = jnp.exp2((scores - peak) * (HEAD_DIM**-0.5 * LOG2E))
                share = 1.0 / jnp.sum(powers, axis=1, keepdims=True)
                probs_low = (powers * share).astype(BF16)
                probs[2 * pair_at + side] = probs_low
                parts.append(jnp.dot(probs_low, value_rows, preferred_element_type=F32))
            joined = jnp.where((lane // HEAD_DIM) == 0, parts[0], parts[1])
            att[i, :, 2 * HEAD_DIM * pair_at : 2 * HEAD_DIM * (pair_at + 1)] = joined.astype(BF16)
        image_copy(3, i).start()
        image_copy(4, i).start()
        attended = att[i]

        @pl.when(i > 0)
        def _():
            given_copy(i - 1).wait_send()

        theirs[...] = lax.dot_general(attended, out_full[2 * local :, :], NT, preferred_element_type=F32).astype(BF16)
        given_copy(i).start()
        mine[...] = lax.dot_general(attended, out_full[: 2 * local, :], NT, preferred_element_type=F32)
        given_copy(i).wait_recv()
        pair[i] = (mine[...] + given[i].astype(F32)).astype(BF16)
        pair_copy(i).start()

        @pl.when(i == 0)
        def _():
            for code in codes[1:]:
                relay(2, code)

        @pl.when(i == 1)
        def _():
            for code in codes[:2]:
                relay(3, code)

    for code in codes[2:]:
        relay(3, code)
    outs = ((qkv_full, qkv_out), (out_full, outw_out), (vectors, vectors_out), (cot, cot_out), (move, move_out), (kept, kept_out), (fc1_grad, fc1_grad_out), (fc2_half, fc2_half_out), (fc2_grad, fc2_grad_out), (total.at[pl.ds(0, count - 1)], grad_out))

    def out_copy(k):
        return pltpu.make_async_copy(outs[k][0], outs[k][1], out_sem.at[k])

    for k in range(3):
        out_copy(k).start()
    bias_out[...] = jnp.zeros_like(bias_out)
    step = hidden_width // 4
    given_copy(count - 1).wait_send()
    arrived(2)
    arrived(3)

    @pl.loop(0, count)
    def _(i):
        y_copy(1, i).wait_recv()
        hand_copy(1, i).start()
        pair_copy(i).wait_recv()
        total[i, :, :local] = (pair[i, :, :local].astype(F32) + pair_in[i, :, local:].astype(F32)).astype(BF16)
        total[i, :, local : 2 * local] = (pair[i, :, local:].astype(F32) + pair_in[i, :, :local].astype(F32)).astype(BF16)
        total_copy(i).start()
        image_copy(1, i).wait()
        pair_copy(i).wait_send()
        here_copy(1, i).wait()
        core_copy(1, i).wait_recv()
        hand_copy(1, i).wait_recv()
        bias_out[1:2, :local] += jnp.sum(cot[i, :, :local].astype(F32), axis=0, keepdims=True)
        total_copy(i).wait_recv()
        image_copy(5, i).start()
        values = source[i].astype(F32) + total[i].astype(F32) + vectors[4:5, :]
        kept[i] = values[:, :local] + fc2_bias_ref[...]
        middle = jnp.sum(values, axis=1, keepdims=True) / width
        square = jnp.sum(values * values, axis=1, keepdims=True) / width
        inverse = lax.rsqrt(square - middle * middle + NORM_EPS)
        low[i] = ((values - middle) * inverse * vectors[2:3, :] + vectors[3:4, :]).astype(BF16)
        @pl.loop(0, 4)
        def _(part):
            cols = pl.ds(pl.multiple_of(part * step, step), step)
            pre_act = jnp.dot(low[i], fc1_full[:, cols], preferred_element_type=F32) + fc1_bias_ref[:, cols]
            gate = 0.5 * (1.0 + lax.erf(pre_act * ROOT_HALF))
            active[i, :, cols] = (pre_act * gate).astype(BF16)
            slope = gate + pre_act * jnp.exp(-0.5 * pre_act * pre_act) / ROOT_TWO_PI
            grad_pre = jnp.dot(cot[i], fc2_full[:, cols], preferred_element_type=F32) * slope
            bias_out[0:1, cols] += jnp.sum(grad_pre, axis=0, keepdims=True)
            gelu_grad[i, :, cols] = grad_pre.astype(BF16)

        @pl.when(i > 0)
        def _():
            given_back(i - 1).wait_send()

        theirs[...] = lax.dot_general(gelu_grad[i], fc1_full[2 * local :, :], NT, preferred_element_type=F32).astype(BF16)
        image_copy(5, i).wait()
        given_back(i).start()
        mine[...] = lax.dot_general(gelu_grad[i], fc1_full[: 2 * local, :], NT, preferred_element_type=F32)
        given_back(i).wait_recv()
        pair[i] = (mine[...] + given[i].astype(F32)).astype(BF16)

        @pl.when(i < count - 1)
        def _():
            pair_back(i).start()

    out_copy(3).start()
    late_copy = pltpu.make_async_copy(pair.at[count - 1], late_out, out_sem.at[10])
    late_copy.start()

    def weight_grad(out, left, right):
        @pl.loop(0, 4)
        def _(part):
            span = pl.ds(pl.multiple_of(part * local, local), local)
            terms = [lax.dot_general(left[i, :, span], right[i], TN, preferred_element_type=F32) for i in range(count)]
            out[span, :] = sum(terms[1:], terms[0]).astype(BF16)

    weight_grad(fc2_grad, cot, active)
    for code in odd_codes:
        half_copy(code).start()
    out_copy(8).start()
    given_back(count - 1).wait_send()

    @pl.loop(0, count)
    def _(i):
        @pl.when(i > 0)
        def _():
            move_copy(i - 1).wait_send()

        theirs[...] = lax.dot_general(active[i], fc2_full[2 * local :, :], NT, preferred_element_type=F32).astype(BF16)
        move_copy(i).start()
        mine[...] = lax.dot_general(active[i], fc2_full[: 2 * local, :], NT, preferred_element_type=F32)
        move_copy(i).wait_recv()
        kept[i] += mine[:, :local] + move_given[i, :, :local].astype(F32)
        move[i] = (mine[:, local:] + move_given[i, :, local:].astype(F32)).astype(BF16)

    out_copy(4).start()
    out_copy(5).start()
    weight_grad(fc1_grad, low, gelu_grad)
    out_copy(6).start()

    @pl.loop(0, count - 1)
    def _(i):
        pair_back(i).wait_recv()
        total_copy(i).wait_send()
        total[i, :, :local] = (pair[i, :, :local].astype(F32) + grad_in[i, :, local:].astype(F32)).astype(BF16)
        total[i, :, local : 2 * local] = (pair[i, :, local:].astype(F32) + grad_in[i, :, :local].astype(F32)).astype(BF16)
        total_back(i).start()

        @pl.when(i == count - 2)
        def _():
            for code in odd_codes:
                half_copy(code).wait_recv()
                there = row_place(crossed(row, code), row_count, place, block)
                mine_part = fc2_grad[there, half_of(dp, hidden_width)].astype(F32)
                fc2_half[there, :] = (mine_part + dp_in[there, :].astype(F32)).astype(BF16)
            for code in range(0, row_count, 2):
                there = row_place(crossed(row, code), row_count, place, block)
                fc2_half[there, :] = fc2_grad[there, half_of(dp, hidden_width)]
            out_copy(7).start()

    for i in range(count - 1):
        total_back(i).wait_recv()
    out_copy(9).start()
    for w in range(4):
        for code in codes:
            row_copy(w, code).wait_send()
            dp_copy(w, code).wait_send()
    for a, i in wanted:
        y_copy(a, i).wait_send()
        core_copy(a, i).wait_send()
        hand_copy(a, i).wait_send()
    for k in range(3):
        vector_copy(k).wait_send()
    total_copy(count - 1).wait_send()
    late_copy.wait()
    for i in range(count - 1):
        pair_back(i).wait_send()
        total_back(i).wait_send()
    for i in range(count):
        image_copy(0, i).wait()
        image_copy(4, i).wait()
    move_copy(count - 1).wait_send()
    image_copy(2, count - 1).wait()
    image_copy(3, count - 1).wait()
    for code in odd_codes:
        half_copy(code).wait_send()
    for k in range(len(outs)):
        out_copy(k).wait()


def ahead(images, cotangent, qkv_block, out_block, fc1_block, fc2_block, vectors, qv_bias, fc1_bias, fc2_bias, seq):
    count, rows, local = images.shape
    row_count = lax.axis_size("row")
    width = 4 * local
    heads = local // HEAD_DIM
    hidden = fc1_block.shape[1]

    def wide(*shape):
        return shape, BF16

    all_wide = wide(count, rows, width)
    all_pair = wide(count, rows, 2 * local)
    all_own = wide(count, rows, local)
    own_f32 = ((count, rows, local), F32)
    norm_rows = ((8, width), F32)
    outs = [
        all_wide, all_wide, all_wide, wide(count, rows, 3 * local), wide(count, heads, rows, rows), all_own, all_wide,
        wide(count - 1, rows, width), wide(3, width, local), wide(width, local), norm_rows, all_own, own_f32,
        wide(width, hidden), wide(width, hidden // 2), wide(width, hidden), wide(rows, 2 * local),
        ((2, hidden), F32),
    ]
    scratch = [
        all_wide, all_wide, all_wide, wide(rows, 3 * local), wide(heads, rows, rows), all_own,
        wide(rows, 2 * local), all_pair, ((rows, 2 * local), F32), all_pair, all_pair, all_wide,
        wide(3, width, local), wide(width, local), wide(width, hidden), wide(width, hidden), norm_rows, ((8, local), F32),
        wide(count, rows, hidden), wide(count, rows, hidden), all_pair, all_pair, own_f32, all_own,
        wide(width, hidden), wide(width, hidden), wide(width, hidden // 2), wide(width, hidden // 2),
    ]
    dma = pltpu.SemaphoreType.DMA
    whole = pl.BlockSpec(memory_space=pl.ANY)
    vmem = pl.BlockSpec(memory_space=pltpu.VMEM)
    return pl.pallas_call(
        functools.partial(ahead_kernel, (count, seq, rows, local, row_count)),
        out_shape=[jax.ShapeDtypeStruct(*s) for s in outs],
        in_specs=[whole] * 6 + [vmem] * 8,
        out_specs=[whole] * (len(outs) - 1) + [vmem],
        scratch_shapes=[pltpu.VMEM(*s) for s in scratch]
        + [dma((4, row_count))] * 4
        + [dma((4,)), dma((2, 4, count)), dma((2, 3, count)), dma((4,)), dma((3,))]
        + [dma((3, count)), dma((3, count)), dma((6, count)), dma((11,))]
        + [dma((4, count)), dma((4, count)), dma((row_count,)), dma((row_count,))],
        name="ahead",
        compiler_params=pltpu.CompilerParams(
            vmem_limit_bytes=63 * 2**20, collective_id=0, has_side_effects=True
        ),
    )(images, cotangent, qkv_block, out_block, fc1_block, fc2_block, *vectors, qv_bias, fc1_bias, fc2_bias)


def back_kernel(
    sizes,
    source_ref, total_ref, cot_ref, grad_ref, mixed_ref, probs_ref, att_ref, low_ref, move_ref, kept_ref,
    qkv_ref, outw_ref, fc1_grad_ref, fc2_half_ref, fc2_grad_ref, late_ref, vectors_ref, mlp_bias_ref,
    images_out, images_grad_out, small_out, qkv_out, outw_out, fc1_out, fc2_out,
    source, total, cot, grad_in, mixed, probs, att, low,
    hidden_low, mixed_grad, grad_hidden, normed1, inverse1, qkv_sum, outw_sum, k_turned, v_turned,
    theirs, given, mine, kept_grad, send, got, stat, stat_given, stat_pair, stat_in,
    late_pair, late_in, late_grad, move_in, kept, finished, qkv, outw, qkv_grad, outw_grad, small, small_in,
    half_fc2, half_fc1, half_outw, half_qkv, dp_fc2, dp_fc1, dp_outw, dp_qkv,
    row_fc2, row_fc1, row_outw, row_qkv, tot_fc2, tot_fc1, tot_outw, tot_qkv,
    early_sem, late_sem, once_sem, sum_send, sum_recv, move_send, move_recv, small_send, small_recv,
    dp_send, dp_recv, row_send, row_recv, tot_send, tot_recv, late_send, late_recv, out_sem,
):
    count, rows, local, row_count = sizes
    dp, row, place = lax.axis_index("dp"), lax.axis_index("row"), lax.axis_index("col")
    core_at = {"col": place + 1 - 2 * (place % 2)}
    y_at = {"col": (place + 2) % 4}
    dp_at = {"dp": 1 - dp}
    rounds = [dp_at]
    distance = 1
    while distance < row_count:
        rounds.append({"row": crossed(row, distance)})
        distance *= 2
    greet([core_at, y_at] + rounds)
    width = 4 * local
    block = width // row_count
    two = 2 * HEAD_DIM
    scale = HEAD_DIM**-0.5

    early = ((source_ref, source), (total_ref, total), (cot_ref, cot), (grad_ref, grad_in))
    late = ((mixed_ref, mixed), (probs_ref, probs), (att_ref, att), (low_ref, low))

    def early_load(k, i):
        here, there = early[k]
        return pltpu.make_async_copy(here.at[i], there.at[i % 2] if k == 0 else there, early_sem.at[k])

    def late_load(k, i):
        here, there = late[k]
        return pltpu.make_async_copy(here.at[i], there, late_sem.at[k])

    once = (
        (outw_ref, outw), (qkv_ref, qkv), (fc2_half_ref, half_fc2),
        (fc1_grad_ref.at[:, half_of(dp, fc1_grad_ref.shape[1])], half_fc1), (kept_ref, kept), (late_ref, late_pair),
    )

    def once_load(k):
        return pltpu.make_async_copy(once[k][0], once[k][1], once_sem.at[k])

    grads = (fc2_grad_ref, fc1_grad_ref, outw_grad, qkv_grad)
    halves = (half_fc2, half_fc1, half_outw, half_qkv)
    dp_ins = (dp_fc2, dp_fc1, dp_outw, dp_qkv)
    row_ins = (row_fc2, row_fc1, row_outw, row_qkv)
    tots = (tot_fc2, tot_fc1, tot_outw, tot_qkv)

    codes = sorted(range(1, row_count), key=lambda code: (code & -code, -code)) + [0]

    def rows_at(code):
        return row_place(crossed(row, code), row_count, place, block)

    def dp_copy(w, code):
        full = grads[w]
        return copy_to(
            part_at(full, rows_at(code), other_half_of(dp, full.shape[-1])),
            part_at(dp_ins[w], rows_at(code), slice(None)),
            dp_send.at[w, code],
            dp_recv.at[w, code],
            dp_at,
        )

    def row_copy(w, code):
        return copy_to(
            part_at(halves[w], rows_at(code), slice(None)),
            row_ins[w].at[code],
            row_send.at[w, code],
            row_recv.at[w, code],
            {"row": crossed(row, code & -code)},
        )

    def tot_copy(w):
        part = part_at(tots[w], slice(None), half_of(dp, tots[w].shape[-1]))
        return copy_to(part, part, tot_send.at[w], tot_recv.at[w], dp_at)

    def add_to(w, code, term):
        at = (slice(None), rows_at(code), slice(None)) if len(halves[w].shape) == 3 else (rows_at(code), slice(None))
        halves[w][at] = (halves[w][at].astype(F32) + term.astype(F32)).astype(BF16)

    def dp_sum(w, code):
        dp_copy(w, code).wait_recv()
        at = (slice(None), rows_at(code), slice(None)) if len(halves[w].shape) == 3 else (rows_at(code), slice(None))
        add_to(w, code, dp_ins[w][at])

    def row_take(w, code):
        row_copy(w, code).wait_recv()
        add_to(w, code - (code & -code), row_ins[w][code])

    def row_first(w):
        for code in codes[:-1]:
            if code % 2:
                row_copy(w, code).start()

    def row_next(w):
        for code in codes[:-1]:
            if code % 2 == 0:
                far = 1
                while far < code & -code:
                    row_take(w, code + far)
                    far *= 2
                row_copy(w, code).start()

    def row_last(w):
        far = 1
        while far < row_count:
            row_take(w, far)
            far *= 2
        own = halves[w][:, rows_at(0), :] if len(halves[w].shape) == 3 else halves[w][rows_at(0), :]
        cols = half_of(dp, tots[w].shape[-1])
        if len(halves[w].shape) == 3:
            tots[w][:, :, cols] = own
        else:
            tots[w][:, cols] = own
        tot_copy(w).start()

    def given_copy(i):
        return copy_to(theirs.at[i], given.at[i], sum_send.at[0, i], sum_recv.at[0, i], core_at)

    def stat_copy(i):
        return copy_to(stat.at[i], stat_given.at[i], sum_send.at[1, i], sum_recv.at[1, i], core_at)

    def got_copy(i):
        return copy_to(send.at[i], got.at[i], sum_send.at[2, i], sum_recv.at[2, i], y_at)

    def stat_pair_copy(i):
        return copy_to(stat_pair.at[i], stat_in.at[i], sum_send.at[3, i], sum_recv.at[3, i], y_at)

    late_y = copy_to(late_ref, late_in, late_send.at[0], late_recv.at[0], y_at)
    late_core = copy_to(
        late_grad.at[:, pl.ds(0, 2 * local)], late_grad.at[:, pl.ds(2 * local, 2 * local)], late_send.at[1], late_recv.at[1], core_at
    )

    def move_copy(i):
        return copy_to(move_ref.at[i], move_in.at[i], move_send.at[i], move_recv.at[i], y_at)

    def small_copy(s):
        return copy_to(small.at[s], small_in.at[s], small_send.at[s], small_recv.at[s], rounds[s])

    late_y.start()
    for k in range(4):
        early_load(k, 0).start()
    once_load(2).start()
    once_load(0).start()
    for k in range(4):
        late_load(k, 0).start()
    for k in (1, 3, 5, 4):
        once_load(k).start()
    for i in range(count):
        move_copy(i).start()
    for code in codes:
        if code % 2 == 0:
            dp_copy(0, code).start()
    for code in codes:
        dp_copy(1, code).start()

    small[0] = jnp.zeros_like(small[0])
    small[0, 7:8, :] = mlp_bias_ref[1:2, :local]
    for part in range(mlp_bias_ref.shape[1] // local):
        small[0, 8 + part : 9 + part, :] = mlp_bias_ref[0:1, part * local : (part + 1) * local]
    qkv_sum[...] = jnp.zeros_like(qkv_sum)
    outw_sum[...] = jnp.zeros_like(outw_sum)
    once_load(2).wait()
    row_first(0)

    def product_of(span):
        terms = [
            lax.dot_general(mixed_grad[:, c * local : (c + 1) * local], qkv[c, span, :], NT, preferred_element_type=F32)
            for c in range(3)
        ]
        return terms[0] + terms[1] + terms[2]

    lane = lax.broadcasted_iota(jnp.int32, (1, two), 1)
    down = lax.broadcasted_iota(jnp.int32, (two, two), 0)
    across = lax.broadcasted_iota(jnp.int32, (two, two), 1)
    eye = (down == across).astype(BF16)

    @pl.loop(0, count)
    def _(i):
        for k in range(3):
            early_load(k, i).wait()

        @pl.when(i < count - 1)
        def _():
            early_load(3, i).wait()

        @pl.when(i == count - 1)
        def _():
            late_core.wait_recv()
            grad_in[...] = late_grad[...]

        values = source[i % 2].astype(F32) + total[...].astype(F32) + vectors_ref[4:5, :]
        middle = jnp.sum(values, axis=1, keepdims=True) / width
        square = jnp.sum(values * values, axis=1, keepdims=True) / width
        inverse = lax.rsqrt(square - middle * middle + NORM_EPS)
        normed = (values - middle) * inverse
        grad = grad_in[...].astype(F32)
        small[0, 5:6, :] += jnp.sum(grad[:, :local] * normed[:, :local], axis=0, keepdims=True)
        small[0, 6:7, :] += jnp.sum(grad[:, :local], axis=0, keepdims=True)
        scaled = grad * vectors_ref[2:3, :]
        first = jnp.sum(scaled, axis=1, keepdims=True) / width
        second = jnp.sum(scaled * normed, axis=1, keepdims=True) / width
        whole_grad = cot[...].astype(F32) + inverse * (scaled - first - normed * second)
        grad_hidden[i] = whole_grad[:, :local]
        small[0, 2:3, :] += jnp.sum(whole_grad[:, :local], axis=0, keepdims=True)
        hidden_low[...] = whole_grad.astype(BF16)

        @pl.when(i + 1 < count)
        def _():
            for k in range(3):
                early_load(k, i + 1).start()

        @pl.when(i + 2 < count)
        def _():
            early_load(3, i + 1).start()

        for k in range(4):
            late_load(k, i).wait()

        @pl.when(i == 0)
        def _():
            once_load(0).wait()
            once_load(1).wait()

        grad_att = jnp.dot(hidden_low[...], outw[...], preferred_element_type=F32).astype(BF16)
        for part in range(4):
            span = slice(part * local, (part + 1) * local)
            outw_sum[span, :] += lax.dot_general(hidden_low[:, span], att[...], TN, preferred_element_type=F32)
        for pair in range(local // two):
            base = pair * two
            cols = slice(pair * two, (pair + 1) * two)
            queries = mixed[:, cols]
            key_rows = mixed[:, local + base : local + base + two]
            value_rows = mixed[:, 2 * local + base : 2 * local + base + two]
            pair_grad = grad_att[:, cols]
            q_turned = lax.dot_general(eye, queries, NT, preferred_element_type=F32).astype(BF16)
            grad_turned = lax.dot_general(eye, pair_grad, NT, preferred_element_type=F32).astype(BF16)
            product = pair_grad.astype(F32) * att[:, cols].astype(F32)
            parts = []
            for side in range(2):
                mask = (lane // HEAD_DIM) == side
                turn = slice(side * HEAD_DIM, (side + 1) * HEAD_DIM)
                head_grad = jnp.where(mask, pair_grad, jnp.zeros_like(pair_grad))
                grad_probs = lax.dot_general(head_grad, value_rows, NT, preferred_element_type=F32)
                delta = jnp.sum(jnp.where(mask, product, 0.0), axis=1, keepdims=True)
                probs_low = probs[2 * pair + side]
                grad_scores = (probs_low.astype(F32) * (grad_probs - delta)).astype(BF16)
                parts.append(jnp.dot(grad_scores, key_rows, preferred_element_type=F32))
                k_turned[turn, :] = jnp.dot(q_turned[turn, :], grad_scores, preferred_element_type=F32)
                v_turned[turn, :] = jnp.dot(grad_turned[turn, :], probs_low, preferred_element_type=F32)
            q_grad = jnp.where((lane // HEAD_DIM) == 0, parts[0], parts[1]) * scale
            v_grad = v_turned[...].T
            mixed_grad[:, cols] = q_grad.astype(BF16)
            mixed_grad[:, local + base : local + base + two] = (k_turned[...].T * scale).astype(BF16)
            mixed_grad[:, 2 * local + base : 2 * local + base + two] = v_grad.astype(BF16)
            small[0, 0:1, cols] += jnp.sum(q_grad, axis=0, keepdims=True)
            small[0, 1:2, cols] += jnp.sum(v_grad, axis=0, keepdims=True)
        @pl.when(i + 1 < count)
        def _():
            for k in range(3):
                late_load(k, i + 1).start()

        values = source[i % 2].astype(F32)
        middle = jnp.sum(values, axis=1, keepdims=True) / width
        square = jnp.sum(values * values, axis=1, keepdims=True) / width
        inverse = lax.rsqrt(square - middle * middle + NORM_EPS)
        normed = (values - middle) * inverse
        normed1[i] = normed[:, :local]
        inverse1[i] = inverse
        scaled_in = normed * vectors_ref[0:1, :]
        far = product_of(slice(2 * local, 4 * local))
        theirs[i] = far.astype(BF16)
        given_copy(i).start()
        near = product_of(slice(0, 2 * local))
        mine[...] = near
        first = jnp.sum(far * vectors_ref[0:1, 2 * local :], axis=1, keepdims=True) + jnp.sum(
            near * vectors_ref[0:1, : 2 * local], axis=1, keepdims=True
        )
        second = jnp.sum(far * scaled_in[:, 2 * local :], axis=1, keepdims=True) + jnp.sum(
            near * scaled_in[:, : 2 * local], axis=1, keepdims=True
        )
        spread = jnp.where(lane == 0, first, jnp.where(lane == 1, second, 0.0))
        stat[i] = spread.T[:8, :]
        stat_copy(i).start()
        for part in range(4):
            span = slice(part * local, (part + 1) * local)
            term = lax.dot_general(low[:, span], mixed_grad[...], TN, preferred_element_type=F32)
            for c in range(3):
                qkv_sum[c, span, :] += term[:, c * local : (c + 1) * local]

        @pl.when(i + 1 < count)
        def _():
            late_load(3, i + 1).start()

        given_copy(i).wait_recv()
        kept_grad[i] = mine[:, :local] + given[i, :, :local].astype(F32)
        send[i] = (mine[:, local:] + given[i, :, local:].astype(F32)).astype(BF16)
        got_copy(i).start()
        stat_copy(i).wait_recv()
        stat_pair[i] = stat[i] + stat_given[i]
        stat_pair_copy(i).start()

        @pl.when(i == 0)
        def _():
            for code in codes:
                if code % 2 == 0:
                    dp_sum(0, code)
            row_next(0)
            once_load(3).wait()

        @pl.when(i == 1)
        def _():
            for code in codes:
                if code % 2:
                    dp_sum(1, code)
                    row_copy(1, code).start()

        @pl.when(i == count - 2)
        def _():
            once_load(5).wait()
            late_y.wait_recv()
            late_grad[:, :local] = (late_pair[:, :local].astype(F32) + late_in[:, local:].astype(F32)).astype(BF16)
            late_grad[:, local : 2 * local] = (late_pair[:, local:].astype(F32) + late_in[:, :local].astype(F32)).astype(BF16)
            late_core.start()

    outw_grad[...] = outw_sum[...].astype(BF16)
    half_outw[...] = outw_grad[:, half_of(dp, local)]
    for code in codes:
        dp_copy(2, code).start()
    qkv_grad[...] = qkv_sum[...].astype(BF16)
    half_qkv[...] = qkv_grad[:, :, half_of(dp, local)]
    for code in codes:
        dp_copy(3, code).start()
    for code in codes:
        if code % 2 == 0:
            dp_sum(1, code)
    row_next(1)
    row_last(0)
    once_load(4).wait()

    @pl.loop(0, count)
    def _(i):
        move_copy(i).wait_recv()
        finished[i] = (kept[i] + move_in[i].astype(F32)).astype(BF16)

    for w in (2, 3):
        for code in codes:
            if code % 2:
                dp_sum(w, code)
                row_copy(w, code).start()
    row_last(1)

    for w in (2, 3):
        for code in codes:
            if code % 2 == 0:
                dp_sum(w, code)
        row_next(w)

    @pl.loop(0, count)
    def _(i):
        got_copy(i).wait_recv()
        stat_pair_copy(i).wait_recv()
        sums = stat_pair[i] + stat_in[i]
        spread = jnp.concatenate([sums, jnp.zeros((two - 8, rows), F32)], axis=0).T / width
        grad = kept_grad[i] + got[i].astype(F32)
        small[0, 3:4, :] += jnp.sum(grad * normed1[i], axis=0, keepdims=True)
        small[0, 4:5, :] += jnp.sum(grad, axis=0, keepdims=True)
        scaled = grad * vectors_ref[0:1, :local]
        grad_hidden[i] += inverse1[i] * (scaled - spread[:, 0:1] - normed1[i] * spread[:, 1:2])

    pltpu.make_async_copy(finished, images_out, out_sem.at[0]).start()
    pltpu.make_async_copy(grad_hidden, images_grad_out, out_sem.at[1]).start()
    small_copy(0).start()
    row_last(2)
    row_last(3)
    for s in range(len(rounds)):
        small_copy(s).wait_recv()
        small[s + 1] = small[s] + small_in[s]
        if s + 1 < len(rounds):
            small_copy(s + 1).start()
    outs = ((tot_fc2, fc2_out), (tot_fc1, fc1_out), (tot_outw, outw_out), (tot_qkv, qkv_out))
    for w, (here, there) in enumerate(outs):
        tot_copy(w).wait_recv()
        pltpu.make_async_copy(here, there, out_sem.at[2 + w]).start()
    small_out[...] = small[len(rounds)]
    for i in range(count):
        given_copy(i).wait_send()
        stat_copy(i).wait_send()
        got_copy(i).wait_send()
        stat_pair_copy(i).wait_send()
        move_copy(i).wait_send()
    late_y.wait_send()
    late_core.wait_send()
    for s in range(len(rounds)):
        small_copy(s).wait_send()
    for w in range(4):
        tot_copy(w).wait_send()
        for code in codes:
            if w or code % 2 == 0:
                dp_copy(w, code).wait_send()
            if code:
                row_copy(w, code).wait_send()
    for k, (here, there) in enumerate(((finished, images_out), (grad_hidden, images_grad_out), *outs)):
        pltpu.make_async_copy(here, there, out_sem.at[k]).wait()


def back(
    source, total, cot, grad_low, mixed, probs, att, low, move, kept, qkv, outw, fc1_grad, fc2_half, fc2_grad, late, vectors, mlp_bias
):
    count, rows, width = source.shape
    local = width // 4
    row_count = lax.axis_size("row")
    block = width // row_count
    hidden = fc1_grad.shape[1]
    qkv_width = 3 * local
    heads = local // HEAD_DIM
    rounds = row_count.bit_length()
    outs = [
        ((count, rows, local), BF16), ((count, rows, local), F32), ((16, local), F32),
        ((3, block, local), BF16), ((block, local), BF16), ((block, hidden), BF16), ((block, hidden), BF16),
    ]
    own_f32 = ((count, rows, local), F32)
    own_low = ((count, rows, local), BF16)
    pair_low = ((count, rows, 2 * local), BF16)
    stat = ((count, 8, rows), F32)
    wide = ((rows, width), BF16)
    turned = ((2 * HEAD_DIM, rows), F32)
    columns = (((), hidden), ((), hidden), ((), local), ((3,), local))
    scratch = [
        ((2, rows, width), BF16), wide, wide, wide, ((rows, qkv_width), BF16), ((heads, rows, rows), BF16), ((rows, local), BF16), wide,
        wide, ((rows, qkv_width), BF16), own_f32, own_f32, ((count, rows, 1), F32),
        ((3, width, local), F32), ((width, local), F32), turned, turned,
        pair_low, pair_low, ((rows, 2 * local), F32), own_f32, own_low, own_low, stat, stat, stat, stat,
        ((rows, 2 * local), BF16), ((rows, 2 * local), BF16), wide, own_low, own_f32, own_low, ((3, width, local), BF16), ((width, local), BF16),
        ((3, width, local), BF16), ((width, local), BF16), ((rounds + 1, 16, local), F32), ((rounds, 16, local), F32),
        *[((*lead, width, c // 2), BF16) for lead, c in columns],
        *[((*lead, width, c // 2), BF16) for lead, c in columns],
        *[((row_count, *lead, block, c // 2), BF16) for lead, c in columns],
        *[((*lead, block, c), BF16) for lead, c in columns],
    ]
    dma = pltpu.SemaphoreType.DMA
    whole = pl.BlockSpec(memory_space=pl.ANY)
    vmem = pl.BlockSpec(memory_space=pltpu.VMEM)
    return pl.pallas_call(
        functools.partial(back_kernel, (count, rows, local, row_count)),
        out_shape=[jax.ShapeDtypeStruct(*s) for s in outs],
        in_specs=[whole] * 16 + [vmem] * 2,
        out_specs=[whole, whole, vmem] + [whole] * 4,
        scratch_shapes=[pltpu.VMEM(*s) for s in scratch]
        + [dma((4,)), dma((4,)), dma((6,)), dma((4, count)), dma((4, count)), dma((count,)), dma((count,)), dma((rounds,)), dma((rounds,))]
        + [dma((4, row_count))] * 4
        + [dma((4,)), dma((4,)), dma((2,)), dma((2,)), dma((6,))],
        name="back",
        compiler_params=pltpu.CompilerParams(
            vmem_limit_bytes=63 * 2**20, collective_id=2, has_side_effects=True
        ),
    )(source, total, cot, grad_low, mixed, probs, att, low, move, kept, qkv, outw, fc1_grad, fc2_half, fc2_grad, late, vectors, mlp_bias)


def adam_step(weight, grad, momentum, variance):
    moment_new = BETA_FIRST * momentum + (1.0 - BETA_FIRST) * grad
    second_new = BETA_SECOND * variance + (1.0 - BETA_SECOND) * grad * grad
    corrected = moment_new / (1.0 - BETA_FIRST**STEP)
    second_corrected = second_new / (1.0 - BETA_SECOND**STEP)
    master = weight.astype(jnp.float32)
    updated = master - LEARN_RATE * (
        corrected / (jnp.sqrt(second_corrected) + ADAM_EPS) + WEIGHT_DECAY * master
    )
    return (updated, moment_new, second_new)


def update_kernel(seq, *refs):
    images_in, grad_in, small = refs[:3]
    blocks = refs[3:19]
    images_out, grad_out = refs[19:21]
    grads = refs[21:25]
    sums = refs[25:33]
    fresh = refs[33:45]
    images_out[...] = images_in[:, :seq, :]
    grad_out[...] = grad_in[:, :seq, :]
    sums[0][...] = small[0:2, :]
    local = small.shape[1]
    for k, line in enumerate((2, None, 7, 3, 4, 5, 6)):
        if line is None:
            for part in range(4):
                sums[k + 1][:, part * local : (part + 1) * local] = small[8 + part : 9 + part, :]
        else:
            sums[k + 1][...] = small[line : line + 1, :]
    for w in range(4):
        weight, total, momentum, variance = (blocks[4 * w + k] for k in range(4))
        grad = total[...].astype(F32)
        grads[w][...] = grad
        updated, moment_new, second_new = adam_step(weight[...], grad, momentum[...], variance[...])
        fresh[w][...] = updated
        fresh[4 + w][...] = moment_new
        fresh[8 + w][...] = second_new


def update(images, images_grad, small, blocks, seq):
    count, rows, local = images.shape
    steps = 4

    def image_spec(lines):
        return pl.BlockSpec((1, lines, local), lambda i: (jnp.minimum(i, count - 1), 0, 0))

    def rows_spec(shape):
        if len(shape) == 3:
            return pl.BlockSpec((shape[0], shape[1] // steps, shape[2]), lambda i: (0, i, 0))
        return pl.BlockSpec((shape[0] // steps, shape[1]), lambda i: (i, 0))

    def whole_spec(shape):
        return pl.BlockSpec(shape, lambda i: (0, 0))

    flat = [array for group in blocks for array in group]
    shapes = [group[0].shape for group in blocks]
    hidden = shapes[2][1]
    sum_shapes = [(2, local), (1, local), (1, hidden), *[(1, local)] * 5]
    outs = [((count, seq, local), BF16), ((count, seq, local), F32)]
    outs += [(shape, F32) for shape in (*shapes, *sum_shapes, *shapes, *shapes, *shapes)]
    out_specs = [image_spec(seq), image_spec(seq), *[rows_spec(s) for s in shapes], *[whole_spec(s) for s in sum_shapes]]
    out_specs += [rows_spec(s) for s in shapes] * 3
    return pl.pallas_call(
        functools.partial(update_kernel, seq),
        grid=(steps,),
        out_shape=[jax.ShapeDtypeStruct(*s) for s in outs],
        in_specs=[image_spec(rows), image_spec(rows), whole_spec(small.shape), *[rows_spec(a.shape) for a in flat]],
        out_specs=out_specs,
        name="update",
        compiler_params=pltpu.CompilerParams(vmem_limit_bytes=63 * 2**20),
    )(images, images_grad, small, *flat)


def per_device(
    images_in,
    cotangent,
    first_gain,
    first_shift,
    second_gain,
    second_shift,
    qkv_weight,
    qv_bias,
    out_weight,
    out_bias,
    fc1_weight,
    fc1_bias,
    fc2_weight,
    fc2_bias,
    qkv_momentum,
    qkv_variance,
    out_momentum,
    out_variance,
    fc1_momentum,
    fc1_variance,
    fc2_momentum,
    fc2_variance,
):
    image_count, seq, local = images_in.shape
    width = 4 * local
    rows = -(-seq // ROW_TILE) * ROW_TILE
    place = lax.axis_index("col")

    vectors = [v[None] for v in (first_gain, first_shift, second_gain, second_shift, out_bias)]
    (
        source_all, cot_all, low_all, mixed_all, probs_all, att_all, total_all, grad_low2, qkv_full, out_full, vectors,
        move, kept, fc1_grad, fc2_half, fc2_grad, late, mlp_bias,
    ) = ahead(
        jnp.pad(images_in, ((0, 0), (0, rows - seq), (0, 0))),
        jnp.pad(cotangent, ((0, 0), (0, rows - seq), (0, 0))),
        qkv_weight.transpose(1, 0, 2),
        out_weight,
        fc1_weight,
        fc2_weight,
        vectors,
        qv_bias,
        fc1_bias[None],
        fc2_bias[None],
        seq,
    )
    images_out, images_grad, small, qkv_total, out_total, fc1_total, fc2_total = back(
        source_all, total_all, cot_all, grad_low2, mixed_all, probs_all, att_all, low_all, move, kept,
        qkv_full, out_full, fc1_grad, fc2_half, fc2_grad, late, vectors, mlp_bias,
    )
    def turned(value):
        return value.transpose(1, 0, 2)

    results = update(
        images_out,
        images_grad,
        small,
        (
            (turned(qkv_weight), qkv_total, turned(qkv_momentum), turned(qkv_variance)),
            (out_weight, out_total, out_momentum, out_variance),
            (fc1_weight, fc1_total, fc1_momentum, fc1_variance),
            (fc2_weight, fc2_total, fc2_momentum, fc2_variance),
        ),
        seq,
    )
    results = [turned(r) if k in (2, 14, 18, 22) else r for k, r in enumerate(results)]
    return tuple(r.reshape(-1) if 7 <= k < 14 else r for k, r in enumerate(results))


def solution(mesh):
    return jax.shard_map(
        per_device,
        mesh=mesh,
        in_specs=(
            P(("dp", "row"), None, "col"),
            P(("dp", "row"), None, "col"),
            P("col"),
            P("col"),
            P("col"),
            P("col"),
            P("row", None, "col"),
            P(None, "col"),
            P("row", "col"),
            P("col"),
            P("row", "col"),
            P("col"),
            P("row", "col"),
            P("col"),
            P("row", None, "col"),
            P("row", None, "col"),
            P("row", "col"),
            P("row", "col"),
            P("row", "col"),
            P("row", "col"),
            P("row", "col"),
            P("row", "col"),
        ),
        out_specs=(
            P(("dp", "row"), None, "col"),
            P(("dp", "row"), None, "col"),
            P("row", None, "col"),
            P("row", "col"),
            P("row", "col"),
            P("row", "col"),
            P(None, "col"),
            P("col"),
            P("col"),
            P("col"),
            P("col"),
            P("col"),
            P("col"),
            P("col"),
            P("row", None, "col"),
            P("row", "col"),
            P("row", "col"),
            P("row", "col"),
            P("row", None, "col"),
            P("row", "col"),
            P("row", "col"),
            P("row", "col"),
            P("row", None, "col"),
            P("row", "col"),
            P("row", "col"),
            P("row", "col"),
        ),
        check_vma=False,
    )
```

```python
import functools

import jax
import jax.numpy as jnp
from jax import lax
from jax.experimental import pallas as pl
from jax.experimental.pallas import tpu as pltpu
from jax.sharding import PartitionSpec as P

HEAD_DIM = 64
STEP = 3


NORM_EPS = 1e-06
LEARN_RATE = 0.02
BETA_FIRST = 0.9
BETA_SECOND = 0.999
ADAM_EPS = 1e-08
WEIGHT_DECAY = 0.05
ROOT_HALF = 0.7071067811865476
ROOT_TWO_PI = 2.5066282746310002
LOG2E = 1.4426950408889634
ROW_TILE = 16
MESH = pl.DeviceIdType.MESH
NT = (((1,), (1,)), ((), ()))
TN = (((0,), (0,)), ((), ()))
F32 = jnp.float32
BF16 = jnp.bfloat16


def copy_to(src, dst, send, recv, where):
    return pltpu.make_async_remote_copy(
        src_ref=src, dst_ref=dst, send_sem=send, recv_sem=recv, device_id=where, device_id_type=MESH
    )


def rel_place(quarter, place):
    return (quarter // 2 + place // 2) % 2 + 2 * ((quarter % 2 + place % 2) % 2)


def crossed(row, code):
    distance = 1
    while distance <= code:
        if code & distance:
            row = row + distance * (1 - 2 * ((row // distance) % 2))
        distance *= 2
    return row


def half_of(dp, full_width):
    half = full_width // 2
    return pl.ds(pl.multiple_of(dp * half, half), half)


def other_half_of(dp, full_width):
    half = full_width // 2
    return pl.ds(pl.multiple_of((1 - dp) * half, half), half)


def row_place(owner, row_count, place, block):
    per = row_count // 4
    at = (rel_place(owner // per, place) * per + owner % per) * block
    return pl.ds(pl.multiple_of(at, block), block)


def part_at(full, rows, cols):
    return full.at[:, rows, cols] if len(full.shape) == 3 else full.at[rows, cols]


def greet(partners):
    barrier = pltpu.get_barrier_semaphore()
    for partner in partners:
        pl.semaphore_signal(barrier, inc=1, device_id=partner, device_id_type=MESH)
    pl.semaphore_wait(barrier, len(partners))


def ahead_kernel(
    sizes,
    images_ref, cot_ref, qkv_ref, out_ref, fc1_ref, fc2_ref,
    gain1_ref, shift1_ref, gain2_ref, shift2_ref, out_bias_ref, qv_bias_ref, fc1_bias_ref, fc2_bias_ref,
    source_out, cot_out, low_out, mixed_out, probs_out, att_out, total_out, grad_out, qkv_out, outw_out, vectors_out,
    move_out, kept_out, fc1_grad_out, fc2_half_out, fc2_grad_out, late_out, bias_out,
    source, cot, low, mixed, probs, att, theirs, given, mine, pair, pair_in, total, qkv_full, out_full, fc1_full, fc2_full, vectors, vectors_ref,
    active, gelu_grad, grad_in, move_given, kept, move, fc1_grad, fc2_grad, dp_in, fc2_half,
    row_send, row_recv, dp_send, dp_recv, own_sem, in_send, in_recv, vec_send, vec_recv, sum_send, sum_recv, image_sem, out_sem,
    back_send, back_recv, half_send, half_recv,
):
    count, seq, rows, local, row_count = sizes
    dp, row, place = lax.axis_index("dp"), lax.axis_index("row"), lax.axis_index("col")
    core_at = {"col": place + 1 - 2 * (place % 2)}
    y_at = {"col": (place + 2) % 4}
    dp_at = {"dp": 1 - dp}
    codes = sorted(range(1, row_count), key=lambda code: -(code & -code))
    fars = [code for code in codes if code & -code == code]
    greet([core_at, y_at, dp_at] + [{"row": crossed(row, far)} for far in fars])
    block = out_ref.shape[0]
    width = 4 * local
    weights = ((qkv_ref, qkv_full), (out_ref, out_full), (fc1_ref, fc1_full), (fc2_ref, fc2_full))

    def row_copy(w, code):
        ref, full = weights[w]
        cols = half_of(dp, full.shape[-1])
        far = code & -code
        held = part_at(full, row_place(crossed(row, code - far), row_count, place, block), cols)
        return copy_to(
            part_at(ref, slice(None), cols) if code == far else held, held, row_send.at[w, code], row_recv.at[w, code], {"row": crossed(row, far)}
        )

    def dp_copy(w, code):
        _, full = weights[w]
        part = part_at(full, row_place(crossed(row, code), row_count, place, block), half_of(dp, full.shape[-1]))
        return copy_to(part, part, dp_send.at[w, code], dp_recv.at[w, code], dp_at)

    def own_copy(w):
        ref, full = weights[w]
        return pltpu.make_async_copy(ref, part_at(full, row_place(row, row_count, place, block), slice(None)), own_sem.at[w])

    inputs = ((images_ref, source), (cot_ref, cot))

    def y_copy(a, i):
        ref, full = inputs[a]
        return copy_to(ref.at[i], full.at[i, :, pl.ds(local, local)], in_send.at[a, 0, i], in_recv.at[a, 0, i], y_at)

    def core_copy(a, i):
        ref, full = inputs[a]
        return copy_to(ref.at[i], full.at[i, :, pl.ds(2 * local, local)], in_send.at[a, 1, i], in_recv.at[a, 1, i], core_at)

    def hand_copy(a, i):
        _, full = inputs[a]
        return copy_to(
            full.at[i, :, pl.ds(local, local)],
            full.at[i, :, pl.ds(3 * local, local)],
            in_send.at[a, 2, i],
            in_recv.at[a, 2, i],
            core_at,
        )

    def here_copy(a, i):
        ref, full = inputs[a]
        return pltpu.make_async_copy(ref.at[i], full.at[i, :, pl.ds(0, local)], in_send.at[a, 3, i])

    def vector_copy(k):
        src = vectors.at[:, pl.ds(local, local)] if k == 2 else vectors_ref
        at = (local, 2 * local, 3 * local)[k]
        return copy_to(
            src, vectors.at[:, pl.ds(at, local)], vec_send.at[k], vec_recv.at[k], (y_at, core_at, core_at)[k]
        )

    for k, vector in enumerate((gain1_ref, shift1_ref, gain2_ref, shift2_ref, out_bias_ref)):
        vectors_ref[k : k + 1, :] = vector[...]
    vectors_ref[5:8, :] = jnp.zeros((3, local), F32)
    vector_here = pltpu.make_async_copy(vectors_ref, vectors.at[:, pl.ds(0, local)], vec_send.at[3])

    def given_copy(i):
        return copy_to(theirs, given.at[i], sum_send.at[0, i], sum_recv.at[0, i], core_at)

    def given_back(i):
        return copy_to(theirs, given.at[i], back_send.at[0, i], back_recv.at[0, i], core_at)

    def pair_back(i):
        return copy_to(pair.at[i], grad_in.at[i], back_send.at[1, i], back_recv.at[1, i], y_at)

    def total_back(i):
        return copy_to(
            total.at[i, :, pl.ds(0, 2 * local)],
            total.at[i, :, pl.ds(2 * local, 2 * local)],
            back_send.at[2, i],
            back_recv.at[2, i],
            core_at,
        )

    def move_copy(i):
        return copy_to(theirs, move_given.at[i], back_send.at[3, i], back_recv.at[3, i], core_at)

    hidden_width = fc1_full.shape[1]

    odd_codes = sorted(range(1, row_count, 2), reverse=True)

    def half_copy(code):
        there = row_place(crossed(row, code), row_count, place, block)
        return copy_to(
            fc2_grad.at[there, other_half_of(dp, hidden_width)], dp_in.at[there, :], half_send.at[code], half_recv.at[code], dp_at
        )

    def pair_copy(i):
        return copy_to(pair.at[i], pair_in.at[i], sum_send.at[1, i], sum_recv.at[1, i], y_at)

    def total_copy(i):
        return copy_to(
            total.at[i, :, pl.ds(0, 2 * local)],
            total.at[i, :, pl.ds(2 * local, 2 * local)],
            sum_send.at[2, i],
            sum_recv.at[2, i],
            core_at,
        )

    def start_own(w):
        for far in fars:
            row_copy(w, far).start()

    def relay(w, code):
        row_copy(w, code).wait_recv()
        for far in fars:
            if far < code & -code:
                row_copy(w, code + far).start()
        dp_copy(w, code).start()

    def arrived(w):
        for code in codes:
            dp_copy(w, code).wait_recv()
        own_copy(w).wait()

    kinds = ((source, source_out), (low, low_out), (mixed, mixed_out), (probs, probs_out), (att, att_out), (total, total_out))

    def image_copy(k, i):
        here, there = kinds[k]
        return pltpu.make_async_copy(here if k in (2, 3) else here.at[i], there.at[i], image_sem.at[k, i])

    wanted = [(a, i) for a in range(2) for i in range(count)]
    start_own(0)
    start_own(1)
    vector_copy(0).start()
    for a, i in wanted:
        y_copy(a, i).start()
    vector_copy(1).start()
    vector_here.start()
    for a, i in wanted:
        core_copy(a, i).start()
        here_copy(a, i).start()
    for w in range(4):
        own_copy(w).start()
    vector_copy(0).wait_recv()
    vector_copy(2).start()
    relay(0, codes[0])
    relay(1, codes[0])
    start_own(2)
    vector_here.wait()
    vector_copy(1).wait_recv()
    vector_copy(2).wait_recv()

    @pl.loop(0, count)
    def _(i):
        y_copy(0, i).wait_recv()
        hand_copy(0, i).start()
        here_copy(0, i).wait()
        core_copy(0, i).wait_recv()
        hand_copy(0, i).wait_recv()
        image_copy(0, i).start()
        values = source[i].astype(F32)
        middle = jnp.sum(values, axis=1, keepdims=True) / width
        square = jnp.sum(values * values, axis=1, keepdims=True) / width
        inverse = lax.rsqrt(square - middle * middle + NORM_EPS)
        low[i] = ((values - middle) * inverse * vectors[0:1, :] + vectors[1:2, :]).astype(BF16)
        image_copy(1, i).start()

        @pl.when(i == 0)
        def _():
            for code in codes[1:]:
                relay(0, code)
                relay(1, code)

    relay(2, codes[0])
    start_own(3)
    arrived(0)
    arrived(1)

    lane = lax.broadcasted_iota(jnp.int32, (1, 2 * HEAD_DIM), 1)
    key_at = lax.broadcasted_iota(jnp.int32, (1, rows), 1)
    pairs = local // (2 * HEAD_DIM)

    @pl.loop(0, count)
    def _(i):
        @pl.when(i > 0)
        def _():
            image_copy(2, i - 1).wait()

        for c in range(3):
            cols = slice(c * local, (c + 1) * local)
            rows_out = jnp.dot(low[i], qkv_full[c], preferred_element_type=F32)
            if c != 1:
                rows_out += qv_bias_ref[c // 2 : c // 2 + 1, :]
            mixed[:, cols] = rows_out.astype(BF16)
        image_copy(2, i).start()

        @pl.when(i > 0)
        def _():
            image_copy(3, i - 1).wait()

        for pair_at in range(pairs):
            base = pair_at * 2 * HEAD_DIM
            queries = mixed[:, base : base + 2 * HEAD_DIM]
            key_rows = mixed[:, local + base : local + base + 2 * HEAD_DIM]
            value_rows = mixed[:, 2 * local + base : 2 * local + base + 2 * HEAD_DIM]
            parts = []
            for side in range(2):
                mask = (lane // HEAD_DIM) == side
                head_q = jnp.where(mask, queries, jnp.zeros_like(queries))
                scores = lax.dot_general(head_q, key_rows, NT, preferred_element_type=F32)
                scores = jnp.where(key_at < seq, scores, -1e30)
                peak = jnp.max(scores, axis=1, keepdims=True)
                powers = jnp.exp2((scores - peak) * (HEAD_DIM**-0.5 * LOG2E))
                share = 1.0 / jnp.sum(powers, axis=1, keepdims=True)
                probs_low = (powers * share).astype(BF16)
                probs[2 * pair_at + side] = probs_low
                parts.append(jnp.dot(probs_low, value_rows, preferred_element_type=F32))
            joined = jnp.where((lane // HEAD_DIM) == 0, parts[0], parts[1])
            att[i, :, 2 * HEAD_DIM * pair_at : 2 * HEAD_DIM * (pair_at + 1)] = joined.astype(BF16)
        image_copy(3, i).start()
        image_copy(4, i).start()
        attended = att[i]

        @pl.when(i > 0)
        def _():
            given_copy(i - 1).wait_send()

        theirs[...] = lax.dot_general(attended, out_full[2 * local :, :], NT, preferred_element_type=F32).astype(BF16)
        given_copy(i).start()
        mine[...] = lax.dot_general(attended, out_full[: 2 * local, :], NT, preferred_element_type=F32)
        given_copy(i).wait_recv()
        pair[i] = (mine[...] + given[i].astype(F32)).astype(BF16)
        pair_copy(i).start()

        @pl.when(i == 0)
        def _():
            for code in codes[1:]:
                relay(2, code)

        @pl.when(i == 1)
        def _():
            for code in codes[:2]:
                relay(3, code)

    outs = ((qkv_full, qkv_out), (out_full, outw_out), (vectors, vectors_out), (cot, cot_out), (move, move_out), (kept, kept_out), (fc1_grad, fc1_grad_out), (fc2_half, fc2_half_out), (fc2_grad, fc2_grad_out), (total.at[pl.ds(0, count - 1)], grad_out))

    def out_copy(k):
        return pltpu.make_async_copy(outs[k][0], outs[k][1], out_sem.at[k])

    for k in range(3):
        out_copy(k).start()
    bias_out[...] = jnp.zeros_like(bias_out)
    step = hidden_width // 4
    given_copy(count - 1).wait_send()

    @pl.loop(0, count)
    def _(i):
        y_copy(1, i).wait_recv()
        hand_copy(1, i).start()
        pair_copy(i).wait_recv()
        total[i, :, :local] = (pair[i, :, :local].astype(F32) + pair_in[i, :, local:].astype(F32)).astype(BF16)
        total[i, :, local : 2 * local] = (pair[i, :, local:].astype(F32) + pair_in[i, :, :local].astype(F32)).astype(BF16)
        total_copy(i).start()

        @pl.when(i == 0)
        def _():
            for code in codes[2:]:
                relay(3, code)

        image_copy(1, i).wait()
        pair_copy(i).wait_send()
        here_copy(1, i).wait()
        core_copy(1, i).wait_recv()
        hand_copy(1, i).wait_recv()
        bias_out[1:2, :local] += jnp.sum(cot[i, :, :local].astype(F32), axis=0, keepdims=True)
        total_copy(i).wait_recv()
        image_copy(5, i).start()
        values = source[i].astype(F32) + total[i].astype(F32) + vectors[4:5, :]
        kept[i] = values[:, :local] + fc2_bias_ref[...]
        middle = jnp.sum(values, axis=1, keepdims=True) / width
        square = jnp.sum(values * values, axis=1, keepdims=True) / width
        inverse = lax.rsqrt(square - middle * middle + NORM_EPS)
        low[i] = ((values - middle) * inverse * vectors[2:3, :] + vectors[3:4, :]).astype(BF16)

        @pl.when(i == 0)
        def _():
            arrived(2)
            arrived(3)

        @pl.loop(0, 4)
        def _(part):
            cols = pl.ds(pl.multiple_of(part * step, step), step)
            pre_act = jnp.dot(low[i], fc1_full[:, cols], preferred_element_type=F32) + fc1_bias_ref[:, cols]
            gate = 0.5 * (1.0 + lax.erf(pre_act * ROOT_HALF))
            active[i, :, cols] = (pre_act * gate).astype(BF16)
            slope = gate + pre_act * jnp.exp(-0.5 * pre_act * pre_act) / ROOT_TWO_PI
            grad_pre = jnp.dot(cot[i], fc2_full[:, cols], preferred_element_type=F32) * slope
            bias_out[0:1, cols] += jnp.sum(grad_pre, axis=0, keepdims=True)
            gelu_grad[i, :, cols] = grad_pre.astype(BF16)

        @pl.when(i > 0)
        def _():
            given_back(i - 1).wait_send()

        theirs[...] = lax.dot_general(gelu_grad[i], fc1_full[2 * local :, :], NT, preferred_element_type=F32).astype(BF16)
        image_copy(5, i).wait()
        given_back(i).start()
        mine[...] = lax.dot_general(gelu_grad[i], fc1_full[: 2 * local, :], NT, preferred_element_type=F32)
        given_back(i).wait_recv()
        pair[i] = (mine[...] + given[i].astype(F32)).astype(BF16)

        @pl.when(i < count - 1)
        def _():
            pair_back(i).start()

    out_copy(3).start()
    late_copy = pltpu.make_async_copy(pair.at[count - 1], late_out, out_sem.at[10])
    late_copy.start()

    def weight_grad(out, left, right):
        @pl.loop(0, 4)
        def _(part):
            span = pl.ds(pl.multiple_of(part * local, local), local)
            terms = [lax.dot_general(left[i, :, span], right[i], TN, preferred_element_type=F32) for i in range(count)]
            out[span, :] = sum(terms[1:], terms[0]).astype(BF16)

    weight_grad(fc2_grad, cot, active)
    for code in odd_codes:
        half_copy(code).start()
    out_copy(8).start()
    given_back(count - 1).wait_send()

    @pl.loop(0, count)
    def _(i):
        @pl.when(i > 0)
        def _():
            move_copy(i - 1).wait_send()

        theirs[...] = lax.dot_general(active[i], fc2_full[2 * local :, :], NT, preferred_element_type=F32).astype(BF16)
        move_copy(i).start()
        mine[...] = lax.dot_general(active[i], fc2_full[: 2 * local, :], NT, preferred_element_type=F32)
        move_copy(i).wait_recv()
        kept[i] += mine[:, :local] + move_given[i, :, :local].astype(F32)
        move[i] = (mine[:, local:] + move_given[i, :, local:].astype(F32)).astype(BF16)

    out_copy(4).start()
    out_copy(5).start()
    weight_grad(fc1_grad, low, gelu_grad)
    out_copy(6).start()

    @pl.loop(0, count - 1)
    def _(i):
        pair_back(i).wait_recv()
        total_copy(i).wait_send()
        total[i, :, :local] = (pair[i, :, :local].astype(F32) + grad_in[i, :, local:].astype(F32)).astype(BF16)
        total[i, :, local : 2 * local] = (pair[i, :, local:].astype(F32) + grad_in[i, :, :local].astype(F32)).astype(BF16)
        total_back(i).start()

        @pl.when(i == count - 2)
        def _():
            for code in odd_codes:
                half_copy(code).wait_recv()
                there = row_place(crossed(row, code), row_count, place, block)
                mine_part = fc2_grad[there, half_of(dp, hidden_width)].astype(F32)
                fc2_half[there, :] = (mine_part + dp_in[there, :].astype(F32)).astype(BF16)
            for code in range(0, row_count, 2):
                there = row_place(crossed(row, code), row_count, place, block)
                fc2_half[there, :] = fc2_grad[there, half_of(dp, hidden_width)]
            out_copy(7).start()

    for i in range(count - 1):
        total_back(i).wait_recv()
    out_copy(9).start()
    for w in range(4):
        for code in codes:
            row_copy(w, code).wait_send()
            dp_copy(w, code).wait_send()
    for a, i in wanted:
        y_copy(a, i).wait_send()
        core_copy(a, i).wait_send()
        hand_copy(a, i).wait_send()
    for k in range(3):
        vector_copy(k).wait_send()
    total_copy(count - 1).wait_send()
    late_copy.wait()
    for i in range(count - 1):
        pair_back(i).wait_send()
        total_back(i).wait_send()
    for i in range(count):
        image_copy(0, i).wait()
        image_copy(4, i).wait()
    move_copy(count - 1).wait_send()
    image_copy(2, count - 1).wait()
    image_copy(3, count - 1).wait()
    for code in odd_codes:
        half_copy(code).wait_send()
    for k in range(len(outs)):
        out_copy(k).wait()


def ahead(images, cotangent, qkv_block, out_block, fc1_block, fc2_block, vectors, qv_bias, fc1_bias, fc2_bias, seq):
    count, rows, local = images.shape
    row_count = lax.axis_size("row")
    width = 4 * local
    heads = local // HEAD_DIM
    hidden = fc1_block.shape[1]

    def wide(*shape):
        return shape, BF16

    all_wide = wide(count, rows, width)
    all_pair = wide(count, rows, 2 * local)
    all_own = wide(count, rows, local)
    own_f32 = ((count, rows, local), F32)
    norm_rows = ((8, width), F32)
    outs = [
        all_wide, all_wide, all_wide, wide(count, rows, 3 * local), wide(count, heads, rows, rows), all_own, all_wide,
        wide(count - 1, rows, width), wide(3, width, local), wide(width, local), norm_rows, all_own, own_f32,
        wide(width, hidden), wide(width, hidden // 2), wide(width, hidden), wide(rows, 2 * local),
        ((2, hidden), F32),
    ]
    scratch = [
        all_wide, all_wide, all_wide, wide(rows, 3 * local), wide(heads, rows, rows), all_own,
        wide(rows, 2 * local), all_pair, ((rows, 2 * local), F32), all_pair, all_pair, all_wide,
        wide(3, width, local), wide(width, local), wide(width, hidden), wide(width, hidden), norm_rows, ((8, local), F32),
        wide(count, rows, hidden), wide(count, rows, hidden), all_pair, all_pair, own_f32, all_own,
        wide(width, hidden), wide(width, hidden), wide(width, hidden // 2), wide(width, hidden // 2),
    ]
    dma = pltpu.SemaphoreType.DMA
    whole = pl.BlockSpec(memory_space=pl.ANY)
    vmem = pl.BlockSpec(memory_space=pltpu.VMEM)
    return pl.pallas_call(
        functools.partial(ahead_kernel, (count, seq, rows, local, row_count)),
        out_shape=[jax.ShapeDtypeStruct(*s) for s in outs],
        in_specs=[whole] * 6 + [vmem] * 8,
        out_specs=[whole] * (len(outs) - 1) + [vmem],
        scratch_shapes=[pltpu.VMEM(*s) for s in scratch]
        + [dma((4, row_count))] * 4
        + [dma((4,)), dma((2, 4, count)), dma((2, 3, count)), dma((4,)), dma((3,))]
        + [dma((3, count)), dma((3, count)), dma((6, count)), dma((11,))]
        + [dma((4, count)), dma((4, count)), dma((row_count,)), dma((row_count,))],
        name="ahead",
        compiler_params=pltpu.CompilerParams(
            vmem_limit_bytes=63 * 2**20, collective_id=0, has_side_effects=True
        ),
    )(images, cotangent, qkv_block, out_block, fc1_block, fc2_block, *vectors, qv_bias, fc1_bias, fc2_bias)


def back_kernel(
    sizes,
    source_ref, total_ref, cot_ref, grad_ref, mixed_ref, probs_ref, att_ref, low_ref, move_ref, kept_ref,
    qkv_ref, outw_ref, fc1_grad_ref, fc2_half_ref, fc2_grad_ref, late_ref, vectors_ref, mlp_bias_ref,
    images_out, images_grad_out, small_out, qkv_out, outw_out, fc1_out, fc2_out,
    source, total, cot, grad_in, mixed, probs, att, low,
    hidden_low, mixed_grad, grad_hidden, normed1, inverse1, qkv_sum, outw_sum, k_turned, v_turned,
    theirs, given, mine, kept_grad, send, got, stat, stat_given, stat_pair, stat_in,
    late_pair, late_in, late_grad, move_in, kept, finished, qkv, outw, qkv_grad, outw_grad, small, small_in,
    half_fc2, half_fc1, half_outw, half_qkv, dp_fc2, dp_fc1, dp_outw, dp_qkv,
    row_fc2, row_fc1, row_outw, row_qkv, tot_fc2, tot_fc1, tot_outw, tot_qkv,
    early_sem, late_sem, once_sem, sum_send, sum_recv, move_send, move_recv, small_send, small_recv,
    dp_send, dp_recv, row_send, row_recv, tot_send, tot_recv, late_send, late_recv, out_sem,
):
    count, rows, local, row_count = sizes
    dp, row, place = lax.axis_index("dp"), lax.axis_index("row"), lax.axis_index("col")
    core_at = {"col": place + 1 - 2 * (place % 2)}
    y_at = {"col": (place + 2) % 4}
    dp_at = {"dp": 1 - dp}
    rounds = [dp_at]
    distance = 1
    while distance < row_count:
        rounds.append({"row": crossed(row, distance)})
        distance *= 2
    greet([core_at, y_at] + rounds)
    width = 4 * local
    block = width // row_count
    two = 2 * HEAD_DIM
    scale = HEAD_DIM**-0.5

    early = ((source_ref, source), (total_ref, total), (cot_ref, cot), (grad_ref, grad_in))
    late = ((mixed_ref, mixed), (probs_ref, probs), (att_ref, att), (low_ref, low))

    def early_load(k, i):
        here, there = early[k]
        return pltpu.make_async_copy(here.at[i], there.at[i % 2] if k == 0 else there, early_sem.at[k])

    def late_load(k, i):
        here, there = late[k]
        return pltpu.make_async_copy(here.at[i], there, late_sem.at[k])

    once = (
        (outw_ref, outw), (qkv_ref, qkv), (fc2_half_ref, half_fc2),
        (fc1_grad_ref.at[:, half_of(dp, fc1_grad_ref.shape[1])], half_fc1), (kept_ref, kept), (late_ref, late_pair),
    )

    def once_load(k):
        return pltpu.make_async_copy(once[k][0], once[k][1], once_sem.at[k])

    grads = (fc2_grad_ref, fc1_grad_ref, outw_grad, qkv_grad)
    halves = (half_fc2, half_fc1, half_outw, half_qkv)
    dp_ins = (dp_fc2, dp_fc1, dp_outw, dp_qkv)
    row_ins = (row_fc2, row_fc1, row_outw, row_qkv)
    tots = (tot_fc2, tot_fc1, tot_outw, tot_qkv)

    codes = sorted(range(1, row_count), key=lambda code: (code & -code, -code)) + [0]

    def rows_at(code):
        return row_place(crossed(row, code), row_count, place, block)

    def dp_copy(w, code):
        full = grads[w]
        return copy_to(
            part_at(full, rows_at(code), other_half_of(dp, full.shape[-1])),
            part_at(dp_ins[w], rows_at(code), slice(None)),
            dp_send.at[w, code],
            dp_recv.at[w, code],
            dp_at,
        )

    def row_copy(w, code):
        return copy_to(
            part_at(halves[w], rows_at(code), slice(None)),
            row_ins[w].at[code],
            row_send.at[w, code],
            row_recv.at[w, code],
            {"row": crossed(row, code & -code)},
        )

    def tot_copy(w):
        part = part_at(tots[w], slice(None), half_of(dp, tots[w].shape[-1]))
        return copy_to(part, part, tot_send.at[w], tot_recv.at[w], dp_at)

    def add_to(w, code, term):
        at = (slice(None), rows_at(code), slice(None)) if len(halves[w].shape) == 3 else (rows_at(code), slice(None))
        halves[w][at] = (halves[w][at].astype(F32) + term.astype(F32)).astype(BF16)

    def dp_sum(w, code):
        dp_copy(w, code).wait_recv()
        at = (slice(None), rows_at(code), slice(None)) if len(halves[w].shape) == 3 else (rows_at(code), slice(None))
        add_to(w, code, dp_ins[w][at])

    def row_take(w, code):
        row_copy(w, code).wait_recv()
        add_to(w, code - (code & -code), row_ins[w][code])

    def row_first(w):
        for code in codes[:-1]:
            if code % 2:
                row_copy(w, code).start()

    def row_next(w):
        for code in codes[:-1]:
            if code % 2 == 0:
                far = 1
                while far < code & -code:
                    row_take(w, code + far)
                    far *= 2
                row_copy(w, code).start()

    def row_last(w):
        far = 1
        while far < row_count:
            row_take(w, far)
            far *= 2
        own = halves[w][:, rows_at(0), :] if len(halves[w].shape) == 3 else halves[w][rows_at(0), :]
        cols = half_of(dp, tots[w].shape[-1])
        if len(halves[w].shape) == 3:
            tots[w][:, :, cols] = own
        else:
            tots[w][:, cols] = own
        tot_copy(w).start()

    def given_copy(i):
        return copy_to(theirs.at[i], given.at[i], sum_send.at[0, i], sum_recv.at[0, i], core_at)

    def stat_copy(i):
        return copy_to(stat.at[i], stat_given.at[i], sum_send.at[1, i], sum_recv.at[1, i], core_at)

    def got_copy(i):
        return copy_to(send.at[i], got.at[i], sum_send.at[2, i], sum_recv.at[2, i], y_at)

    def stat_pair_copy(i):
        return copy_to(stat_pair.at[i], stat_in.at[i], sum_send.at[3, i], sum_recv.at[3, i], y_at)

    late_y = copy_to(late_ref, late_in, late_send.at[0], late_recv.at[0], y_at)
    late_core = copy_to(
        late_grad.at[:, pl.ds(0, 2 * local)], late_grad.at[:, pl.ds(2 * local, 2 * local)], late_send.at[1], late_recv.at[1], core_at
    )

    def move_copy(i):
        return copy_to(move_ref.at[i], move_in.at[i], move_send.at[i], move_recv.at[i], y_at)

    def small_copy(s):
        return copy_to(small.at[s], small_in.at[s], small_send.at[s], small_recv.at[s], rounds[s])

    late_y.start()
    for k in range(4):
        early_load(k, 0).start()
    once_load(2).start()
    once_load(0).start()
    for k in range(4):
        late_load(k, 0).start()
    for k in (1, 3, 5, 4):
        once_load(k).start()
    for i in range(count):
        move_copy(i).start()
    for code in codes:
        if code % 2 == 0:
            dp_copy(0, code).start()
    for code in codes:
        dp_copy(1, code).start()

    small[0] = jnp.zeros_like(small[0])
    small[0, 7:8, :] = mlp_bias_ref[1:2, :local]
    for part in range(mlp_bias_ref.shape[1] // local):
        small[0, 8 + part : 9 + part, :] = mlp_bias_ref[0:1, part * local : (part + 1) * local]
    qkv_sum[...] = jnp.zeros_like(qkv_sum)
    outw_sum[...] = jnp.zeros_like(outw_sum)
    once_load(2).wait()
    row_first(0)

    def product_of(span):
        terms = [
            lax.dot_general(mixed_grad[:, c * local : (c + 1) * local], qkv[c, span, :], NT, preferred_element_type=F32)
            for c in range(3)
        ]
        return terms[0] + terms[1] + terms[2]

    lane = lax.broadcasted_iota(jnp.int32, (1, two), 1)
    down = lax.broadcasted_iota(jnp.int32, (two, two), 0)
    across = lax.broadcasted_iota(jnp.int32, (two, two), 1)
    eye = (down == across).astype(BF16)

    @pl.loop(0, count)
    def _(i):
        for k in range(3):
            early_load(k, i).wait()

        @pl.when(i < count - 1)
        def _():
            early_load(3, i).wait()

        @pl.when(i == count - 1)
        def _():
            late_core.wait_recv()
            grad_in[...] = late_grad[...]

        values = source[i % 2].astype(F32) + total[...].astype(F32) + vectors_ref[4:5, :]
        middle = jnp.sum(values, axis=1, keepdims=True) / width
        square = jnp.sum(values * values, axis=1, keepdims=True) / width
        inverse = lax.rsqrt(square - middle * middle + NORM_EPS)
        normed = (values - middle) * inverse
        grad = grad_in[...].astype(F32)
        small[0, 5:6, :] += jnp.sum(grad[:, :local] * normed[:, :local], axis=0, keepdims=True)
        small[0, 6:7, :] += jnp.sum(grad[:, :local], axis=0, keepdims=True)
        scaled = grad * vectors_ref[2:3, :]
        first = jnp.sum(scaled, axis=1, keepdims=True) / width
        second = jnp.sum(scaled * normed, axis=1, keepdims=True) / width
        whole_grad = cot[...].astype(F32) + inverse * (scaled - first - normed * second)
        grad_hidden[i] = whole_grad[:, :local]
        small[0, 2:3, :] += jnp.sum(whole_grad[:, :local], axis=0, keepdims=True)
        hidden_low[...] = whole_grad.astype(BF16)

        @pl.when(i + 1 < count)
        def _():
            for k in range(3):
                early_load(k, i + 1).start()

        @pl.when(i + 2 < count)
        def _():
            early_load(3, i + 1).start()

        for k in range(4):
            late_load(k, i).wait()

        @pl.when(i == 0)
        def _():
            once_load(0).wait()
            once_load(1).wait()

        grad_att = jnp.dot(hidden_low[...], outw[...], preferred_element_type=F32).astype(BF16)
        for part in range(4):
            span = slice(part * local, (part + 1) * local)
            outw_sum[span, :] += lax.dot_general(hidden_low[:, span], att[...], TN, preferred_element_type=F32)
        for pair in range(local // two):
            base = pair * two
            cols = slice(pair * two, (pair + 1) * two)
            queries = mixed[:, cols]
            key_rows = mixed[:, local + base : local + base + two]
            value_rows = mixed[:, 2 * local + base : 2 * local + base + two]
            pair_grad = grad_att[:, cols]
            q_turned = lax.dot_general(eye, queries, NT, preferred_element_type=F32).astype(BF16)
            grad_turned = lax.dot_general(eye, pair_grad, NT, preferred_element_type=F32).astype(BF16)
            product = pair_grad.astype(F32) * att[:, cols].astype(F32)
            parts = []
            for side in range(2):
                mask = (lane // HEAD_DIM) == side
                turn = slice(side * HEAD_DIM, (side + 1) * HEAD_DIM)
                head_grad = jnp.where(mask, pair_grad, jnp.zeros_like(pair_grad))
                grad_probs = lax.dot_general(head_grad, value_rows, NT, preferred_element_type=F32)
                delta = jnp.sum(jnp.where(mask, product, 0.0), axis=1, keepdims=True)
                probs_low = probs[2 * pair + side]
                grad_scores = (probs_low.astype(F32) * (grad_probs - delta)).astype(BF16)
                parts.append(jnp.dot(grad_scores, key_rows, preferred_element_type=F32))
                k_turned[turn, :] = jnp.dot(q_turned[turn, :], grad_scores, preferred_element_type=F32)
                v_turned[turn, :] = jnp.dot(grad_turned[turn, :], probs_low, preferred_element_type=F32)
            q_grad = jnp.where((lane // HEAD_DIM) == 0, parts[0], parts[1]) * scale
            v_grad = v_turned[...].T
            mixed_grad[:, cols] = q_grad.astype(BF16)
            mixed_grad[:, local + base : local + base + two] = (k_turned[...].T * scale).astype(BF16)
            mixed_grad[:, 2 * local + base : 2 * local + base + two] = v_grad.astype(BF16)
            small[0, 0:1, cols] += jnp.sum(q_grad, axis=0, keepdims=True)
            small[0, 1:2, cols] += jnp.sum(v_grad, axis=0, keepdims=True)
        @pl.when(i + 1 < count)
        def _():
            for k in range(3):
                late_load(k, i + 1).start()

        values = source[i % 2].astype(F32)
        middle = jnp.sum(values, axis=1, keepdims=True) / width
        square = jnp.sum(values * values, axis=1, keepdims=True) / width
        inverse = lax.rsqrt(square - middle * middle + NORM_EPS)
        normed = (values - middle) * inverse
        normed1[i] = normed[:, :local]
        inverse1[i] = inverse
        scaled_in = normed * vectors_ref[0:1, :]
        far = product_of(slice(2 * local, 4 * local))
        theirs[i] = far.astype(BF16)
        given_copy(i).start()
        near = product_of(slice(0, 2 * local))
        mine[...] = near
        first = jnp.sum(far * vectors_ref[0:1, 2 * local :], axis=1, keepdims=True) + jnp.sum(
            near * vectors_ref[0:1, : 2 * local], axis=1, keepdims=True
        )
        second = jnp.sum(far * scaled_in[:, 2 * local :], axis=1, keepdims=True) + jnp.sum(
            near * scaled_in[:, : 2 * local], axis=1, keepdims=True
        )
        spread = jnp.where(lane == 0, first, jnp.where(lane == 1, second, 0.0))
        stat[i] = spread.T[:8, :]
        stat_copy(i).start()
        for part in range(4):
            span = slice(part * local, (part + 1) * local)
            term = lax.dot_general(low[:, span], mixed_grad[...], TN, preferred_element_type=F32)
            for c in range(3):
                qkv_sum[c, span, :] += term[:, c * local : (c + 1) * local]

        @pl.when(i + 1 < count)
        def _():
            late_load(3, i + 1).start()

        given_copy(i).wait_recv()
        kept_grad[i] = mine[:, :local] + given[i, :, :local].astype(F32)
        send[i] = (mine[:, local:] + given[i, :, local:].astype(F32)).astype(BF16)
        got_copy(i).start()
        stat_copy(i).wait_recv()
        stat_pair[i] = stat[i] + stat_given[i]
        stat_pair_copy(i).start()

        @pl.when(i == 0)
        def _():
            for code in codes:
                if code % 2 == 0:
                    dp_sum(0, code)
            row_next(0)
            once_load(3).wait()

        @pl.when(i == 1)
        def _():
            for code in codes:
                if code % 2:
                    dp_sum(1, code)
                    row_copy(1, code).start()

        @pl.when(i == count - 2)
        def _():
            once_load(5).wait()
            late_y.wait_recv()
            late_grad[:, :local] = (late_pair[:, :local].astype(F32) + late_in[:, local:].astype(F32)).astype(BF16)
            late_grad[:, local : 2 * local] = (late_pair[:, local:].astype(F32) + late_in[:, :local].astype(F32)).astype(BF16)
            late_core.start()

    outw_grad[...] = outw_sum[...].astype(BF16)
    half_outw[...] = outw_grad[:, half_of(dp, local)]
    for code in codes:
        dp_copy(2, code).start()
    qkv_grad[...] = qkv_sum[...].astype(BF16)
    half_qkv[...] = qkv_grad[:, :, half_of(dp, local)]
    for code in codes:
        dp_copy(3, code).start()
    for code in codes:
        if code % 2 == 0:
            dp_sum(1, code)
    row_next(1)
    row_last(0)
    once_load(4).wait()

    @pl.loop(0, count)
    def _(i):
        move_copy(i).wait_recv()
        finished[i] = (kept[i] + move_in[i].astype(F32)).astype(BF16)

    for w in (2, 3):
        for code in codes:
            if code % 2:
                dp_sum(w, code)
                row_copy(w, code).start()
    row_last(1)

    for w in (2, 3):
        for code in codes:
            if code % 2 == 0:
                dp_sum(w, code)
        row_next(w)

    @pl.loop(0, count)
    def _(i):
        got_copy(i).wait_recv()
        stat_pair_copy(i).wait_recv()
        sums = stat_pair[i] + stat_in[i]
        spread = jnp.concatenate([sums, jnp.zeros((two - 8, rows), F32)], axis=0).T / width
        grad = kept_grad[i] + got[i].astype(F32)
        small[0, 3:4, :] += jnp.sum(grad * normed1[i], axis=0, keepdims=True)
        small[0, 4:5, :] += jnp.sum(grad, axis=0, keepdims=True)
        scaled = grad * vectors_ref[0:1, :local]
        grad_hidden[i] += inverse1[i] * (scaled - spread[:, 0:1] - normed1[i] * spread[:, 1:2])

    pltpu.make_async_copy(finished, images_out, out_sem.at[0]).start()
    pltpu.make_async_copy(grad_hidden, images_grad_out, out_sem.at[1]).start()
    small_copy(0).start()
    row_last(2)
    row_last(3)
    for s in range(len(rounds)):
        small_copy(s).wait_recv()
        small[s + 1] = small[s] + small_in[s]
        if s + 1 < len(rounds):
            small_copy(s + 1).start()
    outs = ((tot_fc2, fc2_out), (tot_fc1, fc1_out), (tot_outw, outw_out), (tot_qkv, qkv_out))
    for w, (here, there) in enumerate(outs):
        tot_copy(w).wait_recv()
        pltpu.make_async_copy(here, there, out_sem.at[2 + w]).start()
    small_out[...] = small[len(rounds)]
    for i in range(count):
        given_copy(i).wait_send()
        stat_copy(i).wait_send()
        got_copy(i).wait_send()
        stat_pair_copy(i).wait_send()
        move_copy(i).wait_send()
    late_y.wait_send()
    late_core.wait_send()
    for s in range(len(rounds)):
        small_copy(s).wait_send()
    for w in range(4):
        tot_copy(w).wait_send()
        for code in codes:
            if w or code % 2 == 0:
                dp_copy(w, code).wait_send()
            if code:
                row_copy(w, code).wait_send()
    for k, (here, there) in enumerate(((finished, images_out), (grad_hidden, images_grad_out), *outs)):
        pltpu.make_async_copy(here, there, out_sem.at[k]).wait()


def back(
    source, total, cot, grad_low, mixed, probs, att, low, move, kept, qkv, outw, fc1_grad, fc2_half, fc2_grad, late, vectors, mlp_bias
):
    count, rows, width = source.shape
    local = width // 4
    row_count = lax.axis_size("row")
    block = width // row_count
    hidden = fc1_grad.shape[1]
    qkv_width = 3 * local
    heads = local // HEAD_DIM
    rounds = row_count.bit_length()
    outs = [
        ((count, rows, local), BF16), ((count, rows, local), F32), ((16, local), F32),
        ((3, block, local), BF16), ((block, local), BF16), ((block, hidden), BF16), ((block, hidden), BF16),
    ]
    own_f32 = ((count, rows, local), F32)
    own_low = ((count, rows, local), BF16)
    pair_low = ((count, rows, 2 * local), BF16)
    stat = ((count, 8, rows), F32)
    wide = ((rows, width), BF16)
    turned = ((2 * HEAD_DIM, rows), F32)
    columns = (((), hidden), ((), hidden), ((), local), ((3,), local))
    scratch = [
        ((2, rows, width), BF16), wide, wide, wide, ((rows, qkv_width), BF16), ((heads, rows, rows), BF16), ((rows, local), BF16), wide,
        wide, ((rows, qkv_width), BF16), own_f32, own_f32, ((count, rows, 1), F32),
        ((3, width, local), F32), ((width, local), F32), turned, turned,
        pair_low, pair_low, ((rows, 2 * local), F32), own_f32, own_low, own_low, stat, stat, stat, stat,
        ((rows, 2 * local), BF16), ((rows, 2 * local), BF16), wide, own_low, own_f32, own_low, ((3, width, local), BF16), ((width, local), BF16),
        ((3, width, local), BF16), ((width, local), BF16), ((rounds + 1, 16, local), F32), ((rounds, 16, local), F32),
        *[((*lead, width, c // 2), BF16) for lead, c in columns],
        *[((*lead, width, c // 2), BF16) for lead, c in columns],
        *[((row_count, *lead, block, c // 2), BF16) for lead, c in columns],
        *[((*lead, block, c), BF16) for lead, c in columns],
    ]
    dma = pltpu.SemaphoreType.DMA
    whole = pl.BlockSpec(memory_space=pl.ANY)
    vmem = pl.BlockSpec(memory_space=pltpu.VMEM)
    return pl.pallas_call(
        functools.partial(back_kernel, (count, rows, local, row_count)),
        out_shape=[jax.ShapeDtypeStruct(*s) for s in outs],
        in_specs=[whole] * 16 + [vmem] * 2,
        out_specs=[whole, whole, vmem] + [whole] * 4,
        scratch_shapes=[pltpu.VMEM(*s) for s in scratch]
        + [dma((4,)), dma((4,)), dma((6,)), dma((4, count)), dma((4, count)), dma((count,)), dma((count,)), dma((rounds,)), dma((rounds,))]
        + [dma((4, row_count))] * 4
        + [dma((4,)), dma((4,)), dma((2,)), dma((2,)), dma((6,))],
        name="back",
        compiler_params=pltpu.CompilerParams(
            vmem_limit_bytes=63 * 2**20, collective_id=2, has_side_effects=True
        ),
    )(source, total, cot, grad_low, mixed, probs, att, low, move, kept, qkv, outw, fc1_grad, fc2_half, fc2_grad, late, vectors, mlp_bias)


def adam_step(weight, grad, momentum, variance):
    moment_new = BETA_FIRST * momentum + (1.0 - BETA_FIRST) * grad
    second_new = BETA_SECOND * variance + (1.0 - BETA_SECOND) * grad * grad
    corrected = moment_new / (1.0 - BETA_FIRST**STEP)
    second_corrected = second_new / (1.0 - BETA_SECOND**STEP)
    master = weight.astype(jnp.float32)
    updated = master - LEARN_RATE * (
        corrected / (jnp.sqrt(second_corrected) + ADAM_EPS) + WEIGHT_DECAY * master
    )
    return (updated, moment_new, second_new)


def update_kernel(seq, *refs):
    images_in, grad_in, small = refs[:3]
    blocks = refs[3:19]
    images_out, grad_out = refs[19:21]
    grads = refs[21:25]
    sums = refs[25:33]
    fresh = refs[33:45]
    images_out[...] = images_in[:, :seq, :]
    grad_out[...] = grad_in[:, :seq, :]
    sums[0][...] = small[0:2, :]
    local = small.shape[1]
    for k, line in enumerate((2, None, 7, 3, 4, 5, 6)):
        if line is None:
            for part in range(4):
                sums[k + 1][:, part * local : (part + 1) * local] = small[8 + part : 9 + part, :]
        else:
            sums[k + 1][...] = small[line : line + 1, :]
    for w in range(4):
        weight, total, momentum, variance = (blocks[4 * w + k] for k in range(4))
        grad = total[...].astype(F32)
        grads[w][...] = grad
        updated, moment_new, second_new = adam_step(weight[...], grad, momentum[...], variance[...])
        fresh[w][...] = updated
        fresh[4 + w][...] = moment_new
        fresh[8 + w][...] = second_new


def update(images, images_grad, small, blocks, seq):
    count, rows, local = images.shape
    steps = 4

    def image_spec(lines):
        return pl.BlockSpec((1, lines, local), lambda i: (jnp.minimum(i, count - 1), 0, 0))

    def rows_spec(shape):
        if len(shape) == 3:
            return pl.BlockSpec((shape[0], shape[1] // steps, shape[2]), lambda i: (0, i, 0))
        return pl.BlockSpec((shape[0] // steps, shape[1]), lambda i: (i, 0))

    def whole_spec(shape):
        return pl.BlockSpec(shape, lambda i: (0, 0))

    flat = [array for group in blocks for array in group]
    shapes = [group[0].shape for group in blocks]
    hidden = shapes[2][1]
    sum_shapes = [(2, local), (1, local), (1, hidden), *[(1, local)] * 5]
    outs = [((count, seq, local), BF16), ((count, seq, local), F32)]
    outs += [(shape, F32) for shape in (*shapes, *sum_shapes, *shapes, *shapes, *shapes)]
    out_specs = [image_spec(seq), image_spec(seq), *[rows_spec(s) for s in shapes], *[whole_spec(s) for s in sum_shapes]]
    out_specs += [rows_spec(s) for s in shapes] * 3
    return pl.pallas_call(
        functools.partial(update_kernel, seq),
        grid=(steps,),
        out_shape=[jax.ShapeDtypeStruct(*s) for s in outs],
        in_specs=[image_spec(rows), image_spec(rows), whole_spec(small.shape), *[rows_spec(a.shape) for a in flat]],
        out_specs=out_specs,
        name="update",
        compiler_params=pltpu.CompilerParams(vmem_limit_bytes=63 * 2**20),
    )(images, images_grad, small, *flat)


def per_device(
    images_in,
    cotangent,
    first_gain,
    first_shift,
    second_gain,
    second_shift,
    qkv_weight,
    qv_bias,
    out_weight,
    out_bias,
    fc1_weight,
    fc1_bias,
    fc2_weight,
    fc2_bias,
    qkv_momentum,
    qkv_variance,
    out_momentum,
    out_variance,
    fc1_momentum,
    fc1_variance,
    fc2_momentum,
    fc2_variance,
):
    image_count, seq, local = images_in.shape
    width = 4 * local
    rows = -(-seq // ROW_TILE) * ROW_TILE
    place = lax.axis_index("col")

    vectors = [v[None] for v in (first_gain, first_shift, second_gain, second_shift, out_bias)]
    (
        source_all, cot_all, low_all, mixed_all, probs_all, att_all, total_all, grad_low2, qkv_full, out_full, vectors,
        move, kept, fc1_grad, fc2_half, fc2_grad, late, mlp_bias,
    ) = ahead(
        jnp.pad(images_in, ((0, 0), (0, rows - seq), (0, 0))),
        jnp.pad(cotangent, ((0, 0), (0, rows - seq), (0, 0))),
        qkv_weight.transpose(1, 0, 2),
        out_weight,
        fc1_weight,
        fc2_weight,
        vectors,
        qv_bias,
        fc1_bias[None],
        fc2_bias[None],
        seq,
    )
    images_out, images_grad, small, qkv_total, out_total, fc1_total, fc2_total = back(
        source_all, total_all, cot_all, grad_low2, mixed_all, probs_all, att_all, low_all, move, kept,
        qkv_full, out_full, fc1_grad, fc2_half, fc2_grad, late, vectors, mlp_bias,
    )
    def turned(value):
        return value.transpose(1, 0, 2)

    results = update(
        images_out,
        images_grad,
        small,
        (
            (turned(qkv_weight), qkv_total, turned(qkv_momentum), turned(qkv_variance)),
            (out_weight, out_total, out_momentum, out_variance),
            (fc1_weight, fc1_total, fc1_momentum, fc1_variance),
            (fc2_weight, fc2_total, fc2_momentum, fc2_variance),
        ),
        seq,
    )
    results = [turned(r) if k in (2, 14, 18, 22) else r for k, r in enumerate(results)]
    return tuple(r.reshape(-1) if 7 <= k < 14 else r for k, r in enumerate(results))


def solution(mesh):
    return jax.shard_map(
        per_device,
        mesh=mesh,
        in_specs=(
            P(("dp", "row"), None, "col"),
            P(("dp", "row"), None, "col"),
            P("col"),
            P("col"),
            P("col"),
            P("col"),
            P("row", None, "col"),
            P(None, "col"),
            P("row", "col"),
            P("col"),
            P("row", "col"),
            P("col"),
            P("row", "col"),
            P("col"),
            P("row", None, "col"),
            P("row", None, "col"),
            P("row", "col"),
            P("row", "col"),
            P("row", "col"),
            P("row", "col"),
            P("row", "col"),
            P("row", "col"),
        ),
        out_specs=(
            P(("dp", "row"), None, "col"),
            P(("dp", "row"), None, "col"),
            P("row", None, "col"),
            P("row", "col"),
            P("row", "col"),
            P("row", "col"),
            P(None, "col"),
            P("col"),
            P("col"),
            P("col"),
            P("col"),
            P("col"),
            P("col"),
            P("col"),
            P("row", None, "col"),
            P("row", "col"),
            P("row", "col"),
            P("row", "col"),
            P("row", None, "col"),
            P("row", "col"),
            P("row", "col"),
            P("row", "col"),
            P("row", None, "col"),
            P("row", "col"),
            P("row", "col"),
            P("row", "col"),
        ),
        check_vma=False,
    )
```
